32 devices in a mesh: wide: 16 (over z, y, core), narrow: 2 (over x).
Axes of the slice: x: 2, y: 2, z: 4, core: 2. Of those that a mesh axis runs over, the one named last changes fastest.
Arguments:
- examples: bfloat16 [80, 8192], P('wide', 'narrow'), may hold values from -6 to 6
- references: bfloat16 [128, 8192], P('wide', 'narrow'), may hold values from -6 to 6
- gate_weight: bfloat16 [8192, 28672], P('narrow', 'wide'), may hold values from -0.0625 to 0.0625
- up_weight: bfloat16 [8192, 28672], P('narrow', 'wide'), may hold values from -0.0625 to 0.0625
- down_weight: bfloat16 [28672, 8192], P('wide', 'narrow'), may hold values from -0.03125 to 0.03125
- cotangent: bfloat16 [80, 8192], P('wide', 'narrow'), may hold values from -6 to 6
- pair_ref: int32 [80, 4], replicated, may hold values from 0 to 127
- points: int32 [8], replicated, may hold values from 1 to 8
Outputs:
- expected: bfloat16 [80, 8192], P('wide', 'narrow')
The draws below stay inside these ranges and needn't reach their ends.
All inputs are finite; a program needn't handle non-finite values.
Results may differ from the reference program's by a relative error of at most 0.005.
Values may be sent and summed in bfloat16 or wider, within the bound.
No kernel may reach another device: no remote copies, remote signals or barrier semaphores. Data moves between devices by JAX's collectives and lax.ppermute only.
A program may use at most 128 MiB of HBM per device.

```python
import jax
import jax.numpy as jnp

D = 8192
FF = 28672
REFS = 128
PAIRS = 4
POINTS = 8
EXAMPLES = 80


def touch_ends(drawn, key, smallest, high):
    index_at = [jax.random.randint(jax.random.fold_in(key, axis), (), 0, length) for axis, length in enumerate(drawn.shape)]
    widest = drawn.shape.index(max(drawn.shape))
    next_to = index_at[:widest] + [(index_at[widest] + 1) % drawn.shape[widest]] + index_at[widest + 1:]
    return drawn.at[tuple(index_at)].set(smallest).at[tuple(next_to)].set(high)


def steps_of(own_key, dims, shards, smallest, top_value):
    factor_of = 1.0
    for axis_at, parts in shards:
        heights = jax.random.uniform(jax.random.fold_in(jax.random.fold_in(own_key, 6), axis_at), (parts,), jnp.float32, smallest / len(shards), top_value / len(shards))
        factor_of = factor_of * jnp.repeat(jnp.exp(heights), dims[axis_at] // parts).reshape((-1,) + (1,) * (len(dims) - 1 - axis_at))
    return factor_of


def noise(stream_key, shape, width, bound, cuts=(), dtype=jnp.bfloat16):
    drawn = jax.random.normal(stream_key, shape, jnp.float32) * width
    if len(cuts) > 0:
        drawn = steps_of(stream_key, shape, cuts, -0.22, 0.18) * drawn
    return jnp.clip(drawn, min=-bound, max=bound).astype(dtype)


def setup_inputs(seed: int = 0) -> dict:
    arg_keys = jax.random.split(jax.random.key(seed), 9)
    return {
        "examples": noise(arg_keys[0], (EXAMPLES, D), 1.0, 6.0, ((0, 16), (1, 2))),
        "references": noise(arg_keys[1], (REFS, D), 1.0, 6.0, ((0, 16), (1, 2))),
        "gate_weight": noise(arg_keys[2], (D, FF), D ** -0.5, 0.0625, ((0, 2), (1, 16))),
        "up_weight": noise(arg_keys[3], (D, FF), D ** -0.5, 0.0625, ((0, 2), (1, 16))),
        "down_weight": noise(arg_keys[4], (FF, D), FF ** -0.5, 0.03125, ((0, 16), (1, 2))),
        "cotangent": noise(arg_keys[5], (EXAMPLES, D), 1.0, 6.0, ((0, 16), (1, 2))),
        "pair_ref": touch_ends(jax.random.randint(arg_keys[6], (EXAMPLES, PAIRS), 0, REFS), jax.random.fold_in(arg_keys[6], 1), 0, REFS - 1).astype(jnp.int32),
        "points": touch_ends(jax.random.randint(arg_keys[7], (POINTS,), 1, 9), jax.random.fold_in(arg_keys[7], 1), 1, 8).astype(jnp.int32),
    }


def path_coefficients(example_gate, example_up, reference_gate, reference_up, pair_ref, points):
    alphas = points.astype(jnp.float32) / 8.0
    coef_gate = jnp.zeros(example_gate.shape, jnp.float32)
    coef_up = jnp.zeros(example_gate.shape, jnp.float32)
    for pair_slot in range(pair_ref.shape[1]):
        chosen = pair_ref[:, pair_slot].astype(jnp.int32)
        base_gate = jnp.take(reference_gate, chosen, axis=0)
        base_up = jnp.take(reference_up, chosen, axis=0)
        step_gate = example_gate - base_gate
        step_up = example_up - base_up
        for point_slot in range(alphas.shape[0]):
            position = alphas[point_slot]
            along_gate = base_gate + position * step_gate
            along_up = base_up + position * step_up
            sigmoid = jax.nn.sigmoid(along_gate)
            coef_gate = coef_gate + along_up * sigmoid * (1.0 + along_gate * (1.0 - sigmoid))
            coef_up = coef_up + along_gate * sigmoid
    total = pair_ref.shape[1] * alphas.shape[0]
    return coef_gate / total, coef_up / total


def reference(examples, references, gate_weight, up_weight, down_weight, cotangent, pair_ref, points):
    example_gate = jnp.dot(examples, gate_weight, preferred_element_type=jnp.float32)
    example_up = jnp.dot(examples, up_weight, preferred_element_type=jnp.float32)
    reference_gate = jnp.dot(references, gate_weight, preferred_element_type=jnp.float32)
    reference_up = jnp.dot(references, up_weight, preferred_element_type=jnp.float32)
    upstream = jnp.dot(cotangent, down_weight.T, preferred_element_type=jnp.float32)
    coef_gate, coef_up = path_coefficients(example_gate, example_up, reference_gate, reference_up, pair_ref, points)
    grad_gate = (upstream * coef_gate).astype(jnp.bfloat16)
    grad_up = (upstream * coef_up).astype(jnp.bfloat16)
    result = jnp.dot(grad_gate, gate_weight.T, preferred_element_type=jnp.float32)
    result = result + jnp.dot(grad_up, up_weight.T, preferred_element_type=jnp.float32)
    return result.astype(jnp.bfloat16)
```

```python
import functools

import jax
import jax.numpy as jnp
from jax import lax
from jax.experimental import pallas as pl
from jax.experimental.pallas import tpu as pltpu
from jax.sharding import PartitionSpec as P


VMEM = pl.BlockSpec(memory_space=pltpu.VMEM)
SMEM = pl.BlockSpec(memory_space=pltpu.SMEM)
ANY = pl.BlockSpec(memory_space=pl.ANY)


def factors(size):
    pair = 2 if size % 2 == 0 else 1
    near = 2 if (size // pair) % 2 == 0 else 1
    return size // (pair * near), near, pair


def rounded(rows, unit):
    return -(-rows // unit) * unit


def shift_permute(array, axis, dims, digit, amount):
    below = 1
    for size in dims[digit + 1:]:
        below *= size
    size = dims[digit]
    total = below * size
    for d in dims[:digit]:
        total *= d
    pairs = []
    for at in range(total):
        own = (at // below) % size
        to = (own + amount) % size
        pairs.append((at, at + (to - own) * below))
    return lax.ppermute(array, axis, pairs)


def selection(blocks, kept, padded):
    row = lax.broadcasted_iota(jnp.int32, (blocks * kept, blocks * padded), 0)
    col = lax.broadcasted_iota(jnp.int32, (blocks * kept, blocks * padded), 1)
    wanted = jnp.zeros_like(col)
    for b in range(blocks):
        inside = (row >= b * kept) & (row < (b + 1) * kept)
        wanted = jnp.where(inside, row - b * kept + b * padded, wanted)
    return (col == wanted).astype(jnp.float32).astype(jnp.bfloat16)


def assemble(own, layout, width):
    blocks = len(own)

    def body(*refs):
        out, stack = refs[-2], refs[-1]
        start = at = 0
        for kept, padded in layout:
            for b in range(blocks):
                rows = refs[b][pl.ds(start, padded), :]
                if kept == padded:
                    out[pl.ds(at + b * kept, kept), :] = rows
                else:
                    stack[pl.ds(b * padded, padded), :] = rows
            if kept != padded:
                out[pl.ds(at, blocks * kept), :] = jnp.dot(
                    selection(blocks, kept, padded),
                    stack[pl.ds(0, blocks * padded), :],
                    preferred_element_type=jnp.float32,
                ).astype(jnp.bfloat16)
            start += padded
            at += blocks * kept

    dtype = own[0].dtype
    return pl.pallas_call(
        body,
        out_shape=jax.ShapeDtypeStruct((blocks * sum(kept for kept, _ in layout), width), dtype),
        in_specs=[VMEM] * blocks,
        out_specs=VMEM,
        scratch_shapes=[pltpu.VMEM((blocks * max(padded for _, padded in layout), width), dtype)],
        compiler_params=pltpu.CompilerParams(vmem_limit_bytes=12 * 1024 * 1024),
        cost_estimate=pl.CostEstimate(flops=10**9, bytes_accessed=10**6, transcendentals=0),
        name="assemble",
    )(*own)


def join(halves, layout):
    width = halves[0].shape[1]
    blocks = halves[0].shape[0] // sum(layout)
    e, r, k = (blocks * rows for rows in layout)
    count = len(halves)

    def body(*refs):
        main, side = refs[-2:]
        for h in range(count):
            main[pl.ds(h * e, e), :] = refs[h][pl.ds(0, e), :]
            main[pl.ds(count * e + h * r, r), :] = refs[h][pl.ds(e, r), :]
            side[pl.ds(h * k, k), :] = refs[h][pl.ds(e + r, k), :]

    dtype = halves[0].dtype
    return pl.pallas_call(
        body,
        out_shape=(
            jax.ShapeDtypeStruct((count * (e + r), width), dtype),
            jax.ShapeDtypeStruct((count * k, width), dtype),
        ),
        in_specs=[VMEM] * count,
        out_specs=(VMEM, VMEM),
        compiler_params=pltpu.CompilerParams(vmem_limit_bytes=12 * 1024 * 1024),
        cost_estimate=pl.CostEstimate(flops=10**9, bytes_accessed=10**6, transcendentals=0),
        name="join",
    )(*halves)


def across(left, right):
    return lax.dot_general(left, right, (((1,), (1,)), ((), ())), preferred_element_type=jnp.float32)


def parts_of(size, unit):
    for count in (4, 2):
        if size % (count * unit) == 0:
            return [(i * (size // count), size // count) for i in range(count)]
    return [(0, size)]


def forward(main, side, weights, start, width, aligned, dtype):
    rows, side_rows = main.shape[0], side.shape[0]
    depth = main.shape[1]
    by_depth, by_unit = parts_of(depth, 128), parts_of(width, 32)

    def body(at, main_ref, side_ref, gate_hbm, up_hbm, down_hbm, out, gate, up, down, total, sems):
        first = pl.multiple_of(at[0], 128) if aligned else 0
        cols = pl.ds(first, width)
        copies = {}
        for w, (source, target) in enumerate(((gate_hbm, gate), (up_hbm, up))):
            for i, (row, count) in enumerate(by_depth):
                some = pl.ds(row, count)
                copies[w, i] = pltpu.make_async_copy(source.at[some, cols], target.at[some], sems.at[w, i])
        for i, (row, count) in enumerate(by_unit):
            copies[2, i] = pltpu.make_async_copy(
                down_hbm.at[pl.ds(first + row, count)], down.at[pl.ds(row, count)], sems.at[2, i]
            )
        for copy in copies.values():
            copy.start()
        for w, target in enumerate((gate, up)):
            for i, (row, count) in enumerate(by_depth):
                copies[w, i].wait()
                some = pl.ds(row, count)
                part = jnp.dot(main_ref[:, some], target[some, :], preferred_element_type=jnp.float32)
                if i == len(by_depth) - 1:
                    if i > 0:
                        part = total[...] + part
                    out[pl.ds(w * rows, rows), :] = part.astype(dtype)
                elif i == 0:
                    total[...] = part
                else:
                    total[...] += part
        for i, (row, count) in enumerate(by_unit):
            copies[2, i].wait()
            out[pl.ds(2 * rows, side_rows), pl.ds(row, count)] = across(
                side_ref[...], down[pl.ds(row, count), :]
            ).astype(dtype)

    flops = 2 * depth * width * (2 * rows + side_rows)
    return pl.pallas_call(
        body,
        out_shape=jax.ShapeDtypeStruct((2 * rows + side_rows, width), dtype),
        in_specs=[SMEM, VMEM, VMEM, ANY, ANY, ANY],
        out_specs=VMEM,
        scratch_shapes=[
            pltpu.VMEM((depth, width), jnp.bfloat16),
            pltpu.VMEM((depth, width), jnp.bfloat16),
            pltpu.VMEM((width, depth), jnp.bfloat16),
            pltpu.VMEM((rows, width), jnp.float32),
            pltpu.SemaphoreType.DMA((3, 4)),
        ],
        compiler_params=pltpu.CompilerParams(vmem_limit_bytes=24 * 1024 * 1024),
        cost_estimate=pl.CostEstimate(
            flops=flops, bytes_accessed=6 * depth * width, transcendentals=0
        ),
        name="forward",
    )(start, main, side, *weights)


def coefficients(kept, received, chosen, points, examples, references):
    width = kept.shape[1]
    rows = examples + references
    pairs = chosen.shape[1]
    count = points.shape[0]
    lanes = 128 if width % 128 == 0 else width
    piece = 16 if examples % 16 == 0 else examples
    scale = 1.0 / (pairs * count)

    def body(points_ref, chosen_ref, kept_ref, *refs):
        got, out, base_gate, base_up = refs[:-3], refs[-3], refs[-2], refs[-1]

        def total(start, size):
            value = kept_ref[pl.ds(start, size), :]
            for ref in got:
                value = value + ref[pl.ds(start, size), :].astype(jnp.float32)
            return value

        picks = jnp.concatenate(
            [
                (
                    lax.broadcasted_iota(jnp.int32, (examples, references), 1)
                    == chosen_ref[:, pl.ds(p, 1)]
                ).astype(jnp.float32)
                for p in range(pairs)
            ],
            axis=0,
        ).astype(jnp.bfloat16)
        for start, target in ((examples, base_gate), (rows + examples, base_up)):
            value = total(start, references)
            high = value.astype(jnp.bfloat16)
            low = (value - high.astype(jnp.float32)).astype(jnp.bfloat16)
            target[...] = jnp.dot(picks, high, preferred_element_type=jnp.float32) + jnp.dot(
                picks, low, preferred_element_type=jnp.float32
            )
        steps = [points_ref[m].astype(jnp.float32) * 0.125 for m in range(count)]
        for first in range(0, examples, piece):
            gate = total(first, piece) * 0.5
            up = total(rows + first, piece)
            coef_gate = jnp.zeros_like(gate)
            coef_up = jnp.zeros_like(gate)
            for p in range(pairs):
                start = base_gate[pl.ds(p * examples + first, piece), :] * 0.5
                span = gate - start
                flat = jnp.zeros_like(gate)
                tilted = jnp.zeros_like(gate)
                for t in steps:
                    half = start + t * span
                    two_s = 1.0 + jnp.tanh(half)
                    silu = half * two_s
                    slope = two_s + silu * (2.0 - two_s)
                    coef_up = coef_up + silu
                    flat = flat + slope
                    tilted = tilted + t * slope
                start_up = base_up[pl.ds(p * examples + first, piece), :]
                coef_gate = coef_gate + (start_up * flat + (up - start_up) * tilted)
            upstream = total(2 * rows + first, piece)
            out[pl.ds(first, piece), :] = (upstream * (coef_gate * (0.5 * scale))).astype(jnp.bfloat16)
            out[pl.ds(examples + first, piece), :] = (upstream * (coef_up * scale)).astype(jnp.bfloat16)

    all_rows = kept.shape[0]
    block = lambda n: pl.BlockSpec((n, lanes), lambda j: (0, j))
    return pl.pallas_call(
        body,
        grid=(width // lanes,),
        out_shape=jax.ShapeDtypeStruct((2 * examples, width), jnp.bfloat16),
        in_specs=[
            SMEM,
            pl.BlockSpec(chosen.shape, lambda j: (0, 0)),
            block(all_rows),
        ]
        + [block(all_rows)] * len(received),
        out_specs=block(2 * examples),
        scratch_shapes=[pltpu.VMEM((pairs * examples, lanes), jnp.float32)] * 2,
        compiler_params=pltpu.CompilerParams(vmem_limit_bytes=12 * 1024 * 1024),
        cost_estimate=pl.CostEstimate(flops=5 * 10**9, bytes_accessed=10**6, transcendentals=0),
        name="coefficients",
    )(points, chosen, kept, *received)


def backward(grads, weights, start, total, aligned, final):
    rows = grads.shape[0] // 2
    width = grads.shape[1]
    depth = weights[0].shape[0]
    by_depth = parts_of(depth, 128)

    def body(at, *refs):
        grads_ref, gate_hbm, up_hbm, *refs = refs
        *outs, gate, up, sems = refs
        first = pl.multiple_of(at[0], 128) if aligned else 0
        copies = {}
        for i, (row, count) in enumerate(by_depth):
            some = pl.ds(row, count)
            for w, (source, target) in enumerate(((gate_hbm, gate), (up_hbm, up))):
                copies[w, i] = pltpu.make_async_copy(
                    source.at[some, pl.ds(first, width)], target.at[some], sems.at[w, i]
                )
                copies[w, i].start()
        for i, (row, count) in enumerate(by_depth):
            some = pl.ds(row, count)
            copies[0, i].wait()
            copies[1, i].wait()
            value = across(grads_ref[pl.ds(0, rows), :], gate[some, :]) + across(
                grads_ref[pl.ds(rows, rows), :], up[some, :]
            )
            if total is not None:
                value = value + outs[0][:, some]
            if final:
                outs[-2][:, some] = value[rows // 2:, :].astype(jnp.bfloat16)
                outs[-1][:, some] = value[:rows // 2, :]
            else:
                outs[-1][:, some] = value

    operands = [grads, *weights]
    specs = [VMEM, ANY, ANY]
    if total is not None:
        operands.append(total)
        specs.append(VMEM)
    if final:
        out_shape = (
            jax.ShapeDtypeStruct((rows // 2, depth), jnp.bfloat16),
            jax.ShapeDtypeStruct((rows // 2, depth), jnp.float32),
        )
        out_specs = (VMEM, VMEM)
    else:
        out_shape, out_specs = jax.ShapeDtypeStruct((rows, depth), jnp.float32), VMEM
    return pl.pallas_call(
        body,
        out_shape=out_shape,
        in_specs=[SMEM] + specs,
        out_specs=out_specs,
        scratch_shapes=[
            pltpu.VMEM((depth, width), jnp.bfloat16),
            pltpu.VMEM((depth, width), jnp.bfloat16),
            pltpu.SemaphoreType.DMA((2, 4)),
        ],
        compiler_params=pltpu.CompilerParams(vmem_limit_bytes=20 * 1024 * 1024),
        cost_estimate=pl.CostEstimate(
            flops=4 * rows * width * depth, bytes_accessed=4 * width * depth, transcendentals=0
        ),
        name="backward",
    )(start, *operands)


def chunks_of(width):
    if width % 128 or width < 512:
        return [(0, width)]
    first = rounded(width // 2, 256)
    return [(0, first), (first, width - first)]


def on_device(
    examples, references, gate_weight, up_weight, down_weight, cotangent, pair_ref, points
):
    dims = factors(lax.axis_size("wide"))
    far, near, pair = dims
    peers = lax.axis_size("narrow")
    e, r, k = examples.shape[0], references.shape[0], cotangent.shape[0]
    ep, rp, kp = rounded(e, 8), rounded(r, 8), rounded(k, 8)
    depth, hidden = gate_weight.shape
    blocks = far * near * pair

    at = lax.axis_index("wide")
    z, y, c = at // (near * pair), (at // pair) % near, at % pair
    n = lax.axis_index("narrow")

    def padded(array, rows):
        return jnp.pad(array, ((0, rows - array.shape[0]), (0, 0)))

    own = jnp.concatenate([padded(examples, ep), padded(references, rp), padded(cotangent, kp)])
    column = [own] + [shift_permute(own, "wide", dims, 0, s) for s in range(1, far)]
    plane = list(column)
    for b in range(1, near):
        plane += [shift_permute(x, "wide", dims, 1, b) for x in column]
    half = assemble(plane, ((e, ep), (r, rp), (k, kp)), depth)
    halves = [half] + [shift_permute(half, "wide", dims, 2, b) for b in range(1, pair)]
    main, side = join(halves, (e, r, k))

    order = jnp.asarray(
        [[s, b, q] for q in range(pair) for b in range(near) for s in range(far)], jnp.int32
    )
    owner = (
        ((z - order[:, 0]) % far * near + (y - order[:, 1]) % near) * pair + (c - order[:, 2]) % pair
    )
    chosen = jnp.take(pair_ref.reshape(blocks, -1), owner, axis=0).reshape(blocks * e, -1)
    host, inside = chosen // r, chosen % r
    back = (z - host // (near * pair)) % far
    beside = (y - host // pair % near) % near
    chosen = (((c - host % pair) % pair * near + beside) * far + back) * r + inside

    share = hidden // peers
    aligned = share % 128 == 0
    if aligned:
        gate_weight, up_weight, down_weight = (
            pltpu.with_memory_space_constraint(w, pltpu.MemorySpace.HBM)
            for w in (gate_weight, up_weight, down_weight)
        )

    def at_peer(m, offset, width):
        start = m * share + offset
        if aligned:
            return jnp.reshape(start, (1,)).astype(jnp.int32), (gate_weight, up_weight, down_weight)
        return jnp.zeros((1,), jnp.int32), (
            lax.dynamic_slice_in_dim(gate_weight, start, width, 1),
            lax.dynamic_slice_in_dim(up_weight, start, width, 1),
            lax.dynamic_slice_in_dim(down_weight, start, width, 0),
        )

    parts = []
    for offset, width in chunks_of(share):
        received = []
        for s in range(1, peers):
            start, weights = at_peer((n + s) % peers, offset, width)
            sent = forward(main, side, weights, start, width, aligned, jnp.bfloat16)
            received.append(shift_permute(sent, "narrow", (peers,), 0, s))
        parts.append((offset, width, received))

    jobs = []
    for offset, width, received in parts:
        start, weights = at_peer(n, offset, width)
        kept = forward(main, side, weights, start, width, aligned, jnp.float32)
        grads = coefficients(kept, received, chosen, points, blocks * e, blocks * r)
        jobs.append((grads, offset, width, 0))
        jobs += [
            (shift_permute(grads, "narrow", (peers,), 0, s), offset, width, s) for s in range(1, peers)
        ]
    jobs.sort(key=lambda job: job[3])
    total = None
    for i, (grads, offset, width, s) in enumerate(jobs):
        start, weights = at_peer((n - s) % peers, offset, width)
        total = backward(
            grads, weights[:2], start, total, aligned, i == len(jobs) - 1 and pair == 2
        )

    if pair == 2:
        sent, kept = total
        total = kept + shift_permute(sent, "wide", dims, 2, 1).astype(jnp.float32)
    if near == 2:
        half = total.shape[0] // 2
        sent = total[half:].astype(jnp.bfloat16)
        total = total[:half] + shift_permute(sent, "wide", dims, 1, 1).astype(jnp.float32)
    result = total[:e]
    got = [
        shift_permute(total[s * e:(s + 1) * e].astype(jnp.bfloat16), "wide", dims, 0, far - s)
        for s in range(1, far)
    ]
    for piece in got:
        result = result + piece.astype(jnp.float32)
    return result.astype(jnp.bfloat16)


def solution(mesh):
    in_specs = (
        P("wide", "narrow"),
        P("wide", "narrow"),
        P("narrow", "wide"),
        P("narrow", "wide"),
        P("wide", "narrow"),
        P("wide", "narrow"),
        P(),
        P(),
    )
    out_specs = P("wide", "narrow")
    return jax.shard_map(
        on_device, mesh=mesh, in_specs=in_specs, out_specs=out_specs, check_vma=False
    )
```

```python
import functools

import jax
import jax.numpy as jnp
from jax import lax
from jax.experimental import pallas as pl
from jax.experimental.pallas import tpu as pltpu
from jax.sharding import PartitionSpec as P


VMEM = pl.BlockSpec(memory_space=pltpu.VMEM)
SMEM = pl.BlockSpec(memory_space=pltpu.SMEM)
ANY = pl.BlockSpec(memory_space=pl.ANY)


def factors(size):
    pair = 2 if size % 2 == 0 else 1
    near = 2 if (size // pair) % 2 == 0 else 1
    return size // (pair * near), near, pair


def rounded(rows, unit):
    return -(-rows // unit) * unit


def shift_permute(array, axis, dims, digit, amount):
    below = 1
    for size in dims[digit + 1:]:
        below *= size
    size = dims[digit]
    total = below * size
    for d in dims[:digit]:
        total *= d
    pairs = []
    for at in range(total):
        own = (at // below) % size
        to = (own + amount) % size
        pairs.append((at, at + (to - own) * below))
    return lax.ppermute(array, axis, pairs)


def pack(arrays):
    rows = jnp.concatenate(arrays)
    count, width = rows.shape
    whole = count // 8 * 8
    rest = count - whole
    if rest == 0:
        return rows, whole, 1
    pieces = whole // rest if whole else 0
    if not pieces or whole % rest or width % (pieces * 128):
        return jnp.pad(rows, ((0, 8 - rest), (0, 0))), whole + 8, 1
    cut = rows[whole:].reshape(rest * pieces, width // pieces)
    return jnp.concatenate([rows[:whole], cut], axis=1), whole, pieces


def assemble(own, whole, pieces, counts, width):
    blocks = len(own)
    packed = own[0].shape
    total = blocks * sum(counts)
    across_lanes = width // pieces

    def body(*refs):
        out, stack = refs[-2], refs[-1]
        for b in range(blocks):
            stack[pl.ds(b * packed[0], packed[0]), :] = refs[b][...]
        row = lax.broadcasted_iota(jnp.int32, (total, blocks * packed[0]), 0)
        col = lax.broadcasted_iota(jnp.int32, (total, blocks * packed[0]), 1)
        held = jnp.zeros_like(row)
        block = jnp.zeros_like(row)
        at = first = 0
        for count in counts:
            for b in range(blocks):
                inside = (row >= at) & (row < at + count)
                held = jnp.where(inside, row - at + first, held)
                block = jnp.where(inside, b, block)
                at += count
            first += count

        def pick(wanted, valid):
            return (valid & (col == wanted)).astype(jnp.float32).astype(jnp.bfloat16)

        base = block * packed[0]
        uncut = pick(base + held, held < whole)
        for j in range(pieces):
            lanes = pl.ds(j * across_lanes, across_lanes)
            value = jnp.dot(uncut, stack[:, lanes], preferred_element_type=jnp.float32)
            if packed[1] > width:
                value = value + jnp.dot(
                    pick(base + (held - whole) * pieces + j, held >= whole),
                    stack[:, pl.ds(width, across_lanes)],
                    preferred_element_type=jnp.float32,
                )
            out[:, lanes] = value.astype(jnp.bfloat16)

    dtype = own[0].dtype
    return pl.pallas_call(
        body,
        out_shape=jax.ShapeDtypeStruct((total, width), dtype),
        in_specs=[VMEM] * blocks,
        out_specs=VMEM,
        scratch_shapes=[pltpu.VMEM((blocks * packed[0], packed[1]), dtype)],
        compiler_params=pltpu.CompilerParams(vmem_limit_bytes=6 * 1024 * 1024),
        cost_estimate=pl.CostEstimate(flops=10**9, bytes_accessed=10**6, transcendentals=0),
        name="assemble",
    )(*own)


def join(halves, layout):
    width = halves[0].shape[1]
    blocks = halves[0].shape[0] // sum(layout)
    e, r, k = (blocks * rows for rows in layout)
    count = len(halves)

    def body(*refs):
        main, side = refs[-2:]
        for h in range(count):
            main[pl.ds(h * e, e), :] = refs[h][pl.ds(0, e), :]
            main[pl.ds(count * e + h * r, r), :] = refs[h][pl.ds(e, r), :]
            side[pl.ds(h * k, k), :] = refs[h][pl.ds(e + r, k), :]

    dtype = halves[0].dtype
    return pl.pallas_call(
        body,
        out_shape=(
            jax.ShapeDtypeStruct((count * (e + r), width), dtype),
            jax.ShapeDtypeStruct((count * k, width), dtype),
        ),
        in_specs=[VMEM] * count,
        out_specs=(VMEM, VMEM),
        compiler_params=pltpu.CompilerParams(vmem_limit_bytes=4 * 1024 * 1024),
        cost_estimate=pl.CostEstimate(flops=10**9, bytes_accessed=10**6, transcendentals=0),
        name="join",
    )(*halves)


def across(left, right):
    return lax.dot_general(left, right, (((1,), (1,)), ((), ())), preferred_element_type=jnp.float32)


def parts_of(size, unit):
    for count in (4, 2):
        if size % (count * unit) == 0:
            return [(i * (size // count), size // count) for i in range(count)]
    return [(0, size)]


def streams(weights, buffers, sems, first, width, by_depth, by_unit):
    gate, up, down = weights
    both, below = buffers
    units, depths = [], []
    for i, (row, count) in enumerate(by_unit):
        units.append(
            pltpu.make_async_copy(
                down.at[pl.ds(first + row, count)], below.at[pl.ds(row, count)], sems.at[2, i]
            )
        )
    for i, (row, count) in enumerate(by_depth):
        some = pl.ds(row, count)
        depths.append(
            [
                pltpu.make_async_copy(
                    source.at[some, pl.ds(first, width)],
                    both.at[some, pl.ds(w * width, width)],
                    sems.at[w, i],
                )
                for w, source in enumerate((gate, up))
            ]
        )
    return units, depths


def fetch(weights, start, width, aligned):
    depth = weights[0].shape[0]
    by_depth, by_unit = parts_of(depth, 128), parts_of(width, 32)

    def body(at, gate, up, down, both, below, ready, sems):
        first = pl.multiple_of(at[0], 128) if aligned else 0
        units, depths = streams((gate, up, down), (both, below), sems, first, width, by_depth, by_unit)
        copies = units + [copy for pair in depths for copy in pair]
        for copy in copies:
            copy.start()
        ready[...] = jnp.zeros_like(ready)
        for copy in copies:
            copy.wait()

    return pl.pallas_call(
        body,
        out_shape=(
            pltpu.VMEM((depth, 2 * width), jnp.bfloat16),
            pltpu.VMEM((width, depth), jnp.bfloat16),
            jax.ShapeDtypeStruct((8, 128), jnp.float32),
        ),
        in_specs=[SMEM, ANY, ANY, ANY],
        out_specs=(VMEM, VMEM, VMEM),
        scratch_shapes=[pltpu.SemaphoreType.DMA((3, 4))],
        compiler_params=pltpu.CompilerParams(vmem_limit_bytes=1024 * 1024),
        cost_estimate=pl.CostEstimate(
            flops=4 * 10**9, bytes_accessed=6 * depth * width, transcendentals=0
        ),
        name="fetch",
    )(start, *weights)


def forward(main, side, weights, start, width, aligned, dtype, fetched=False):
    rows, half = main.shape[0], side.shape[0] // 2
    depth = main.shape[1]
    by_depth, by_unit = parts_of(depth, 128), parts_of(width, 32)

    def put_side(out, value, lanes):
        first, count = lanes
        out[pl.ds(rows, half), pl.ds(first, count)] = value[:half].astype(dtype)
        out[pl.ds(rows, half), pl.ds(width + first, count)] = value[half:].astype(dtype)

    def body_fetched(main_ref, side_ref, both, below, out):
        out[pl.ds(0, rows), :] = jnp.dot(
            main_ref[...], both[...], preferred_element_type=jnp.float32
        ).astype(dtype)
        put_side(out, across(side_ref[...], below[...]), (0, width))

    def body(at, main_ref, side_ref, gate, up, down, out, both, below, total, sems):
        first = pl.multiple_of(at[0], 128) if aligned else 0
        units, depths = streams((gate, up, down), (both, below), sems, first, width, by_depth, by_unit)
        for copy in units + [copy for pair in depths for copy in pair]:
            copy.start()
        for copy in units:
            copy.wait()
        put_side(out, across(side_ref[...], below[...]), (0, width))
        for i, (row, count) in enumerate(by_depth):
            for copy in depths[i]:
                copy.wait()
            some = pl.ds(row, count)
            part = jnp.dot(main_ref[:, some], both[some, :], preferred_element_type=jnp.float32)
            if i > 0:
                part = total[...] + part
            if i == len(by_depth) - 1:
                out[pl.ds(0, rows), :] = part.astype(dtype)
            else:
                total[...] = part

    common = dict(
        out_shape=jax.ShapeDtypeStruct((rows + half, 2 * width), dtype),
        out_specs=VMEM,
        cost_estimate=pl.CostEstimate(
            flops=4 * depth * width * (rows + half), bytes_accessed=6 * depth * width, transcendentals=0
        ),
        name="forward",
    )
    if fetched:
        return pl.pallas_call(
            body_fetched,
            in_specs=[VMEM] * 4,
            compiler_params=pltpu.CompilerParams(vmem_limit_bytes=4 * 1024 * 1024),
            **common,
        )(main, side, *weights)
    return pl.pallas_call(
        body,
        in_specs=[SMEM, VMEM, VMEM, ANY, ANY, ANY],
        scratch_shapes=[
            pltpu.VMEM((depth, 2 * width), jnp.bfloat16),
            pltpu.VMEM((width, depth), jnp.bfloat16),
            pltpu.VMEM((rows, 2 * width), jnp.float32),
            pltpu.SemaphoreType.DMA((3, 4)),
        ],
        compiler_params=pltpu.CompilerParams(vmem_limit_bytes=20 * 1024 * 1024),
        **common,
    )(start, main, side, *weights)


def coefficients(kept, received, chosen, points, examples, references):
    width = kept.shape[1] // 2
    rows = examples + references
    pairs = chosen.shape[1]
    count = points.shape[0]
    lanes = 128 if width % 128 == 0 else width
    piece = 16 if examples % 32 == 16 else examples // 2
    scale = 1.0 / (pairs * count)

    def body(points_ref, chosen_ref, kept_ref, *refs):
        got, out, base_gate, base_up = refs[:-3], refs[-3], refs[-2], refs[-1]
        picks = jnp.concatenate(
            [
                (
                    lax.broadcasted_iota(jnp.int32, (examples, references), 1)
                    == chosen_ref[:, pl.ds(p, 1)]
                ).astype(jnp.float32)
                for p in range(pairs)
            ],
            axis=0,
        ).astype(jnp.bfloat16)
        steps = [points_ref[m].astype(jnp.float32) * 0.125 for m in range(count)]

        def block(j, _):
            if lanes == width:
                of = [pl.ds(w * width, width) for w in range(2)]
            else:
                of = [pl.ds(pl.multiple_of(w * width + j * lanes, 128), lanes) for w in range(2)]

            def total(start, size, w):
                value = kept_ref[pl.ds(start, size), of[w]]
                for ref in got:
                    value = value + ref[pl.ds(start, size), of[w]].astype(jnp.float32)
                return value

            for w, target in enumerate((base_gate, base_up)):
                value = total(0, references, w)
                high = value.astype(jnp.bfloat16)
                low = (value - high.astype(jnp.float32)).astype(jnp.bfloat16)
                target[...] = jnp.dot(picks, high, preferred_element_type=jnp.float32) + jnp.dot(
                    picks, low, preferred_element_type=jnp.float32
                )
            upstream = [total(rows, examples // 2, w) for w in range(2)]
            for first in range(0, examples, piece):
                gate = total(references + first, piece, 0) * 0.5
                up = total(references + first, piece, 1)
                coef_gate = jnp.zeros_like(gate)
                coef_up = jnp.zeros_like(gate)
                for p in range(pairs):
                    start = base_gate[pl.ds(p * examples + first, piece), :] * 0.5
                    span = gate - start
                    flat = jnp.zeros_like(gate)
                    tilted = jnp.zeros_like(gate)
                    for t in steps:
                        half = start + t * span
                        two_s = 1.0 + jnp.tanh(half)
                        silu = half * two_s
                        slope = two_s + silu * (2.0 - two_s)
                        coef_up = coef_up + silu
                        flat = flat + slope
                        tilted = tilted + t * slope
                    start_up = base_up[pl.ds(p * examples + first, piece), :]
                    coef_gate = coef_gate + (start_up * flat + (up - start_up) * tilted)
                base_gate[pl.ds(first, piece), :] = coef_gate * (0.5 * scale)
                base_up[pl.ds(first, piece), :] = coef_up * scale
            for w, source in enumerate((base_gate, base_up)):
                for h in range(2):
                    some = pl.ds(h * (examples // 2), examples // 2)
                    out[some, of[w]] = (upstream[h] * source[some, :]).astype(jnp.bfloat16)
            return 0

        lax.fori_loop(0, width // lanes, block, 0)

    return pl.pallas_call(
        body,
        out_shape=jax.ShapeDtypeStruct((examples, 2 * width), jnp.bfloat16),
        in_specs=[SMEM, VMEM, VMEM] + [VMEM] * len(received),
        out_specs=VMEM,
        scratch_shapes=[pltpu.VMEM((pairs * examples, lanes), jnp.float32)] * 2,
        compiler_params=pltpu.CompilerParams(vmem_limit_bytes=4 * 1024 * 1024),
        cost_estimate=pl.CostEstimate(flops=5 * 10**9, bytes_accessed=10**6, transcendentals=0),
        name="coefficients",
    )(points, chosen, kept, *received)


def backward(grads, weights, start, total, aligned, final):
    rows = grads.shape[0]
    width = grads.shape[1] // 2
    depth = weights[0].shape[0]
    by_depth = parts_of(depth, 128)

    def body(at, *refs):
        grads_ref, gate, up, *outs = refs
        *outs, both, sems = outs
        first = pl.multiple_of(at[0], 128) if aligned else 0
        _, depths = streams((gate, up, None), (both, None), sems, first, width, by_depth, [])
        for pair in depths:
            for copy in pair:
                copy.start()
        for i, (row, count) in enumerate(by_depth):
            for copy in depths[i]:
                copy.wait()
            some = pl.ds(row, count)
            value = across(grads_ref[...], both[some, :])
            if total is not None:
                value = value + outs[0][:, some]
            if final:
                outs[-2][:, some] = value[rows // 2:, :].astype(jnp.bfloat16)
                outs[-1][:, some] = value[:rows // 2, :]
            else:
                outs[-1][:, some] = value

    operands = [grads, *weights]
    specs = [VMEM, ANY, ANY]
    if total is not None:
        operands.append(total)
        specs.append(VMEM)
    if final:
        out_shape = (
            jax.ShapeDtypeStruct((rows // 2, depth), jnp.bfloat16),
            jax.ShapeDtypeStruct((rows // 2, depth), jnp.float32),
        )
        out_specs = (VMEM, VMEM)
    else:
        out_shape, out_specs = jax.ShapeDtypeStruct((rows, depth), jnp.float32), VMEM
    return pl.pallas_call(
        body,
        out_shape=out_shape,
        in_specs=[SMEM] + specs,
        out_specs=out_specs,
        scratch_shapes=[pltpu.VMEM((depth, 2 * width), jnp.bfloat16), pltpu.SemaphoreType.DMA((2, 4))],
        compiler_params=pltpu.CompilerParams(vmem_limit_bytes=12 * 1024 * 1024),
        cost_estimate=pl.CostEstimate(
            flops=4 * rows * width * depth, bytes_accessed=4 * width * depth, transcendentals=0
        ),
        name="backward",
    )(start, *operands)


def chunks_of(width):
    if width % 128 or width < 512:
        return [(0, rounded(width, 128))]
    first = rounded(width // 2, 256)
    return [(0, first), (first, width - first)]


def on_device(
    examples, references, gate_weight, up_weight, down_weight, cotangent, pair_ref, points
):
    dims = factors(lax.axis_size("wide"))
    far, near, pair = dims
    peers = lax.axis_size("narrow")
    e, r, k = examples.shape[0], references.shape[0], cotangent.shape[0]
    depth, hidden = gate_weight.shape
    blocks = far * near * pair

    at = lax.axis_index("wide")
    z, y, c = at // (near * pair), (at // pair) % near, at % pair
    n = lax.axis_index("narrow")

    order = jnp.asarray(
        [[s, b, q] for q in range(pair) for b in range(near) for s in range(far)], jnp.int32
    )
    owner = (
        ((z - order[:, 0]) % far * near + (y - order[:, 1]) % near) * pair + (c - order[:, 2]) % pair
    )
    chosen = jnp.take(pair_ref.reshape(blocks, -1), owner, axis=0).reshape(blocks * e, -1)
    host, inside = chosen // r, chosen % r
    back = (z - host // (near * pair)) % far
    beside = (y - host // pair % near) % near
    chosen = (((c - host % pair) % pair * near + beside) * far + back) * r + inside

    share = hidden // peers
    aligned = share % 128 == 0
    if aligned:
        gate_weight, up_weight, down_weight = (
            pltpu.with_memory_space_constraint(w, pltpu.MemorySpace.HBM)
            for w in (gate_weight, up_weight, down_weight)
        )

    def at_peer(m, offset, width):
        start = m * share + offset
        if aligned:
            return jnp.reshape(start, (1,)).astype(jnp.int32), (gate_weight, up_weight, down_weight)
        more = width - share

        def cut(weight, axis):
            piece = lax.dynamic_slice_in_dim(weight, start, share, axis)
            return jnp.pad(piece, [(0, more if d == axis else 0) for d in range(2)])

        return jnp.zeros((1,), jnp.int32), (
            cut(gate_weight, 1),
            cut(up_weight, 1),
            cut(down_weight, 0),
        )

    own, whole, pieces = pack([references, examples, cotangent])
    column = [own] + [shift_permute(own, "wide", dims, 0, s) for s in range(1, far)]
    plane = list(column)
    first_chunk = chunks_of(share)[0]
    ahead = aligned and peers == 2 and near > 1
    if ahead:
        start, weights = at_peer((n + 1) % peers, *first_chunk)
        column[1], start, chosen = lax.optimization_barrier((column[1], start, chosen))
        *fetched, ready = fetch(weights, start, first_chunk[1], aligned)
    for b in range(1, near):
        for s, block in enumerate(column):
            if ahead and s == far - 2:
                block, ready = lax.optimization_barrier((block, ready))
            plane.append(shift_permute(block, "wide", dims, 1, b))
    half = assemble(plane, whole, pieces, (r, e, k), depth)
    halves = [half] + [shift_permute(half, "wide", dims, 2, b) for b in range(1, pair)]
    main, side = join(halves, (r, e, k))

    parts = []
    for offset, width in chunks_of(share):
        received = []
        for s in range(1, peers):
            start, weights = at_peer((n + s) % peers, offset, width)
            if ahead and not parts:
                sent = forward(main, side, fetched, None, width, aligned, jnp.bfloat16, True)
            else:
                sent = forward(main, side, weights, start, width, aligned, jnp.bfloat16)
            received.append(shift_permute(sent, "narrow", (peers,), 0, s))
        parts.append((offset, width, received))

    jobs = []
    for offset, width, received in parts:
        start, weights = at_peer(n, offset, width)
        kept = forward(main, side, weights, start, width, aligned, jnp.float32)
        grads = coefficients(kept, received, chosen, points, blocks * e, blocks * r)
        jobs.append((grads, offset, width, 0))
        jobs += [
            (shift_permute(grads, "narrow", (peers,), 0, s), offset, width, s) for s in range(1, peers)
        ]
    jobs.sort(key=lambda job: job[3])
    total = None
    for i, (grads, offset, width, s) in enumerate(jobs):
        start, weights = at_peer((n - s) % peers, offset, width)
        total = backward(
            grads, weights[:2], start, total, aligned, i == len(jobs) - 1 and pair == 2
        )

    if pair == 2:
        sent, kept = total
        total = kept + shift_permute(sent, "wide", dims, 2, 1).astype(jnp.float32)
    if near == 2:
        half = total.shape[0] // 2
        sent = total[half:].astype(jnp.bfloat16)
        total = total[:half] + shift_permute(sent, "wide", dims, 1, 1).astype(jnp.float32)
    result = total[:e]
    got = [
        shift_permute(total[s * e:(s + 1) * e].astype(jnp.bfloat16), "wide", dims, 0, far - s)
        for s in range(1, far)
    ]
    for piece in got:
        result = result + piece.astype(jnp.float32)
    return result.astype(jnp.bfloat16)


def solution(mesh):
    in_specs = (
        P("wide", "narrow"),
        P("wide", "narrow"),
        P("narrow", "wide"),
        P("narrow", "wide"),
        P("wide", "narrow"),
        P("wide", "narrow"),
        P(),
        P(),
    )
    out_specs = P("wide", "narrow")
    return jax.shard_map(
        on_device, mesh=mesh, in_specs=in_specs, out_specs=out_specs, check_vma=False
    )
```

```python
import jax
import jax.numpy as jnp
from jax import lax
from jax.experimental import pallas as pl
from jax.experimental.pallas import tpu as pltpu
from jax.sharding import PartitionSpec as P


VMEM = pl.BlockSpec(memory_space=pltpu.VMEM)
SMEM = pl.BlockSpec(memory_space=pltpu.SMEM)
ANY = pl.BlockSpec(memory_space=pl.ANY)


def factors(size):
    pair = 2 if size % 2 == 0 else 1
    near = 2 if (size // pair) % 2 == 0 else 1
    return size // (pair * near), near, pair


def rounded(rows, unit):
    return -(-rows // unit) * unit


def shift_permute(array, axis, dims, digit, amount):
    below = 1
    for size in dims[digit + 1:]:
        below *= size
    size = dims[digit]
    total = below * size
    for d in dims[:digit]:
        total *= d
    pairs = []
    for at in range(total):
        own = (at // below) % size
        to = (own + amount) % size
        pairs.append((at, at + (to - own) * below))
    return lax.ppermute(array, axis, pairs)


def pack(arrays):
    rows = jnp.concatenate(arrays)
    count, width = rows.shape
    whole = count // 8 * 8
    rest = count - whole
    if rest == 0:
        return rows, whole, 1
    pieces = whole // rest if whole else 0
    if not pieces or whole % rest or width % (pieces * 128):
        return jnp.pad(rows, ((0, 8 - rest), (0, 0))), whole + 8, 1
    cut = rows[whole:].reshape(rest * pieces, width // pieces)
    return jnp.concatenate([rows[:whole], cut], axis=1), whole, pieces


def assemble(own, whole, pieces, counts, width):
    blocks = len(own)
    packed = own[0].shape
    total = blocks * sum(counts)
    across_lanes = width // pieces

    def body(*refs):
        out, stack = refs[-2], refs[-1]
        for b in range(blocks):
            stack[pl.ds(b * packed[0], packed[0]), :] = refs[b][...]
        row = lax.broadcasted_iota(jnp.int32, (total, blocks * packed[0]), 0)
        col = lax.broadcasted_iota(jnp.int32, (total, blocks * packed[0]), 1)
        held = jnp.zeros_like(row)
        block = jnp.zeros_like(row)
        at = first = 0
        for count in counts:
            for b in range(blocks):
                inside = (row >= at) & (row < at + count)
                held = jnp.where(inside, row - at + first, held)
                block = jnp.where(inside, b, block)
                at += count
            first += count

        def pick(wanted, valid):
            return (valid & (col == wanted)).astype(jnp.float32).astype(jnp.bfloat16)

        base = block * packed[0]
        uncut = pick(base + held, held < whole)
        for j in range(pieces):
            lanes = pl.ds(j * across_lanes, across_lanes)
            value = jnp.dot(uncut, stack[:, lanes], preferred_element_type=jnp.float32)
            if packed[1] > width:
                value = value + jnp.dot(
                    pick(base + (held - whole) * pieces + j, held >= whole),
                    stack[:, pl.ds(width, across_lanes)],
                    preferred_element_type=jnp.float32,
                )
            out[:, lanes] = value.astype(jnp.bfloat16)

    dtype = own[0].dtype
    return pl.pallas_call(
        body,
        out_shape=jax.ShapeDtypeStruct((total, width), dtype),
        in_specs=[VMEM] * blocks,
        out_specs=VMEM,
        scratch_shapes=[pltpu.VMEM((blocks * packed[0], packed[1]), dtype)],
        compiler_params=pltpu.CompilerParams(vmem_limit_bytes=6 * 1024 * 1024),
        cost_estimate=pl.CostEstimate(flops=10**9, bytes_accessed=10**6, transcendentals=0),
        name="assemble",
    )(*own)


def join(halves, layout):
    width = halves[0].shape[1]
    blocks = halves[0].shape[0] // sum(layout)
    e, r, k = (blocks * rows for rows in layout)
    count = len(halves)

    def body(*refs):
        main, side = refs[-2:]
        for h in range(count):
            main[pl.ds(h * e, e), :] = refs[h][pl.ds(0, e), :]
            main[pl.ds(count * e + h * r, r), :] = refs[h][pl.ds(e, r), :]
            side[pl.ds(h * k, k), :] = refs[h][pl.ds(e + r, k), :]

    dtype = halves[0].dtype
    return pl.pallas_call(
        body,
        out_shape=(
            jax.ShapeDtypeStruct((count * (e + r), width), dtype),
            jax.ShapeDtypeStruct((count * k, width), dtype),
        ),
        in_specs=[VMEM] * count,
        out_specs=(VMEM, VMEM),
        compiler_params=pltpu.CompilerParams(vmem_limit_bytes=4 * 1024 * 1024),
        cost_estimate=pl.CostEstimate(flops=10**9, bytes_accessed=10**6, transcendentals=0),
        name="join",
    )(*halves)


def across(left, right):
    return lax.dot_general(left, right, (((1,), (1,)), ((), ())), preferred_element_type=jnp.float32)


def parts_of(size, unit):
    for count in (4, 2):
        if size % (count * unit) == 0:
            return [(i * (size // count), size // count) for i in range(count)]
    return [(0, size)]


def first_of(place):
    if place is None:
        return 0
    steps, peers, share, offset = place
    return pl.multiple_of((lax.axis_index("narrow") + steps) % peers * share + offset, 128)


def streams(weights, buffers, sems, first, width, by_depth, by_unit):
    gate, up, down = weights
    both, below = buffers
    units, depths = [], []
    for i, (row, count) in enumerate(by_unit):
        units.append(
            pltpu.make_async_copy(
                down.at[pl.ds(first + row, count)], below.at[pl.ds(row, count)], sems.at[2, i]
            )
        )
    for i, (row, count) in enumerate(by_depth):
        some = pl.ds(row, count)
        depths.append(
            [
                pltpu.make_async_copy(
                    source.at[some, pl.ds(first, width)],
                    both.at[some, pl.ds(w * width, width)],
                    sems.at[w, i],
                )
                for w, source in enumerate((gate, up))
            ]
        )
    return units, depths


def fetch(weights, place, width):
    depth = weights[0].shape[0]
    by_depth, by_unit = parts_of(depth, 128), parts_of(width, 32)

    def body(gate, up, down, both, below, sems):
        first = first_of(place)
        units, depths = streams((gate, up, down), (both, below), sems, first, width, by_depth, by_unit)
        copies = units + [copy for pair in depths for copy in pair]
        for copy in copies:
            copy.start()
        for copy in copies:
            copy.wait()

    return pl.pallas_call(
        body,
        out_shape=(
            pltpu.VMEM((depth, 2 * width), jnp.bfloat16),
            pltpu.VMEM((width, depth), jnp.bfloat16),
        ),
        in_specs=[ANY, ANY, ANY],
        out_specs=(VMEM, VMEM),
        scratch_shapes=[pltpu.SemaphoreType.DMA((3, 4))],
        compiler_params=pltpu.CompilerParams(vmem_limit_bytes=1024 * 1024),
        cost_estimate=pl.CostEstimate(
            flops=4 * 10**9, bytes_accessed=6 * depth * width, transcendentals=0
        ),
        name="fetch",
    )(*weights)


def forward(main, side, weights, place, width, dtype, next_one=None):
    rows, half = main.shape[0], side.shape[0] // 2
    depth = main.shape[1]
    by_depth, by_unit = parts_of(depth, 128), parts_of(width, 32)
    ready = len(weights) == 2

    def put_side(out, value):
        out[pl.ds(rows, half), pl.ds(0, width)] = value[:half].astype(dtype)
        out[pl.ds(rows, half), pl.ds(width, width)] = value[half:].astype(dtype)

    def body_ready(main_ref, side_ref, both, below, *refs):
        copies = []
        if next_one is not None:
            *refs, next_both, next_below, sems = refs
            *more, out = refs
            units, depths = streams(
                more, (next_both, next_below), sems, first_of(next_one[1]), next_one[2],
                parts_of(depth, 128), parts_of(next_one[2], 32),
            )
            copies = units + [copy for pair in depths for copy in pair]
        else:
            (out,) = refs
        for copy in copies:
            copy.start()
        out[pl.ds(0, rows), :] = jnp.dot(
            main_ref[...], both[...], preferred_element_type=jnp.float32
        ).astype(dtype)
        put_side(out, across(side_ref[...], below[...]))
        for copy in copies:
            copy.wait()

    def body(main_ref, side_ref, gate, up, down, out, both, below, total, sems):
        first = first_of(place)
        units, depths = streams((gate, up, down), (both, below), sems, first, width, by_depth, by_unit)
        for copy in units + [copy for pair in depths for copy in pair]:
            copy.start()
        for copy in units:
            copy.wait()
        put_side(out, across(side_ref[...], below[...]))
        for i, (row, count) in enumerate(by_depth):
            for copy in depths[i]:
                copy.wait()
            some = pl.ds(row, count)
            part = jnp.dot(main_ref[:, some], both[some, :], preferred_element_type=jnp.float32)
            if i > 0:
                part = total[...] + part
            if i == len(by_depth) - 1:
                out[pl.ds(0, rows), :] = part.astype(dtype)
            else:
                total[...] = part

    out_shape = [jax.ShapeDtypeStruct((rows + half, 2 * width), dtype)]
    operands = [main, side, *weights]
    specs = [VMEM] * 2 + [VMEM if ready else ANY] * len(weights)
    if ready:
        scratch = []
        if next_one is not None:
            operands += next_one[0]
            specs += [ANY] * 3
            out_shape += [
                pltpu.VMEM((depth, 2 * next_one[2]), jnp.bfloat16),
                pltpu.VMEM((next_one[2], depth), jnp.bfloat16),
            ]
            scratch = [pltpu.SemaphoreType.DMA((3, 4))]
    else:
        scratch = [
            pltpu.VMEM((depth, 2 * width), jnp.bfloat16),
            pltpu.VMEM((width, depth), jnp.bfloat16),
            pltpu.VMEM((rows, 2 * width), jnp.float32),
            pltpu.SemaphoreType.DMA((3, 4)),
        ]
    return pl.pallas_call(
        body_ready if ready else body,
        out_shape=out_shape,
        in_specs=specs,
        out_specs=[VMEM] * len(out_shape),
        scratch_shapes=scratch,
        compiler_params=pltpu.CompilerParams(vmem_limit_bytes=(4 if ready else 20) * 1024 * 1024),
        cost_estimate=pl.CostEstimate(
            flops=4 * depth * width * (rows + half), bytes_accessed=6 * depth * width, transcendentals=0
        ),
        name="forward",
    )(*operands)


def coefficients(kept, received, picks, points, examples):
    width = kept.shape[1] // 2
    pairs, references = picks.shape[0] // examples, picks.shape[1]
    rows = examples + references
    count = points.shape[0]
    lanes = 128 if width % 128 == 0 else width
    piece = 16 if examples % 32 == 16 else examples // 2
    scale = 1.0 / (pairs * count)

    def body(points_ref, picks_ref, kept_ref, *refs):
        got, out, base_gate, base_up = refs[:-3], refs[-3], refs[-2], refs[-1]
        picks = picks_ref[...]
        steps = [points_ref[m].astype(jnp.float32) * 0.125 for m in range(count)]

        def block(j, _):
            if lanes == width:
                of = [pl.ds(w * width, width) for w in range(2)]
            else:
                of = [pl.ds(pl.multiple_of(w * width + j * lanes, 128), lanes) for w in range(2)]

            def total(start, size, w):
                value = kept_ref[pl.ds(start, size), of[w]]
                for ref in got:
                    value = value + ref[pl.ds(start, size), of[w]].astype(jnp.float32)
                return value

            for w, target in enumerate((base_gate, base_up)):
                value = total(0, references, w)
                high = value.astype(jnp.bfloat16)
                low = (value - high.astype(jnp.float32)).astype(jnp.bfloat16)
                target[...] = jnp.dot(picks, high, preferred_element_type=jnp.float32) + jnp.dot(
                    picks, low, preferred_element_type=jnp.float32
                )
            upstream = [total(rows, examples // 2, w) for w in range(2)]
            for first in range(0, examples, piece):
                gate = total(references + first, piece, 0) * 0.5
                up = total(references + first, piece, 1)
                coef_gate = jnp.zeros_like(gate)
                coef_up = jnp.zeros_like(gate)
                for p in range(pairs):
                    start = base_gate[pl.ds(p * examples + first, piece), :] * 0.5
                    span = gate - start
                    flat = jnp.zeros_like(gate)
                    tilted = jnp.zeros_like(gate)
                    for t in steps:
                        half = start + t * span
                        two_s = 1.0 + jnp.tanh(half)
                        silu = half * two_s
                        slope = two_s + silu * (2.0 - two_s)
                        coef_up = coef_up + silu
                        flat = flat + slope
                        tilted = tilted + t * slope
                    start_up = base_up[pl.ds(p * examples + first, piece), :]
                    coef_gate = coef_gate + (start_up * flat + (up - start_up) * tilted)
                base_gate[pl.ds(first, piece), :] = coef_gate * (0.5 * scale)
                base_up[pl.ds(first, piece), :] = coef_up * scale
            for w, source in enumerate((base_gate, base_up)):
                for h in range(2):
                    some = pl.ds(h * (examples // 2), examples // 2)
                    out[some, of[w]] = (upstream[h] * source[some, :]).astype(jnp.bfloat16)
            return 0

        lax.fori_loop(0, width // lanes, block, 0)

    return pl.pallas_call(
        body,
        out_shape=jax.ShapeDtypeStruct((examples, 2 * width), jnp.bfloat16),
        in_specs=[SMEM, VMEM, VMEM] + [VMEM] * len(received),
        out_specs=VMEM,
        scratch_shapes=[pltpu.VMEM((pairs * examples, lanes), jnp.float32)] * 2,
        compiler_params=pltpu.CompilerParams(vmem_limit_bytes=4 * 1024 * 1024),
        cost_estimate=pl.CostEstimate(flops=5 * 10**9, bytes_accessed=10**6, transcendentals=0),
        name="coefficients",
    )(points, picks, kept, *received)


def backward(grads, weights, place, total, final):
    rows = grads.shape[0]
    width = grads.shape[1] // 2
    depth = weights[0].shape[0]
    by_depth = parts_of(depth, 128)
    ready = len(weights) == 1

    def body(grads_ref, *refs):
        if ready:
            both, *outs = refs
        else:
            gate, up, *outs, both, sems = refs
            _, depths = streams((gate, up, None), (both, None), sems, first_of(place), width, by_depth, [])
            for pair in depths:
                for copy in pair:
                    copy.start()
        for i, (row, count) in enumerate(by_depth):
            some = pl.ds(row, count)
            if not ready:
                for copy in depths[i]:
                    copy.wait()
            value = across(grads_ref[...], both[some, :])
            if total is not None:
                value = value + outs[0][:, some]
            if final:
                outs[-2][:, some] = value[rows // 2:, :].astype(jnp.bfloat16)
                outs[-1][:, some] = value[:rows // 2, :]
            else:
                outs[-1][:, some] = value

    operands = [grads, *weights]
    specs = [VMEM] + [VMEM if ready else ANY] * len(weights)
    if total is not None:
        operands.append(total)
        specs.append(VMEM)
    if final:
        out_shape = (
            jax.ShapeDtypeStruct((rows // 2, depth), jnp.bfloat16),
            jax.ShapeDtypeStruct((rows // 2, depth), jnp.float32),
        )
        out_specs = (VMEM, VMEM)
    else:
        out_shape, out_specs = jax.ShapeDtypeStruct((rows, depth), jnp.float32), VMEM
    scratch = [pltpu.VMEM((depth, 2 * width), jnp.bfloat16), pltpu.SemaphoreType.DMA((2, 4))]
    return pl.pallas_call(
        body,
        out_shape=out_shape,
        in_specs=specs,
        out_specs=out_specs,
        scratch_shapes=[] if ready else scratch,
        compiler_params=pltpu.CompilerParams(vmem_limit_bytes=(4 if ready else 12) * 1024 * 1024),
        cost_estimate=pl.CostEstimate(
            flops=4 * rows * width * depth, bytes_accessed=4 * width * depth, transcendentals=0
        ),
        name="backward",
    )(*operands)


def choices(pair_ref, dims, e, r):
    far, near, pair = dims
    blocks = far * near * pair
    examples, pairs = pair_ref.shape

    def body(pair_ref, out, rows):
        at = lax.axis_index("wide")
        z, y, c = at // (near * pair), at // pair % near, at % pair
        col = lax.broadcasted_iota(jnp.int32, (examples, blocks * r), 1)
        name = jnp.zeros_like(col)
        for q in range(blocks):
            s, b, p = q % far, q // far % near, q // (far * near)
            owner = ((z + far - s) % far * near + (y + near - b) % near) * pair + (c + pair - p) % pair
            rows[pl.ds(q * e, e), :] = pair_ref[pl.ds(owner * e, e), :]
            name = jnp.where((col >= q * r) & (col < (q + 1) * r), owner * r + col - q * r, name)
        for p in range(pairs):
            out[pl.ds(p * examples, examples), :] = (
                (rows[:, pl.ds(p, 1)] == name).astype(jnp.float32).astype(jnp.bfloat16)
            )

    return pl.pallas_call(
        body,
        out_shape=jax.ShapeDtypeStruct((pairs * examples, blocks * r), jnp.bfloat16),
        in_specs=[VMEM],
        out_specs=VMEM,
        scratch_shapes=[pltpu.VMEM((examples, pairs), jnp.int32)],
        compiler_params=pltpu.CompilerParams(vmem_limit_bytes=2 * 1024 * 1024),
        cost_estimate=pl.CostEstimate(flops=10**9, bytes_accessed=10**6, transcendentals=0),
        name="choices",
    )(pair_ref)


def chunks_of(width):
    if width % 128 or width < 512:
        return [(0, rounded(width, 128))]
    first = rounded(width // 2, 256)
    return [(0, first), (first, width - first)]


def on_device(
    examples, references, gate_weight, up_weight, down_weight, cotangent, pair_ref, points
):
    dims = factors(lax.axis_size("wide"))
    far, near, pair = dims
    peers = lax.axis_size("narrow")
    e, r, k = examples.shape[0], references.shape[0], cotangent.shape[0]
    depth, hidden = gate_weight.shape
    blocks = far * near * pair

    share = hidden // peers
    whole_weights = [gate_weight, up_weight, down_weight]
    aligned = share % 128 == 0
    ahead = aligned and peers == 2
    if aligned:
        whole_weights = [
            pltpu.with_memory_space_constraint(w, pltpu.MemorySpace.HBM) for w in whole_weights
        ]
    chunks = chunks_of(share)
    picks = choices(pair_ref, dims, e, r)

    def at_peer(steps, offset, width):
        if aligned:
            return whole_weights, (steps % peers, peers, share, offset)
        start = (lax.axis_index("narrow") + steps) % peers * share
        more = width - share

        def cut(weight, axis):
            piece = lax.dynamic_slice_in_dim(weight, start, share, axis)
            return jnp.pad(piece, [(0, more if d == axis else 0) for d in range(2)])

        return [cut(gate_weight, 1), cut(up_weight, 1), cut(down_weight, 0)], None

    own, whole, pieces = pack([references, examples, cotangent])
    column = [own]
    for s in range(1, far):
        column.append(shift_permute(own, "wide", dims, 0, s))
    plane = list(column)
    for b in range(1, near):
        for block in column:
            plane.append(shift_permute(block, "wide", dims, 1, b))
    half = assemble(plane, whole, pieces, (r, e, k), depth)
    halves = [half] + [shift_permute(half, "wide", dims, 2, b) for b in range(1, pair)]
    main, side = join(halves, (r, e, k))

    blocks_of_weights = {}
    later = None
    if ahead:
        wanted = [(s, chunk) for s in (1, 0) for chunk in chunks]
        for s, chunk in wanted:
            if len(chunks) == 2 and (s, chunk) == (0, chunks[0]):
                later = (s, chunk)
                continue
            blocks_of_weights[s, chunk[0]] = fetch(*at_peer(s, *chunk), chunk[1])

    parts = []
    for i, (offset, width) in enumerate(chunks):
        received = []
        for s in range(1, peers):
            weights, place = at_peer(s, offset, width)
            next_one = None
            if ahead:
                weights = blocks_of_weights[s, offset]
                if later is not None and i == 1:
                    next_one = (*at_peer(later[0], *later[1]), later[1][1])
            sent, *more = forward(main, side, weights, place, width, jnp.bfloat16, next_one)
            if more:
                blocks_of_weights[later[0], later[1][0]] = more
            received.append(shift_permute(sent, "narrow", (peers,), 0, s))
        parts.append((offset, width, received))

    jobs = []
    for offset, width, received in parts:
        weights, place = at_peer(0, offset, width)
        if ahead:
            weights = blocks_of_weights[0, offset]
        (kept,) = forward(main, side, weights, place, width, jnp.float32)
        grads = coefficients(kept, received, picks, points, blocks * e)
        jobs.append((grads, offset, width, 0))
        jobs += [
            (shift_permute(grads, "narrow", (peers,), 0, s), offset, width, s) for s in range(1, peers)
        ]
    jobs.sort(key=lambda job: job[3])
    total = None
    for i, (grads, offset, width, s) in enumerate(jobs):
        weights, place = at_peer(peers - s, offset, width)
        weights = blocks_of_weights[s, offset][:1] if ahead else weights[:2]
        total = backward(grads, weights, place, total, i == len(jobs) - 1 and pair == 2)

    if pair == 2:
        sent, kept = total
        total = kept + shift_permute(sent, "wide", dims, 2, 1).astype(jnp.float32)
    if near == 2:
        half = total.shape[0] // 2
        sent = total[half:].astype(jnp.bfloat16)
        total = total[:half] + shift_permute(sent, "wide", dims, 1, 1).astype(jnp.float32)
    result = total[:e]
    got = [
        shift_permute(total[s * e:(s + 1) * e].astype(jnp.bfloat16), "wide", dims, 0, far - s)
        for s in range(1, far)
    ]
    for piece in got:
        result = result + piece.astype(jnp.float32)
    return result.astype(jnp.bfloat16)


def solution(mesh):
    in_specs = (
        P("wide", "narrow"),
        P("wide", "narrow"),
        P("narrow", "wide"),
        P("narrow", "wide"),
        P("wide", "narrow"),
        P("wide", "narrow"),
        P(),
        P(),
    )
    out_specs = P("wide", "narrow")
    return jax.shard_map(on_device, mesh=mesh, in_specs=in_specs, out_specs=out_specs, check_vma=False)
```

```python
import jax
import jax.numpy as jnp
from jax import lax
from jax.experimental import pallas as pl
from jax.experimental.pallas import tpu as pltpu
from jax.sharding import PartitionSpec as P


VMEM = pl.BlockSpec(memory_space=pltpu.VMEM)
SMEM = pl.BlockSpec(memory_space=pltpu.SMEM)
ANY = pl.BlockSpec(memory_space=pl.ANY)


def factors(size):
    pair = 2 if size % 2 == 0 else 1
    near = 2 if (size // pair) % 2 == 0 else 1
    return size // (pair * near), near, pair


def rounded(rows, unit):
    return -(-rows // unit) * unit


def permute(array, axis, dims, digit, amount):
    below = 1
    for size in dims[digit + 1:]:
        below *= size
    total = below
    for size in dims[:digit + 1]:
        total *= size
    pairs = [
        (at, at + (((at // below) % dims[digit] ^ amount) - (at // below) % dims[digit]) * below)
        for at in range(total)
    ]
    return lax.ppermute(array, axis, pairs)


def shift(array, size, amount):
    return lax.ppermute(array, "narrow", [(at, (at + amount) % size) for at in range(size)])


def halvings(size):
    if size == 1:
        return [0]
    return [2 * v for v in halvings(size // 2)] + [2 * v + 1 for v in halvings(size // 2)]


def pack(arrays):
    count, width = sum(a.shape[0] for a in arrays), arrays[0].shape[1]
    whole = count // 8 * 8
    rest = count - whole
    pieces = whole // rest if rest and whole else 1
    cut = rest > 0 and whole > 0 and whole % rest == 0 and width % (pieces * 128) == 0
    if not cut:
        whole, pieces = rounded(count, 8), 1
    lanes = width // pieces

    def body(*refs):
        sources, (out, *held, sems) = refs[:len(arrays)], refs[len(arrays):]
        copies = [
            pltpu.make_async_copy(source, target, sems.at[i])
            for i, (source, target) in enumerate(zip(sources, held))
        ]
        for copy in copies:
            copy.start()
        for copy in copies:
            copy.wait()
        rows = jnp.concatenate([ref[...].astype(jnp.float32) for ref in held])
        if not cut:
            if whole > count:
                rows = jnp.concatenate([rows, jnp.zeros((whole - count, width), jnp.float32)])
            out[...] = rows.astype(out.dtype)
            return
        out[:, pl.ds(0, width)] = rows[:whole].astype(out.dtype)
        beside = [
            rows[whole + i:whole + i + 1, j * lanes:(j + 1) * lanes]
            for i in range(rest)
            for j in range(pieces)
        ]
        out[:, pl.ds(width, lanes)] = jnp.concatenate(beside).astype(out.dtype)

    packed = pl.pallas_call(
        body,
        out_shape=jax.ShapeDtypeStruct((whole, width + lanes if cut else width), arrays[0].dtype),
        in_specs=[ANY] * len(arrays),
        out_specs=VMEM,
        scratch_shapes=[pltpu.VMEM(a.shape, a.dtype) for a in arrays]
        + [pltpu.SemaphoreType.DMA((len(arrays),))],
        compiler_params=pltpu.CompilerParams(vmem_limit_bytes=4 * 1024 * 1024),
        name="pack",
    )(*(pltpu.with_memory_space_constraint(a, pltpu.MemorySpace.HBM) for a in arrays))
    return packed, whole, pieces


def assemble(own, whole, pieces, counts, width):
    blocks = len(own)
    packed = own[0].shape
    total = blocks * sum(counts)
    across_lanes = width // pieces

    def body(*refs):
        out, stack = refs[-2], refs[-1]
        for b in range(blocks):
            stack[pl.ds(b * packed[0], packed[0]), :] = refs[b][...]
        row = lax.broadcasted_iota(jnp.int32, (total, blocks * packed[0]), 0)
        col = lax.broadcasted_iota(jnp.int32, (total, blocks * packed[0]), 1)
        held = jnp.zeros_like(row)
        block = jnp.zeros_like(row)
        at = first = 0
        for count in counts:
            for b in range(blocks):
                inside = (row >= at) & (row < at + count)
                held = jnp.where(inside, row - at + first, held)
                block = jnp.where(inside, b, block)
                at += count
            first += count

        def pick(wanted, valid):
            return (valid & (col == wanted)).astype(jnp.float32).astype(jnp.bfloat16)

        base = block * packed[0]
        uncut = pick(base + held, held < whole)
        for j in range(pieces):
            lanes = pl.ds(j * across_lanes, across_lanes)
            value = jnp.dot(uncut, stack[:, lanes], preferred_element_type=jnp.float32)
            if packed[1] > width:
                value = value + jnp.dot(
                    pick(base + (held - whole) * pieces + j, held >= whole),
                    stack[:, pl.ds(width, across_lanes)],
                    preferred_element_type=jnp.float32,
                )
            out[:, lanes] = value.astype(jnp.bfloat16)

    dtype = own[0].dtype
    return pl.pallas_call(
        body,
        out_shape=jax.ShapeDtypeStruct((total, width), dtype),
        in_specs=[VMEM] * blocks,
        out_specs=VMEM,
        scratch_shapes=[pltpu.VMEM((blocks * packed[0], packed[1]), dtype)],
        compiler_params=pltpu.CompilerParams(vmem_limit_bytes=6 * 1024 * 1024),
        cost_estimate=pl.CostEstimate(flops=10**9, bytes_accessed=10**6, transcendentals=0),
        name="assemble",
    )(*own)


def join(halves, layout):
    width = halves[0].shape[1]
    blocks = halves[0].shape[0] // sum(layout)
    e, r, k = (blocks * rows for rows in layout)
    count = len(halves)

    def body(*refs):
        main, side = refs[-2:]
        for h in range(count):
            main[pl.ds(h * e, e), :] = refs[h][pl.ds(0, e), :]
            main[pl.ds(count * e + h * r, r), :] = refs[h][pl.ds(e, r), :]
            side[pl.ds(h * k, k), :] = refs[h][pl.ds(e + r, k), :]

    dtype = halves[0].dtype
    return pl.pallas_call(
        body,
        out_shape=(
            jax.ShapeDtypeStruct((count * (e + r), width), dtype),
            jax.ShapeDtypeStruct((count * k, width), dtype),
        ),
        in_specs=[VMEM] * count,
        out_specs=(VMEM, VMEM),
        compiler_params=pltpu.CompilerParams(vmem_limit_bytes=4 * 1024 * 1024),
        cost_estimate=pl.CostEstimate(flops=10**9, bytes_accessed=10**6, transcendentals=0),
        name="join",
    )(*halves)


def across(left, right):
    return lax.dot_general(left, right, (((1,), (1,)), ((), ())), preferred_element_type=jnp.float32)


def parts_of(size, unit):
    for count in (4, 2):
        if size % (count * unit) == 0:
            return [(i * (size // count), size // count) for i in range(count)]
    return [(0, size)]


def first_of(place):
    if place is None:
        return 0
    steps, peers, share, offset = place
    return pl.multiple_of((lax.axis_index("narrow") + steps) % peers * share + offset, 128)


def streams(weights, buffers, sems, first, width, by_depth, by_unit):
    gate, up, down = weights
    both, below = buffers
    units, depths = [], []
    for i, (row, count) in enumerate(by_unit):
        units.append(
            pltpu.make_async_copy(
                down.at[pl.ds(first + row, count)], below.at[pl.ds(row, count)], sems.at[2, i]
            )
        )
    for i, (row, count) in enumerate(by_depth):
        some = pl.ds(row, count)
        depths.append(
            [
                pltpu.make_async_copy(
                    source.at[some, pl.ds(first, width)],
                    both.at[some, pl.ds(w * width, width)],
                    sems.at[w, i],
                )
                for w, source in enumerate((gate, up))
            ]
        )
    return units, depths


def fetch(weights, place, width):
    depth = weights[0].shape[0]
    by_depth, by_unit = parts_of(depth, 128), parts_of(width, 32)

    def body(gate, up, down, both, below, sems):
        first = first_of(place)
        units, depths = streams((gate, up, down), (both, below), sems, first, width, by_depth, by_unit)
        copies = units + [copy for pair in depths for copy in pair]
        for copy in copies:
            copy.start()
        for copy in copies:
            copy.wait()

    return pl.pallas_call(
        body,
        out_shape=(
            pltpu.VMEM((depth, 2 * width), jnp.bfloat16),
            pltpu.VMEM((width, depth), jnp.bfloat16),
        ),
        in_specs=[ANY, ANY, ANY],
        out_specs=(VMEM, VMEM),
        scratch_shapes=[pltpu.SemaphoreType.DMA((3, 4))],
        compiler_params=pltpu.CompilerParams(vmem_limit_bytes=1024 * 1024),
        cost_estimate=pl.CostEstimate(
            flops=4 * 10**9, bytes_accessed=6 * depth * width, transcendentals=0
        ),
        name="fetch",
    )(*weights)


def forward(main, side, weights, place, width, dtype, next_one=None):
    rows, half = main.shape[0], side.shape[0] // 2
    depth = main.shape[1]
    by_depth, by_unit = parts_of(depth, 128), parts_of(width, 32)
    ready = len(weights) == 2

    def put_side(out, value):
        out[pl.ds(rows, half), pl.ds(0, width)] = value[:half].astype(dtype)
        out[pl.ds(rows, half), pl.ds(width, width)] = value[half:].astype(dtype)

    def body_ready(main_ref, side_ref, both, below, *refs):
        copies = []
        if next_one is not None:
            *refs, next_both, next_below, sems = refs
            *more, out = refs
            units, depths = streams(
                more, (next_both, next_below), sems, first_of(next_one[1]), next_one[2],
                parts_of(depth, 128), parts_of(next_one[2], 32),
            )
            copies = units + [copy for pair in depths for copy in pair]
        else:
            (out,) = refs
        for copy in copies:
            copy.start()
        out[pl.ds(0, rows), :] = jnp.dot(
            main_ref[...], both[...], preferred_element_type=jnp.float32
        ).astype(dtype)
        put_side(out, across(side_ref[...], below[...]))
        for copy in copies:
            copy.wait()

    def body(main_ref, side_ref, gate, up, down, out, both, below, total, sems):
        first = first_of(place)
        units, depths = streams((gate, up, down), (both, below), sems, first, width, by_depth, by_unit)
        for copy in units + [copy for pair in depths for copy in pair]:
            copy.start()
        for copy in units:
            copy.wait()
        put_side(out, across(side_ref[...], below[...]))
        for i, (row, count) in enumerate(by_depth):
            for copy in depths[i]:
                copy.wait()
            some = pl.ds(row, count)
            part = jnp.dot(main_ref[:, some], both[some, :], preferred_element_type=jnp.float32)
            if i > 0:
                part = total[...] + part
            if i == len(by_depth) - 1:
                out[pl.ds(0, rows), :] = part.astype(dtype)
            else:
                total[...] = part

    out_shape = [jax.ShapeDtypeStruct((rows + half, 2 * width), dtype)]
    operands = [main, side, *weights]
    specs = [VMEM] * 2 + [VMEM if ready else ANY] * len(weights)
    if ready:
        scratch = []
        if next_one is not None:
            operands += next_one[0]
            specs += [ANY] * 3
            out_shape += [
                pltpu.VMEM((depth, 2 * next_one[2]), jnp.bfloat16),
                pltpu.VMEM((next_one[2], depth), jnp.bfloat16),
            ]
            scratch = [pltpu.SemaphoreType.DMA((3, 4))]
    else:
        scratch = [
            pltpu.VMEM((depth, 2 * width), jnp.bfloat16),
            pltpu.VMEM((width, depth), jnp.bfloat16),
            pltpu.VMEM((rows, 2 * width), jnp.float32),
            pltpu.SemaphoreType.DMA((3, 4)),
        ]
    return pl.pallas_call(
        body_ready if ready else body,
        out_shape=out_shape,
        in_specs=specs,
        out_specs=[VMEM] * len(out_shape),
        scratch_shapes=scratch,
        compiler_params=pltpu.CompilerParams(vmem_limit_bytes=(4 if ready else 20) * 1024 * 1024),
        cost_estimate=pl.CostEstimate(
            flops=4 * depth * width * (rows + half), bytes_accessed=6 * depth * width, transcendentals=0
        ),
        name="forward",
    )(*operands)


def coefficients(kept, received, picks, points, examples):
    width = kept.shape[1] // 2
    pairs, references = picks.shape[0] // examples, picks.shape[1]
    rows = examples + references
    count = points.shape[0]
    lanes = 128 if width % 128 == 0 else width
    piece = 16 if examples % 32 == 16 else examples // 2
    scale = 1.0 / (pairs * count)

    def body(points_ref, picks_ref, kept_ref, *refs):
        got, out, base_gate, base_up = refs[:-3], refs[-3], refs[-2], refs[-1]
        picks = picks_ref[...]
        steps = [points_ref[m].astype(jnp.float32) * 0.125 for m in range(count)]

        def block(j, _):
            if lanes == width:
                of = [pl.ds(w * width, width) for w in range(2)]
            else:
                of = [pl.ds(pl.multiple_of(w * width + j * lanes, 128), lanes) for w in range(2)]

            def total(start, size, w):
                value = kept_ref[pl.ds(start, size), of[w]]
                for ref in got:
                    value = value + ref[pl.ds(start, size), of[w]].astype(jnp.float32)
                return value

            for w, target in enumerate((base_gate, base_up)):
                value = total(0, references, w)
                high = value.astype(jnp.bfloat16)
                low = (value - high.astype(jnp.float32)).astype(jnp.bfloat16)
                target[...] = jnp.dot(picks, high, preferred_element_type=jnp.float32) + jnp.dot(
                    picks, low, preferred_element_type=jnp.float32
                )
            upstream = [total(rows, examples // 2, w) for w in range(2)]
            for first in range(0, examples, piece):
                gate = total(references + first, piece, 0) * 0.5
                up = total(references + first, piece, 1)
                coef_gate = jnp.zeros_like(gate)
                coef_up = jnp.zeros_like(gate)
                for p in range(pairs):
                    start = base_gate[pl.ds(p * examples + first, piece), :] * 0.5
                    span = gate - start
                    flat = jnp.zeros_like(gate)
                    tilted = jnp.zeros_like(gate)
                    for t in steps:
                        half = start + t * span
                        two_s = 1.0 + jnp.tanh(half)
                        silu = half * two_s
                        slope = two_s + silu * (2.0 - two_s)
                        coef_up = coef_up + silu
                        flat = flat + slope
                        tilted = tilted + t * slope
                    start_up = base_up[pl.ds(p * examples + first, piece), :]
                    coef_gate = coef_gate + (start_up * flat + (up - start_up) * tilted)
                base_gate[pl.ds(first, piece), :] = coef_gate * (0.5 * scale)
                base_up[pl.ds(first, piece), :] = coef_up * scale
            for w, source in enumerate((base_gate, base_up)):
                for h in range(2):
                    some = pl.ds(h * (examples // 2), examples // 2)
                    out[some, of[w]] = (upstream[h] * source[some, :]).astype(jnp.bfloat16)
            return 0

        lax.fori_loop(0, width // lanes, block, 0)

    return pl.pallas_call(
        body,
        out_shape=jax.ShapeDtypeStruct((examples, 2 * width), jnp.bfloat16),
        in_specs=[SMEM, VMEM, VMEM] + [VMEM] * len(received),
        out_specs=VMEM,
        scratch_shapes=[pltpu.VMEM((pairs * examples, lanes), jnp.float32)] * 2,
        compiler_params=pltpu.CompilerParams(vmem_limit_bytes=4 * 1024 * 1024),
        cost_estimate=pl.CostEstimate(flops=5 * 10**9, bytes_accessed=10**6, transcendentals=0),
        name="coefficients",
    )(points, picks, kept, *received)


def backward(grads, weights, place, total, final, span=None):
    rows = grads.shape[0]
    width = grads.shape[1] // 2
    depth = weights[0].shape[0]
    low, columns = span or (0, depth)
    by_depth = [(low + row, count) for row, count in parts_of(columns, 128)]
    ready = len(weights) == 1

    def body(grads_ref, *refs):
        if ready:
            both, *outs = refs
        else:
            gate, up, *outs, both, sems = refs
            _, depths = streams((gate, up, None), (both, None), sems, first_of(place), width, by_depth, [])
            for pair in depths:
                for copy in pair:
                    copy.start()
        for i, (row, count) in enumerate(by_depth):
            some, own = pl.ds(row, count), pl.ds(row - low, count)
            if not ready:
                for copy in depths[i]:
                    copy.wait()
            value = across(grads_ref[...], both[some, :])
            if total is not None:
                value = value + outs[0][:, some]
            if final:
                outs[-2][:, own] = value[rows // 2:, :].astype(jnp.bfloat16)
                outs[-1][:, own] = value[:rows // 2, :]
            else:
                outs[-1][:, own] = value

    operands = [grads, *weights]
    specs = [VMEM] + [VMEM if ready else ANY] * len(weights)
    if total is not None:
        operands.append(total)
        specs.append(VMEM)
    if final:
        out_shape = (
            jax.ShapeDtypeStruct((rows // 2, columns), jnp.bfloat16),
            jax.ShapeDtypeStruct((rows // 2, columns), jnp.float32),
        )
        out_specs = (VMEM, VMEM)
    else:
        out_shape, out_specs = jax.ShapeDtypeStruct((rows, columns), jnp.float32), VMEM
    scratch = [pltpu.VMEM((depth, 2 * width), jnp.bfloat16), pltpu.SemaphoreType.DMA((2, 4))]
    return pl.pallas_call(
        body,
        out_shape=out_shape,
        in_specs=specs,
        out_specs=out_specs,
        scratch_shapes=[] if ready else scratch,
        compiler_params=pltpu.CompilerParams(vmem_limit_bytes=(4 if ready else 12) * 1024 * 1024),
        cost_estimate=pl.CostEstimate(
            flops=4 * rows * width * columns, bytes_accessed=4 * width * columns, transcendentals=0
        ),
        name="backward",
    )(*operands)


def choices(pair_ref, dims, e, r):
    far, near, pair = dims
    blocks = far * near * pair
    examples, pairs = pair_ref.shape

    def body(pair_ref, out, rows):
        at = lax.axis_index("wide")
        z, y, c = at // (near * pair), at // pair % near, at % pair
        col = lax.broadcasted_iota(jnp.int32, (examples, blocks * r), 1)
        name = jnp.zeros_like(col)
        for q in range(blocks):
            s, b, p = halvings(far)[q % far], q // far % near, q // (far * near)
            owner = ((z ^ s) * near + (y ^ b)) * pair + (c ^ p)
            rows[pl.ds(q * e, e), :] = pair_ref[pl.ds(owner * e, e), :]
            name = jnp.where((col >= q * r) & (col < (q + 1) * r), owner * r + col - q * r, name)
        for p in range(pairs):
            out[pl.ds(p * examples, examples), :] = (
                (rows[:, pl.ds(p, 1)] == name).astype(jnp.float32).astype(jnp.bfloat16)
            )

    return pl.pallas_call(
        body,
        out_shape=jax.ShapeDtypeStruct((pairs * examples, blocks * r), jnp.bfloat16),
        in_specs=[VMEM],
        out_specs=VMEM,
        scratch_shapes=[pltpu.VMEM((examples, pairs), jnp.int32)],
        compiler_params=pltpu.CompilerParams(vmem_limit_bytes=2 * 1024 * 1024),
        cost_estimate=pl.CostEstimate(flops=10**9, bytes_accessed=10**6, transcendentals=0),
        name="choices",
    )(pair_ref)


def chunks_of(width):
    if width % 128 or width < 512:
        return [(0, rounded(width, 128))]
    last = max(256, width // 4 // 256 * 256)
    return [(0, width - last), (width - last, last)]


def on_device(
    examples, references, gate_weight, up_weight, down_weight, cotangent, pair_ref, points
):
    dims = factors(lax.axis_size("wide"))
    far, near, pair = dims
    peers = lax.axis_size("narrow")
    e, r, k = examples.shape[0], references.shape[0], cotangent.shape[0]
    depth, hidden = gate_weight.shape
    blocks = far * near * pair

    share = hidden // peers
    whole_weights = [gate_weight, up_weight, down_weight]
    aligned = share % 128 == 0
    ahead = aligned and peers == 2
    if aligned:
        whole_weights = [
            pltpu.with_memory_space_constraint(w, pltpu.MemorySpace.HBM) for w in whole_weights
        ]
    chunks = chunks_of(share)
    picks = choices(pair_ref, dims, e, r)

    def at_peer(steps, offset, width):
        if aligned:
            return whole_weights, (steps % peers, peers, share, offset)
        start = (lax.axis_index("narrow") + steps) % peers * share
        more = width - share

        def cut(weight, axis):
            piece = lax.dynamic_slice_in_dim(weight, start, share, axis)
            return jnp.pad(piece, [(0, more if d == axis else 0) for d in range(2)])

        return [cut(gate_weight, 1), cut(up_weight, 1), cut(down_weight, 0)], None

    own, whole, pieces = pack([references, examples, cotangent])
    column = {0: own}
    step = far // 2
    while step:
        for s in sorted(column):
            column[s + step] = permute(column[s], "wide", dims, 0, step)
        step //= 2
    beside = {}
    if near == 2:
        for s, block in column.items():
            beside[s] = permute(block, "wide", dims, 1, 1)
    order = halvings(far)
    plane = [column[s] for s in order] + [beside[s] for s in order if near == 2]
    half = assemble(plane, whole, pieces, (r, e, k), depth)
    halves = [half]
    if pair == 2:
        halves.append(permute(half, "wide", dims, 2, 1))
    main, side = join(halves, (r, e, k))

    blocks_of_weights = {}
    later = None
    if ahead:
        wanted = [(s, chunk) for s in (1, 0) for chunk in chunks]
        for s, chunk in wanted:
            if len(chunks) == 2 and (s, chunk) == (0, chunks[0]):
                later = (s, chunk)
                continue
            blocks_of_weights[s, chunk[0]] = fetch(*at_peer(s, *chunk), chunk[1])

    parts = []
    for i, (offset, width) in enumerate(chunks):
        received = []
        for s in range(1, peers):
            weights, place = at_peer(s, offset, width)
            next_one = None
            if ahead:
                weights = blocks_of_weights[s, offset]
                if later is not None and i == 1:
                    next_one = (*at_peer(later[0], *later[1]), later[1][1])
            sent, *more = forward(main, side, weights, place, width, jnp.bfloat16, next_one)
            if more:
                blocks_of_weights[later[0], later[1][0]] = more
            received.append(shift(sent, peers, s))
        parts.append((offset, width, received))

    jobs = []
    for offset, width, received in parts:
        weights, place = at_peer(0, offset, width)
        if ahead:
            weights = blocks_of_weights[0, offset]
        (kept,) = forward(main, side, weights, place, width, jnp.float32)
        grads = coefficients(kept, received, picks, points, blocks * e)
        jobs.append((grads, offset, width, 0))
        jobs += [(shift(grads, peers, s), offset, width, s) for s in range(1, peers)]
    jobs.sort(key=lambda job: job[3])
    total = None
    last = []
    for i, (grads, offset, width, s) in enumerate(jobs):
        weights, place = at_peer(peers - s, offset, width)
        weights = blocks_of_weights[s, offset][:1] if ahead else weights[:2]
        if i < len(jobs) - 1:
            total = backward(grads, weights, place, total, False)
        else:
            spans = [(0, depth // 2), (depth // 2, depth // 2)] if depth % 256 == 0 else [(0, depth)]
            last = [backward(grads, weights, place, total, pair == 2, span) for span in spans]

    results = []
    for value in last:
        if pair == 2:
            sent, kept = value
            value = kept + permute(sent, "wide", dims, 2, 1).astype(jnp.float32)
        steps = [(1, 1)] * (near == 2) + [(0, 1 << i) for i in range(far.bit_length() - 1)]
        for digit, amount in steps:
            middle = value.shape[0] // 2
            got = permute(value[middle:].astype(jnp.bfloat16), "wide", dims, digit, amount)
            value = value[:middle] + got.astype(jnp.float32)
        results.append(value.astype(jnp.bfloat16))
    return results[0] if len(results) == 1 else jnp.concatenate(results, axis=1)


def solution(mesh):
    in_specs = (
        P("wide", "narrow"),
        P("wide", "narrow"),
        P("narrow", "wide"),
        P("narrow", "wide"),
        P("wide", "narrow"),
        P("wide", "narrow"),
        P(),
        P(),
    )
    out_specs = P("wide", "narrow")
    return jax.shard_map(on_device, mesh=mesh, in_specs=in_specs, out_specs=out_specs, check_vma=False)
```

```python
import jax
import jax.numpy as jnp
from jax import lax
from jax.experimental import pallas as pl
from jax.experimental.pallas import tpu as pltpu
from jax.sharding import PartitionSpec as P


VMEM = pl.BlockSpec(memory_space=pltpu.VMEM)
SMEM = pl.BlockSpec(memory_space=pltpu.SMEM)
ANY = pl.BlockSpec(memory_space=pl.ANY)


def factors(size):
    pair = 2 if size % 2 == 0 else 1
    near = 2 if (size // pair) % 2 == 0 else 1
    return size // (pair * near), near, pair


def rounded(rows, unit):
    return -(-rows // unit) * unit


def permute(array, axis, dims, digit, amount):
    below = 1
    for size in dims[digit + 1:]:
        below *= size
    total = below
    for size in dims[:digit + 1]:
        total *= size
    pairs = [
        (at, at + (((at // below) % dims[digit] ^ amount) - (at // below) % dims[digit]) * below)
        for at in range(total)
    ]
    return lax.ppermute(array, axis, pairs)


def shift(array, size, amount):
    return lax.ppermute(array, "narrow", [(at, (at + amount) % size) for at in range(size)])


def halvings(size):
    if size == 1:
        return [0]
    return [2 * v for v in halvings(size // 2)] + [2 * v + 1 for v in halvings(size // 2)]


def pack(arrays):
    count, width = sum(a.shape[0] for a in arrays), arrays[0].shape[1]
    whole = count // 8 * 8
    rest = count - whole
    pieces = whole // rest if rest and whole else 1
    cut = rest > 0 and whole > 0 and whole % rest == 0 and width % (pieces * 128) == 0
    if not cut:
        whole, pieces = rounded(count, 8), 1
    lanes = width // pieces

    def body(*refs):
        sources, (out, *held, sems) = refs[:len(arrays)], refs[len(arrays):]
        copies = [
            pltpu.make_async_copy(source, target, sems.at[i])
            for i, (source, target) in enumerate(zip(sources, held))
        ]
        for copy in copies:
            copy.start()
        for copy in copies:
            copy.wait()
        rows = jnp.concatenate([ref[...].astype(jnp.float32) for ref in held])
        if not cut:
            if whole > count:
                rows = jnp.concatenate([rows, jnp.zeros((whole - count, width), jnp.float32)])
            out[...] = rows.astype(out.dtype)
            return
        out[:, pl.ds(0, width)] = rows[:whole].astype(out.dtype)
        beside = [
            rows[whole + i:whole + i + 1, j * lanes:(j + 1) * lanes]
            for i in range(rest)
            for j in range(pieces)
        ]
        out[:, pl.ds(width, lanes)] = jnp.concatenate(beside).astype(out.dtype)

    packed = pl.pallas_call(
        body,
        out_shape=jax.ShapeDtypeStruct((whole, width + lanes if cut else width), arrays[0].dtype),
        in_specs=[ANY] * len(arrays),
        out_specs=VMEM,
        scratch_shapes=[pltpu.VMEM(a.shape, a.dtype) for a in arrays]
        + [pltpu.SemaphoreType.DMA((len(arrays),))],
        compiler_params=pltpu.CompilerParams(vmem_limit_bytes=4 * 1024 * 1024),
        name="pack",
    )(*(pltpu.with_memory_space_constraint(a, pltpu.MemorySpace.HBM) for a in arrays))
    return packed, whole, pieces


def assemble(own, whole, pieces, counts, width):
    blocks = len(own)
    packed = own[0].shape
    total = blocks * sum(counts)
    across_lanes = width // pieces

    def body(*refs):
        out, stack = refs[-2], refs[-1]
        for b in range(blocks):
            stack[pl.ds(b * packed[0], packed[0]), :] = refs[b][...]
        row = lax.broadcasted_iota(jnp.int32, (total, blocks * packed[0]), 0)
        col = lax.broadcasted_iota(jnp.int32, (total, blocks * packed[0]), 1)
        held = jnp.zeros_like(row)
        block = jnp.zeros_like(row)
        at = first = 0
        for count in counts:
            for b in range(blocks):
                inside = (row >= at) & (row < at + count)
                held = jnp.where(inside, row - at + first, held)
                block = jnp.where(inside, b, block)
                at += count
            first += count

        def pick(wanted, valid):
            return (valid & (col == wanted)).astype(jnp.float32).astype(jnp.bfloat16)

        base = block * packed[0]
        uncut = pick(base + held, held < whole)
        for j in range(pieces):
            lanes = pl.ds(j * across_lanes, across_lanes)
            value = jnp.dot(uncut, stack[:, lanes], preferred_element_type=jnp.float32)
            if packed[1] > width:
                value = value + jnp.dot(
                    pick(base + (held - whole) * pieces + j, held >= whole),
                    stack[:, pl.ds(width, across_lanes)],
                    preferred_element_type=jnp.float32,
                )
            out[:, lanes] = value.astype(jnp.bfloat16)

    dtype = own[0].dtype
    return pl.pallas_call(
        body,
        out_shape=jax.ShapeDtypeStruct((total, width), dtype),
        in_specs=[VMEM] * blocks,
        out_specs=VMEM,
        scratch_shapes=[pltpu.VMEM((blocks * packed[0], packed[1]), dtype)],
        compiler_params=pltpu.CompilerParams(vmem_limit_bytes=6 * 1024 * 1024),
        cost_estimate=pl.CostEstimate(flops=10**9, bytes_accessed=10**6, transcendentals=0),
        name="assemble",
    )(*own)


def join(halves, layout):
    width = halves[0].shape[1]
    blocks = halves[0].shape[0] // sum(layout)
    e, r, k = (blocks * rows for rows in layout)
    count = len(halves)

    def body(*refs):
        main, side = refs[-2:]
        for h in range(count):
            main[pl.ds(h * e, e), :] = refs[h][pl.ds(0, e), :]
            main[pl.ds(count * e + h * r, r), :] = refs[h][pl.ds(e, r), :]
            side[pl.ds(h * k, k), :] = refs[h][pl.ds(e + r, k), :]

    dtype = halves[0].dtype
    return pl.pallas_call(
        body,
        out_shape=(
            jax.ShapeDtypeStruct((count * (e + r), width), dtype),
            jax.ShapeDtypeStruct((count * k, width), dtype),
        ),
        in_specs=[VMEM] * count,
        out_specs=(VMEM, VMEM),
        compiler_params=pltpu.CompilerParams(vmem_limit_bytes=4 * 1024 * 1024),
        cost_estimate=pl.CostEstimate(flops=10**9, bytes_accessed=10**6, transcendentals=0),
        name="join",
    )(*halves)


def across(left, right):
    return lax.dot_general(left, right, (((1,), (1,)), ((), ())), preferred_element_type=jnp.float32)


def parts_of(size, unit):
    for count in (4, 2):
        if size % (count * unit) == 0:
            return [(i * (size // count), size // count) for i in range(count)]
    return [(0, size)]


def first_of(place):
    if place is None:
        return 0
    steps, peers, share, offset = place
    return pl.multiple_of((lax.axis_index("narrow") + steps) % peers * share + offset, 128)


def streams(weights, buffers, sems, first, width, by_depth, by_unit):
    gate, up, down = weights
    both, below = buffers
    units, depths = [], []
    for i, (row, count) in enumerate(by_unit):
        units.append(
            pltpu.make_async_copy(
                down.at[pl.ds(first + row, count)], below.at[pl.ds(row, count)], sems.at[2, i]
            )
        )
    for i, (row, count) in enumerate(by_depth):
        some = pl.ds(row, count)
        depths.append(
            [
                pltpu.make_async_copy(
                    source.at[some, pl.ds(first, width)],
                    both.at[some, pl.ds(w * width, width)],
                    sems.at[w, i],
                )
                for w, source in enumerate((gate, up))
            ]
        )
    return units, depths


def fetch(weights, place, width):
    depth = weights[0].shape[0]
    by_depth, by_unit = parts_of(depth, 128), parts_of(width, 32)

    def body(gate, up, down, both, below, sems):
        first = first_of(place)
        units, depths = streams((gate, up, down), (both, below), sems, first, width, by_depth, by_unit)
        copies = units + [copy for pair in depths for copy in pair]
        for copy in copies:
            copy.start()
        for copy in copies:
            copy.wait()

    return pl.pallas_call(
        body,
        out_shape=(
            pltpu.VMEM((depth, 2 * width), jnp.bfloat16),
            pltpu.VMEM((width, depth), jnp.bfloat16),
        ),
        in_specs=[ANY, ANY, ANY],
        out_specs=(VMEM, VMEM),
        scratch_shapes=[pltpu.SemaphoreType.DMA((3, 4))],
        compiler_params=pltpu.CompilerParams(vmem_limit_bytes=1024 * 1024),
        cost_estimate=pl.CostEstimate(
            flops=4 * 10**9, bytes_accessed=6 * depth * width, transcendentals=0
        ),
        name="fetch",
    )(*weights)


def forward(main, side, weights, place, width, dtype, next_one=None):
    rows, half = main.shape[0], side.shape[0] // 2
    depth = main.shape[1]
    by_depth, by_unit = parts_of(depth, 128), parts_of(width, 32)
    ready = len(weights) == 2

    def put_side(out, value):
        out[pl.ds(rows, half), pl.ds(0, width)] = value[:half].astype(dtype)
        out[pl.ds(rows, half), pl.ds(width, width)] = value[half:].astype(dtype)

    def body_ready(main_ref, side_ref, both, below, *refs):
        copies = []
        if next_one is not None:
            *refs, next_both, next_below, sems = refs
            *more, out = refs
            units, depths = streams(
                more, (next_both, next_below), sems, first_of(next_one[1]), next_one[2],
                parts_of(depth, 128), parts_of(next_one[2], 32),
            )
            copies = units + [copy for pair in depths for copy in pair]
        else:
            (out,) = refs
        for copy in copies:
            copy.start()
        out[pl.ds(0, rows), :] = jnp.dot(
            main_ref[...], both[...], preferred_element_type=jnp.float32
        ).astype(dtype)
        put_side(out, across(side_ref[...], below[...]))
        for copy in copies:
            copy.wait()

    def body(main_ref, side_ref, gate, up, down, out, both, below, total, sems):
        first = first_of(place)
        units, depths = streams((gate, up, down), (both, below), sems, first, width, by_depth, by_unit)
        for copy in units + [copy for pair in depths for copy in pair]:
            copy.start()
        for copy in units:
            copy.wait()
        put_side(out, across(side_ref[...], below[...]))
        for i, (row, count) in enumerate(by_depth):
            for copy in depths[i]:
                copy.wait()
            some = pl.ds(row, count)
            part = jnp.dot(main_ref[:, some], both[some, :], preferred_element_type=jnp.float32)
            if i > 0:
                part = total[...] + part
            if i == len(by_depth) - 1:
                out[pl.ds(0, rows), :] = part.astype(dtype)
            else:
                total[...] = part

    out_shape = [jax.ShapeDtypeStruct((rows + half, 2 * width), dtype)]
    operands = [main, side, *weights]
    specs = [VMEM] * 2 + [VMEM if ready else ANY] * len(weights)
    if ready:
        scratch = []
        if next_one is not None:
            operands += next_one[0]
            specs += [ANY] * 3
            out_shape += [
                pltpu.VMEM((depth, 2 * next_one[2]), jnp.bfloat16),
                pltpu.VMEM((next_one[2], depth), jnp.bfloat16),
            ]
            scratch = [pltpu.SemaphoreType.DMA((3, 4))]
    else:
        scratch = [
            pltpu.VMEM((depth, 2 * width), jnp.bfloat16),
            pltpu.VMEM((width, depth), jnp.bfloat16),
            pltpu.VMEM((rows, 2 * width), jnp.float32),
            pltpu.SemaphoreType.DMA((3, 4)),
        ]
    return pl.pallas_call(
        body_ready if ready else body,
        out_shape=out_shape,
        in_specs=specs,
        out_specs=[VMEM] * len(out_shape),
        scratch_shapes=scratch,
        compiler_params=pltpu.CompilerParams(vmem_limit_bytes=(4 if ready else 20) * 1024 * 1024),
        cost_estimate=pl.CostEstimate(
            flops=4 * depth * width * (rows + half), bytes_accessed=6 * depth * width, transcendentals=0
        ),
        name="forward",
    )(*operands)


def coefficients(kept, received, picks, points, examples):
    width = kept.shape[1] // 2
    pairs, references = picks.shape[0] // examples, picks.shape[1]
    rows = examples + references
    count = points.shape[0]
    lanes = 128 if width % 128 == 0 else width
    piece = 16 if examples % 32 == 16 else examples // 2
    scale = 1.0 / (pairs * count)

    def body(points_ref, picks_ref, kept_ref, *refs):
        got, out, base_gate, base_up = refs[:-3], refs[-3], refs[-2], refs[-1]
        picks = picks_ref[...]
        steps = [points_ref[m].astype(jnp.float32) * 0.125 for m in range(count)]
        steps_1 = sum(steps[1:], steps[0])
        steps_2 = sum((t * t for t in steps[1:]), steps[0] * steps[0])

        def block(j, _):
            if lanes == width:
                of = [pl.ds(w * width, width) for w in range(2)]
            else:
                of = [pl.ds(pl.multiple_of(w * width + j * lanes, 128), lanes) for w in range(2)]

            def total(start, size, w):
                value = kept_ref[pl.ds(start, size), of[w]]
                for ref in got:
                    value = value + ref[pl.ds(start, size), of[w]].astype(jnp.float32)
                return value

            for w, target in enumerate((base_gate, base_up)):
                value = total(0, references, w)
                high = value.astype(jnp.bfloat16)
                low = (value - high.astype(jnp.float32)).astype(jnp.bfloat16)
                target[...] = jnp.dot(picks, high, preferred_element_type=jnp.float32) + jnp.dot(
                    picks, low, preferred_element_type=jnp.float32
                )
            upstream = [total(rows, examples // 2, w) for w in range(2)]
            for first in range(0, examples, piece):
                gate = total(references + first, piece, 0) * 0.5
                up = total(references + first, piece, 1)
                coef_gate = jnp.zeros_like(gate)
                coef_up = jnp.zeros_like(gate)
                for p in range(pairs):
                    start = base_gate[pl.ds(p * examples + first, piece), :] * 0.5
                    span = gate - start
                    flat = count + (count * start + steps_1 * span)
                    tilted = steps_1 + (steps_1 * start + steps_2 * span)
                    coef_up = coef_up + (count * start + steps_1 * span)
                    for t in steps:
                        half = start + t * span
                        v = jnp.tanh(half)
                        bent = half * v
                        turn = v - v * bent
                        coef_up = coef_up + bent
                        flat = flat + turn
                        tilted = tilted + t * turn
                    start_up = base_up[pl.ds(p * examples + first, piece), :]
                    coef_gate = coef_gate + (start_up * flat + (up - start_up) * tilted)
                base_gate[pl.ds(first, piece), :] = coef_gate * (0.5 * scale)
                base_up[pl.ds(first, piece), :] = coef_up * scale
            for w, source in enumerate((base_gate, base_up)):
                for h in range(2):
                    some = pl.ds(h * (examples // 2), examples // 2)
                    out[some, of[w]] = (upstream[h] * source[some, :]).astype(jnp.bfloat16)
            return 0

        lax.fori_loop(0, width // lanes, block, 0)

    return pl.pallas_call(
        body,
        out_shape=jax.ShapeDtypeStruct((examples, 2 * width), jnp.bfloat16),
        in_specs=[SMEM, VMEM, VMEM] + [VMEM] * len(received),
        out_specs=VMEM,
        scratch_shapes=[pltpu.VMEM((pairs * examples, lanes), jnp.float32)] * 2,
        compiler_params=pltpu.CompilerParams(vmem_limit_bytes=4 * 1024 * 1024),
        cost_estimate=pl.CostEstimate(flops=5 * 10**9, bytes_accessed=10**6, transcendentals=0),
        name="coefficients",
    )(points, picks, kept, *received)


def backward(items, total, final, span=None):
    grads, weights, place = items[0]
    rows, width, depth = grads.shape[0], grads.shape[1] // 2, weights[0].shape[0]
    low, columns = span or (0, depth)
    by_depth = [(low + row, count) for row, count in parts_of(columns, 128)]
    ready = len(weights) == 1

    def body(*refs):
        grads_refs, refs = refs[:len(items)], refs[len(items):]
        if ready:
            boths, outs = refs[:len(items)], refs[len(items):]
        else:
            gate, up, *outs, both, sems = refs
            boths = [both]
            _, depths = streams((gate, up, None), (both, None), sems, first_of(place), width, by_depth, [])
            for pair in depths:
                for copy in pair:
                    copy.start()
        for i, (row, count) in enumerate(by_depth):
            some, own = pl.ds(row, count), pl.ds(row - low, count)
            if not ready:
                for copy in depths[i]:
                    copy.wait()
            value = None if total is None else outs[0][:, some]
            for grads_ref, both in zip(grads_refs, boths):
                part = across(grads_ref[...], both[some, :])
                value = part if value is None else value + part
            if final:
                outs[-2][:, own] = value[rows // 2:, :].astype(jnp.bfloat16)
                outs[-1][:, own] = value[:rows // 2, :]
            else:
                outs[-1][:, own] = value

    operands = [item[0] for item in items] + [w for item in items for w in item[1]]
    specs = [VMEM] * len(items) + [VMEM if ready else ANY] * (len(operands) - len(items))
    if total is not None:
        operands.append(total)
        specs.append(VMEM)
    if final:
        out_shape = (
            jax.ShapeDtypeStruct((rows // 2, columns), jnp.bfloat16),
            jax.ShapeDtypeStruct((rows // 2, columns), jnp.float32),
        )
        out_specs = (VMEM, VMEM)
    else:
        out_shape, out_specs = jax.ShapeDtypeStruct((rows, columns), jnp.float32), VMEM
    scratch = [pltpu.VMEM((depth, 2 * width), jnp.bfloat16), pltpu.SemaphoreType.DMA((2, 4))]
    return pl.pallas_call(
        body,
        out_shape=out_shape,
        in_specs=specs,
        out_specs=out_specs,
        scratch_shapes=[] if ready else scratch,
        compiler_params=pltpu.CompilerParams(vmem_limit_bytes=(4 if ready else 12) * 1024 * 1024),
        cost_estimate=pl.CostEstimate(
            flops=2 * rows * columns * sum(item[0].shape[1] for item in items),
            bytes_accessed=4 * width * columns,
            transcendentals=0,
        ),
        name="backward",
    )(*operands)


def choices(pair_ref, dims, e, r):
    far, near, pair = dims
    blocks = far * near * pair
    examples, pairs = pair_ref.shape

    def body(pair_ref, out, rows):
        at = lax.axis_index("wide")
        z, y, c = at // (near * pair), at // pair % near, at % pair
        col = lax.broadcasted_iota(jnp.int32, (examples, blocks * r), 1)
        name = jnp.zeros_like(col)
        for q in range(blocks):
            s, b, p = halvings(far)[q % far], q // far % near, q // (far * near)
            owner = ((z ^ s) * near + (y ^ b)) * pair + (c ^ p)
            rows[pl.ds(q * e, e), :] = pair_ref[pl.ds(owner * e, e), :]
            name = jnp.where((col >= q * r) & (col < (q + 1) * r), owner * r + col - q * r, name)
        for p in range(pairs):
            out[pl.ds(p * examples, examples), :] = (
                (rows[:, pl.ds(p, 1)] == name).astype(jnp.float32).astype(jnp.bfloat16)
            )

    return pl.pallas_call(
        body,
        out_shape=jax.ShapeDtypeStruct((pairs * examples, blocks * r), jnp.bfloat16),
        in_specs=[VMEM],
        out_specs=VMEM,
        scratch_shapes=[pltpu.VMEM((examples, pairs), jnp.int32)],
        compiler_params=pltpu.CompilerParams(vmem_limit_bytes=2 * 1024 * 1024),
        cost_estimate=pl.CostEstimate(flops=10**9, bytes_accessed=10**6, transcendentals=0),
        name="choices",
    )(pair_ref)


def chunks_of(width):
    if width % 128 or width < 512:
        return [(0, rounded(width, 128))]
    first = rounded(width // 2, 256)
    return [(0, first), (first, width - first)]


def on_device(
    examples, references, gate_weight, up_weight, down_weight, cotangent, pair_ref, points
):
    dims = factors(lax.axis_size("wide"))
    far, near, pair = dims
    peers = lax.axis_size("narrow")
    e, r, k = examples.shape[0], references.shape[0], cotangent.shape[0]
    depth, hidden = gate_weight.shape
    blocks = far * near * pair

    share = hidden // peers
    whole_weights = [gate_weight, up_weight, down_weight]
    aligned = share % 128 == 0
    ahead = aligned and peers == 2
    if aligned:
        whole_weights = [
            pltpu.with_memory_space_constraint(w, pltpu.MemorySpace.HBM) for w in whole_weights
        ]
    chunks = chunks_of(share)
    picks = choices(pair_ref, dims, e, r)

    def at_peer(steps, offset, width):
        if aligned:
            return whole_weights, (steps % peers, peers, share, offset)
        start = (lax.axis_index("narrow") + steps) % peers * share
        more = width - share

        def cut(weight, axis):
            piece = lax.dynamic_slice_in_dim(weight, start, share, axis)
            return jnp.pad(piece, [(0, more if d == axis else 0) for d in range(2)])

        return [cut(gate_weight, 1), cut(up_weight, 1), cut(down_weight, 0)], None

    own, whole, pieces = pack([references, examples, cotangent])
    column = {0: own}
    step = far // 2
    while step:
        for s in sorted(column):
            column[s + step] = permute(column[s], "wide", dims, 0, step)
        step //= 2
    beside = {}
    if near == 2:
        for s, block in column.items():
            beside[s] = permute(block, "wide", dims, 1, 1)
    order = halvings(far)
    plane = [column[s] for s in order] + [beside[s] for s in order if near == 2]
    half = assemble(plane, whole, pieces, (r, e, k), depth)
    halves = [half]
    if pair == 2:
        halves.append(permute(half, "wide", dims, 2, 1))
    main, side = join(halves, (r, e, k))

    blocks_of_weights = {}
    if ahead:
        for chunk in chunks:
            blocks_of_weights[1, chunk[0]] = fetch(*at_peer(1, *chunk), chunk[1])

    parts = []
    for i, (offset, width) in enumerate(chunks):
        received = []
        for s in range(1, peers):
            weights, place = at_peer(s, offset, width)
            next_one = None
            if ahead:
                weights = blocks_of_weights[s, offset]
                later = chunks[-1 - i]
                next_one = (*at_peer(0, *later), later[1])
            sent, *more = forward(main, side, weights, place, width, jnp.bfloat16, next_one)
            if more:
                blocks_of_weights[0, later[0]] = more
            received.append(shift(sent, peers, s))
        parts.append((offset, width, received))

    jobs = []
    for offset, width, received in parts:
        weights, place = at_peer(0, offset, width)
        if ahead:
            weights = blocks_of_weights[0, offset]
        (kept,) = forward(main, side, weights, place, width, jnp.float32)
        grads = coefficients(kept, received, picks, points, blocks * e)
        jobs.append((grads, offset, width, 0))
        jobs += [(shift(grads, peers, s), offset, width, s) for s in range(1, peers)]
    items = []
    for grads, offset, width, s in jobs:
        weights, place = at_peer(peers - s, offset, width)
        weights = blocks_of_weights[s, offset][:1] if ahead else weights[:2]
        items.append((grads, weights, place))
    if ahead and len(items) == 4:
        groups = [items[:1], items[1:3], items[3:]]
    else:
        groups = [[item] for item in items]
    total = None
    for group in groups[:-1]:
        total = backward(group, total, False)
    spans = [(0, depth // 2), (depth // 2, depth // 2)] if depth % 256 == 0 else [(0, depth)]
    last = [backward(groups[-1], total, pair == 2, span) for span in spans]

    results = []
    for value in last:
        if pair == 2:
            sent, kept = value
            value = kept + permute(sent, "wide", dims, 2, 1).astype(jnp.float32)
        steps = [(1, 1)] * (near == 2) + [(0, 1 << i) for i in range(far.bit_length() - 1)]
        for digit, amount in steps:
            middle = value.shape[0] // 2
            got = permute(value[middle:].astype(jnp.bfloat16), "wide", dims, digit, amount)
            value = value[:middle] + got.astype(jnp.float32)
        results.append(value.astype(jnp.bfloat16))
    return results[0] if len(results) == 1 else jnp.concatenate(results, axis=1)


def solution(mesh):
    in_specs = (
        P("wide", "narrow"),
        P("wide", "narrow"),
        P("narrow", "wide"),
        P("narrow", "wide"),
        P("wide", "narrow"),
        P("wide", "narrow"),
        P(),
        P(),
    )
    out_specs = P("wide", "narrow")
    return jax.shard_map(on_device, mesh=mesh, in_specs=in_specs, out_specs=out_specs, check_vma=False)
```

```python
import jax
import jax.numpy as jnp
from jax import lax
from jax.experimental import pallas as pl
from jax.experimental.pallas import tpu as pltpu
from jax.sharding import PartitionSpec as P


VMEM = pl.BlockSpec(memory_space=pltpu.VMEM)
SMEM = pl.BlockSpec(memory_space=pltpu.SMEM)
ANY = pl.BlockSpec(memory_space=pl.ANY)


def factors(size):
    pair = 2 if size % 2 == 0 else 1
    near = 2 if (size // pair) % 2 == 0 else 1
    return size // (pair * near), near, pair


def rounded(rows, unit):
    return -(-rows // unit) * unit


def permute(array, axis, dims, digit, amount):
    below = 1
    for size in dims[digit + 1:]:
        below *= size
    total = below
    for size in dims[:digit + 1]:
        total *= size
    pairs = [
        (at, at + (((at // below) % dims[digit] ^ amount) - (at // below) % dims[digit]) * below)
        for at in range(total)
    ]
    return lax.ppermute(array, axis, pairs)


def shift(array, size, amount):
    return lax.ppermute(array, "narrow", [(at, (at + amount) % size) for at in range(size)])


def halvings(size):
    if size == 1:
        return [0]
    return [2 * v for v in halvings(size // 2)] + [2 * v + 1 for v in halvings(size // 2)]


def pack(arrays):
    count, width = sum(a.shape[0] for a in arrays), arrays[0].shape[1]
    whole = count // 8 * 8
    rest = count - whole
    pieces = whole // rest if rest and whole else 1
    cut = rest > 0 and whole > 0 and whole % rest == 0 and width % (pieces * 128) == 0
    if not cut:
        whole, pieces = rounded(count, 8), 1
    lanes = width // pieces

    def body(*refs):
        sources, (out, *held, sems) = refs[:len(arrays)], refs[len(arrays):]
        copies = [
            pltpu.make_async_copy(source, target, sems.at[i])
            for i, (source, target) in enumerate(zip(sources, held))
        ]
        for copy in copies:
            copy.start()
        for copy in copies:
            copy.wait()
        rows = jnp.concatenate([ref[...].astype(jnp.float32) for ref in held])
        if not cut:
            if whole > count:
                rows = jnp.concatenate([rows, jnp.zeros((whole - count, width), jnp.float32)])
            out[...] = rows.astype(out.dtype)
            return
        out[:, pl.ds(0, width)] = rows[:whole].astype(out.dtype)
        beside = [
            rows[whole + i:whole + i + 1, j * lanes:(j + 1) * lanes]
            for i in range(rest)
            for j in range(pieces)
        ]
        out[:, pl.ds(width, lanes)] = jnp.concatenate(beside).astype(out.dtype)

    packed = pl.pallas_call(
        body,
        out_shape=jax.ShapeDtypeStruct((whole, width + lanes if cut else width), arrays[0].dtype),
        in_specs=[ANY] * len(arrays),
        out_specs=VMEM,
        scratch_shapes=[pltpu.VMEM(a.shape, a.dtype) for a in arrays]
        + [pltpu.SemaphoreType.DMA((len(arrays),))],
        compiler_params=pltpu.CompilerParams(vmem_limit_bytes=4 * 1024 * 1024),
        name="pack",
    )(*(pltpu.with_memory_space_constraint(a, pltpu.MemorySpace.HBM) for a in arrays))
    return packed, whole, pieces


def assemble(own, whole, pieces, counts, width):
    blocks = len(own)
    packed = own[0].shape
    total = blocks * sum(counts)
    across_lanes = width // pieces

    def body(*refs):
        out, stack = refs[-2], refs[-1]
        for b in range(blocks):
            stack[pl.ds(b * packed[0], packed[0]), :] = refs[b][...]
        row = lax.broadcasted_iota(jnp.int32, (total, blocks * packed[0]), 0)
        col = lax.broadcasted_iota(jnp.int32, (total, blocks * packed[0]), 1)
        held = jnp.zeros_like(row)
        block = jnp.zeros_like(row)
        at = first = 0
        for count in counts:
            for b in range(blocks):
                inside = (row >= at) & (row < at + count)
                held = jnp.where(inside, row - at + first, held)
                block = jnp.where(inside, b, block)
                at += count
            first += count

        def pick(wanted, valid):
            return (valid & (col == wanted)).astype(jnp.float32).astype(jnp.bfloat16)

        base = block * packed[0]
        uncut = pick(base + held, held < whole)
        for j in range(pieces):
            lanes = pl.ds(j * across_lanes, across_lanes)
            value = jnp.dot(uncut, stack[:, lanes], preferred_element_type=jnp.float32)
            if packed[1] > width:
                value = value + jnp.dot(
                    pick(base + (held - whole) * pieces + j, held >= whole),
                    stack[:, pl.ds(width, across_lanes)],
                    preferred_element_type=jnp.float32,
                )
            out[:, lanes] = value.astype(jnp.bfloat16)

    dtype = own[0].dtype
    return pl.pallas_call(
        body,
        out_shape=jax.ShapeDtypeStruct((total, width), dtype),
        in_specs=[VMEM] * blocks,
        out_specs=VMEM,
        scratch_shapes=[pltpu.VMEM((blocks * packed[0], packed[1]), dtype)],
        compiler_params=pltpu.CompilerParams(vmem_limit_bytes=6 * 1024 * 1024),
        cost_estimate=pl.CostEstimate(flops=10**9, bytes_accessed=10**6, transcendentals=0),
        name="assemble",
    )(*own)


def join(halves, layout):
    width = halves[0].shape[1]
    blocks = halves[0].shape[0] // sum(layout)
    e, r, k = (blocks * rows for rows in layout)
    count = len(halves)

    def body(*refs):
        main, side = refs[-2:]
        for h in range(count):
            main[pl.ds(h * e, e), :] = refs[h][pl.ds(0, e), :]
            main[pl.ds(count * e + h * r, r), :] = refs[h][pl.ds(e, r), :]
            side[pl.ds(h * k, k), :] = refs[h][pl.ds(e + r, k), :]

    dtype = halves[0].dtype
    return pl.pallas_call(
        body,
        out_shape=(
            jax.ShapeDtypeStruct((count * (e + r), width), dtype),
            jax.ShapeDtypeStruct((count * k, width), dtype),
        ),
        in_specs=[VMEM] * count,
        out_specs=(VMEM, VMEM),
        compiler_params=pltpu.CompilerParams(vmem_limit_bytes=4 * 1024 * 1024),
        cost_estimate=pl.CostEstimate(flops=10**9, bytes_accessed=10**6, transcendentals=0),
        name="join",
    )(*halves)


def across(left, right):
    return lax.dot_general(left, right, (((1,), (1,)), ((), ())), preferred_element_type=jnp.float32)


def parts_of(size, unit):
    for count in (4, 2):
        if size % (count * unit) == 0:
            return [(i * (size // count), size // count) for i in range(count)]
    return [(0, size)]


def first_of(place):
    if place is None:
        return 0
    steps, peers, share, offset = place
    return pl.multiple_of((lax.axis_index("narrow") + steps) % peers * share + offset, 128)


def streams(weights, buffers, sems, first, width, by_depth, by_unit):
    gate, up, down = weights
    both, below = buffers
    units, depths = [], []
    for i, (row, count) in enumerate(by_unit):
        units.append(
            pltpu.make_async_copy(
                down.at[pl.ds(first + row, count)], below.at[pl.ds(row, count)], sems.at[2, i]
            )
        )
    for i, (row, count) in enumerate(by_depth):
        some = pl.ds(row, count)
        depths.append(
            [
                pltpu.make_async_copy(
                    source.at[some, pl.ds(first, width)],
                    both.at[some, pl.ds(w * width, width)],
                    sems.at[w, i],
                )
                for w, source in enumerate((gate, up))
            ]
        )
    return units, depths


def fetch(weights, place, width):
    depth = weights[0].shape[0]
    by_depth, by_unit = parts_of(depth, 128), parts_of(width, 32)

    def body(gate, up, down, both, below, sems):
        first = first_of(place)
        units, depths = streams((gate, up, down), (both, below), sems, first, width, by_depth, by_unit)
        copies = units + [copy for pair in depths for copy in pair]
        for copy in copies:
            copy.start()
        for copy in copies:
            copy.wait()

    return pl.pallas_call(
        body,
        out_shape=(
            pltpu.VMEM((depth, 2 * width), jnp.bfloat16),
            pltpu.VMEM((width, depth), jnp.bfloat16),
        ),
        in_specs=[ANY, ANY, ANY],
        out_specs=(VMEM, VMEM),
        scratch_shapes=[pltpu.SemaphoreType.DMA((3, 4))],
        compiler_params=pltpu.CompilerParams(vmem_limit_bytes=1024 * 1024),
        cost_estimate=pl.CostEstimate(
            flops=4 * 10**9, bytes_accessed=6 * depth * width, transcendentals=0
        ),
        name="fetch",
    )(*weights)


def forward(main, side, weights, place, width, dtype, next_one=None):
    rows, half = main.shape[0], side.shape[0] // 2
    depth = main.shape[1]
    by_depth, by_unit = parts_of(depth, 128), parts_of(width, 32)
    ready = len(weights) == 2

    def put_side(out, value):
        out[pl.ds(rows, half), pl.ds(0, width)] = value[:half].astype(dtype)
        out[pl.ds(rows, half), pl.ds(width, width)] = value[half:].astype(dtype)

    def body_ready(main_ref, side_ref, both, below, *refs):
        copies = []
        if next_one is not None:
            *refs, next_both, next_below, sems = refs
            *more, out = refs
            units, depths = streams(
                more, (next_both, next_below), sems, first_of(next_one[1]), next_one[2],
                parts_of(depth, 128), parts_of(next_one[2], 32),
            )
            copies = units + [copy for pair in depths for copy in pair]
        else:
            (out,) = refs
        for copy in copies:
            copy.start()

        @pl.when(lax.axis_index("narrow") >= 0)
        def _():
            out[pl.ds(0, rows), :] = jnp.dot(
                main_ref[...], both[...], preferred_element_type=jnp.float32
            ).astype(dtype)
            put_side(out, across(side_ref[...], below[...]))

        for copy in copies:
            copy.wait()

    def body(main_ref, side_ref, gate, up, down, out, both, below, total, sems):
        first = first_of(place)
        units, depths = streams((gate, up, down), (both, below), sems, first, width, by_depth, by_unit)
        for copy in units + [copy for pair in depths for copy in pair]:
            copy.start()
        for copy in units:
            copy.wait()
        put_side(out, across(side_ref[...], below[...]))
        for i, (row, count) in enumerate(by_depth):
            for copy in depths[i]:
                copy.wait()
            some = pl.ds(row, count)
            part = jnp.dot(main_ref[:, some], both[some, :], preferred_element_type=jnp.float32)
            if i > 0:
                part = total[...] + part
            if i == len(by_depth) - 1:
                out[pl.ds(0, rows), :] = part.astype(dtype)
            else:
                total[...] = part

    out_shape = [jax.ShapeDtypeStruct((rows + half, 2 * width), dtype)]
    operands = [main, side, *weights]
    specs = [VMEM] * 2 + [VMEM if ready else ANY] * len(weights)
    if ready:
        scratch = []
        if next_one is not None:
            operands += next_one[0]
            specs += [ANY] * 3
            out_shape += [
                pltpu.VMEM((depth, 2 * next_one[2]), jnp.bfloat16),
                pltpu.VMEM((next_one[2], depth), jnp.bfloat16),
            ]
            scratch = [pltpu.SemaphoreType.DMA((3, 4))]
    else:
        scratch = [
            pltpu.VMEM((depth, 2 * width), jnp.bfloat16),
            pltpu.VMEM((width, depth), jnp.bfloat16),
            pltpu.VMEM((rows, 2 * width), jnp.float32),
            pltpu.SemaphoreType.DMA((3, 4)),
        ]
    return pl.pallas_call(
        body_ready if ready else body,
        out_shape=out_shape,
        in_specs=specs,
        out_specs=[VMEM] * len(out_shape),
        scratch_shapes=scratch,
        compiler_params=pltpu.CompilerParams(vmem_limit_bytes=(4 if ready else 20) * 1024 * 1024),
        cost_estimate=pl.CostEstimate(
            flops=4 * depth * width * (rows + half), bytes_accessed=6 * depth * width, transcendentals=0
        ),
        name="forward",
    )(*operands)


def coefficients(kept, received, picks, points, examples):
    width = kept.shape[1] // 2
    pairs, references = picks.shape[0] // examples, picks.shape[1]
    rows = examples + references
    count = points.shape[0]
    lanes = 128 if width % 128 == 0 else width
    piece = 16 if examples % 32 == 16 else examples // 2
    scale = 1.0 / (pairs * count)

    def body(points_ref, picks_ref, kept_ref, *refs):
        got, out, base_gate, base_up = refs[:-3], refs[-3], refs[-2], refs[-1]
        picks = picks_ref[...]
        steps = [points_ref[m].astype(jnp.float32) * 0.125 for m in range(count)]
        steps_1 = sum(steps[1:], steps[0])
        steps_2 = sum((t * t for t in steps[1:]), steps[0] * steps[0])

        def block(j, _):
            if lanes == width:
                of = [pl.ds(w * width, width) for w in range(2)]
            else:
                of = [pl.ds(pl.multiple_of(w * width + j * lanes, 128), lanes) for w in range(2)]

            def total(start, size, w):
                value = kept_ref[pl.ds(start, size), of[w]]
                for ref in got:
                    value = value + ref[pl.ds(start, size), of[w]].astype(jnp.float32)
                return value

            for w, target in enumerate((base_gate, base_up)):
                value = total(0, references, w)
                high = value.astype(jnp.bfloat16)
                low = (value - high.astype(jnp.float32)).astype(jnp.bfloat16)
                target[...] = jnp.dot(picks, high, preferred_element_type=jnp.float32) + jnp.dot(
                    picks, low, preferred_element_type=jnp.float32
                )
            upstream = [total(rows, examples // 2, w) for w in range(2)]
            for first in range(0, examples, piece):
                gate = total(references + first, piece, 0) * 0.5
                up = total(references + first, piece, 1)
                coef_gate = jnp.zeros_like(gate)
                coef_up = jnp.zeros_like(gate)
                for p in range(pairs):
                    start = base_gate[pl.ds(p * examples + first, piece), :] * 0.5
                    span = gate - start
                    flat = count + (count * start + steps_1 * span)
                    tilted = steps_1 + (steps_1 * start + steps_2 * span)
                    coef_up = coef_up + (count * start + steps_1 * span)
                    for t in steps:
                        half = start + t * span
                        v = jnp.tanh(half)
                        bent = half * v
                        turn = v - v * bent
                        coef_up = coef_up + bent
                        flat = flat + turn
                        tilted = tilted + t * turn
                    start_up = base_up[pl.ds(p * examples + first, piece), :]
                    coef_gate = coef_gate + (start_up * flat + (up - start_up) * tilted)
                base_gate[pl.ds(first, piece), :] = coef_gate * (0.5 * scale)
                base_up[pl.ds(first, piece), :] = coef_up * scale
            for w, source in enumerate((base_gate, base_up)):
                for h in range(2):
                    some = pl.ds(h * (examples // 2), examples // 2)
                    out[some, of[w]] = (upstream[h] * source[some, :]).astype(jnp.bfloat16)
            return 0

        lax.fori_loop(0, width // lanes, block, 0)

    return pl.pallas_call(
        body,
        out_shape=jax.ShapeDtypeStruct((examples, 2 * width), jnp.bfloat16),
        in_specs=[SMEM, VMEM, VMEM] + [VMEM] * len(received),
        out_specs=VMEM,
        scratch_shapes=[pltpu.VMEM((pairs * examples, lanes), jnp.float32)] * 2,
        compiler_params=pltpu.CompilerParams(vmem_limit_bytes=4 * 1024 * 1024),
        cost_estimate=pl.CostEstimate(flops=5 * 10**9, bytes_accessed=10**6, transcendentals=0),
        name="coefficients",
    )(points, picks, kept, *received)


def backward(items, total, final, span=None):
    grads, weights, place = items[0]
    rows, width, depth = grads.shape[0], grads.shape[1] // 2, weights[0].shape[0]
    low, columns = span or (0, depth)
    by_depth = [(low + row, count) for row, count in parts_of(columns, 128)]
    ready = len(weights) == 1

    def body(*refs):
        grads_refs, refs = refs[:len(items)], refs[len(items):]
        if ready:
            boths, outs = refs[:len(items)], refs[len(items):]
        else:
            gate, up, *outs, both, sems = refs
            boths = [both]
            _, depths = streams((gate, up, None), (both, None), sems, first_of(place), width, by_depth, [])
            for pair in depths:
                for copy in pair:
                    copy.start()
        for i, (row, count) in enumerate(by_depth):
            some, own = pl.ds(row, count), pl.ds(row - low, count)
            if not ready:
                for copy in depths[i]:
                    copy.wait()
            value = None if total is None else outs[0][:, some]
            for grads_ref, both in zip(grads_refs, boths):
                part = across(grads_ref[...], both[some, :])
                value = part if value is None else value + part
            if final:
                outs[-2][:, own] = value[rows // 2:, :].astype(jnp.bfloat16)
                outs[-1][:, own] = value[:rows // 2, :]
            else:
                outs[-1][:, own] = value

    operands = [item[0] for item in items] + [w for item in items for w in item[1]]
    specs = [VMEM] * len(items) + [VMEM if ready else ANY] * (len(operands) - len(items))
    if total is not None:
        operands.append(total)
        specs.append(VMEM)
    if final:
        out_shape = (
            jax.ShapeDtypeStruct((rows // 2, columns), jnp.bfloat16),
            jax.ShapeDtypeStruct((rows // 2, columns), jnp.float32),
        )
        out_specs = (VMEM, VMEM)
    else:
        out_shape, out_specs = jax.ShapeDtypeStruct((rows, columns), jnp.float32), VMEM
    scratch = [pltpu.VMEM((depth, 2 * width), jnp.bfloat16), pltpu.SemaphoreType.DMA((2, 4))]
    return pl.pallas_call(
        body,
        out_shape=out_shape,
        in_specs=specs,
        out_specs=out_specs,
        scratch_shapes=[] if ready else scratch,
        compiler_params=pltpu.CompilerParams(vmem_limit_bytes=(4 if ready else 12) * 1024 * 1024),
        cost_estimate=pl.CostEstimate(
            flops=2 * rows * columns * sum(item[0].shape[1] for item in items),
            bytes_accessed=4 * width * columns,
            transcendentals=0,
        ),
        name="backward",
    )(*operands)


def choices(pair_ref, dims, e, r):
    far, near, pair = dims
    blocks = far * near * pair
    examples, pairs = pair_ref.shape

    def body(pair_ref, out, rows):
        at = lax.axis_index("wide")
        z, y, c = at // (near * pair), at // pair % near, at % pair
        col = lax.broadcasted_iota(jnp.int32, (examples, blocks * r), 1)
        name = jnp.zeros_like(col)
        for q in range(blocks):
            s, b, p = halvings(far)[q % far], q // far % near, q // (far * near)
            owner = ((z ^ s) * near + (y ^ b)) * pair + (c ^ p)
            rows[pl.ds(q * e, e), :] = pair_ref[pl.ds(owner * e, e), :]
            name = jnp.where((col >= q * r) & (col < (q + 1) * r), owner * r + col - q * r, name)
        for p in range(pairs):
            out[pl.ds(p * examples, examples), :] = (
                (rows[:, pl.ds(p, 1)] == name).astype(jnp.float32).astype(jnp.bfloat16)
            )

    return pl.pallas_call(
        body,
        out_shape=jax.ShapeDtypeStruct((pairs * examples, blocks * r), jnp.bfloat16),
        in_specs=[VMEM],
        out_specs=VMEM,
        scratch_shapes=[pltpu.VMEM((examples, pairs), jnp.int32)],
        compiler_params=pltpu.CompilerParams(vmem_limit_bytes=2 * 1024 * 1024),
        cost_estimate=pl.CostEstimate(flops=10**9, bytes_accessed=10**6, transcendentals=0),
        name="choices",
    )(pair_ref)


def chunks_of(width):
    if width % 128 or width < 512:
        return [(0, rounded(width, 128))]
    first = rounded(width // 2, 256)
    return [(0, first), (first, width - first)]


def on_device(
    examples, references, gate_weight, up_weight, down_weight, cotangent, pair_ref, points
):
    dims = factors(lax.axis_size("wide"))
    far, near, pair = dims
    peers = lax.axis_size("narrow")
    e, r, k = examples.shape[0], references.shape[0], cotangent.shape[0]
    depth, hidden = gate_weight.shape
    blocks = far * near * pair

    share = hidden // peers
    whole_weights = [gate_weight, up_weight, down_weight]
    aligned = share % 128 == 0
    ahead = aligned and peers == 2
    if aligned:
        whole_weights = [
            pltpu.with_memory_space_constraint(w, pltpu.MemorySpace.HBM) for w in whole_weights
        ]
    chunks = chunks_of(share)
    picks = choices(pair_ref, dims, e, r)

    def at_peer(steps, offset, width):
        if aligned:
            return whole_weights, (steps % peers, peers, share, offset)
        start = (lax.axis_index("narrow") + steps) % peers * share
        more = width - share

        def cut(weight, axis):
            piece = lax.dynamic_slice_in_dim(weight, start, share, axis)
            return jnp.pad(piece, [(0, more if d == axis else 0) for d in range(2)])

        return [cut(gate_weight, 1), cut(up_weight, 1), cut(down_weight, 0)], None

    own, whole, pieces = pack([references, examples, cotangent])
    column = {0: own}
    step = far // 2
    while step:
        for s in sorted(column):
            column[s + step] = permute(column[s], "wide", dims, 0, step)
        step //= 2
    beside = {}
    if near == 2:
        for s, block in column.items():
            beside[s] = permute(block, "wide", dims, 1, 1)
    order = halvings(far)
    plane = [column[s] for s in order] + [beside[s] for s in order if near == 2]
    half = assemble(plane, whole, pieces, (r, e, k), depth)
    halves = [half]
    if pair == 2:
        halves.append(permute(half, "wide", dims, 2, 1))
    main, side = join(halves, (r, e, k))

    blocks_of_weights = {}
    if ahead:
        for chunk in chunks:
            blocks_of_weights[1, chunk[0]] = fetch(*at_peer(1, *chunk), chunk[1])

    parts = []
    for i, (offset, width) in enumerate(chunks):
        received = []
        for s in range(1, peers):
            weights, place = at_peer(s, offset, width)
            next_one = None
            if ahead:
                weights = blocks_of_weights[s, offset]
                later = chunks[-1 - i]
                next_one = (*at_peer(0, *later), later[1])
            sent, *more = forward(main, side, weights, place, width, jnp.bfloat16, next_one)
            if more:
                blocks_of_weights[0, later[0]] = more
            received.append(shift(sent, peers, s))
        parts.append((offset, width, received))

    jobs = []
    for offset, width, received in parts:
        weights, place = at_peer(0, offset, width)
        if ahead:
            weights = blocks_of_weights[0, offset]
        (kept,) = forward(main, side, weights, place, width, jnp.float32)
        grads = coefficients(kept, received, picks, points, blocks * e)
        jobs.append((grads, offset, width, 0))
        jobs += [(shift(grads, peers, s), offset, width, s) for s in range(1, peers)]
    items = []
    for grads, offset, width, s in jobs:
        weights, place = at_peer(peers - s, offset, width)
        weights = blocks_of_weights[s, offset][:1] if ahead else weights[:2]
        items.append((grads, weights, place))
    if ahead and len(items) == 4:
        groups = [items[:1], items[1:3], items[3:]]
    else:
        groups = [[item] for item in items]
    total = None
    for group in groups[:-1]:
        total = backward(group, total, False)
    spans = [(0, depth // 2), (depth // 2, depth // 2)] if depth % 256 == 0 else [(0, depth)]
    last = [backward(groups[-1], total, pair == 2, span) for span in spans]

    results = []
    for i, value in enumerate(last):
        if pair == 2:
            sent, kept = value
            value = kept + permute(sent, "wide", dims, 2, 1).astype(jnp.float32)
        digits = [(1, 1)] * (near == 2) + [(0, 1 << bit) for bit in range(far.bit_length() - 1)]
        steps = list(digits)
        if i % 2 and len(steps) > 1:
            steps[:2] = steps[1::-1]
        for step in steps:
            at = digits.index(step)
            outer, inner = 1 << at, value.shape[0] >> (at + 1)
            digits.remove(step)

            def half(which):
                rows = [value[(2 * o + which) * inner:(2 * o + which + 1) * inner] for o in range(outer)]
                return rows[0] if outer == 1 else jnp.concatenate(rows)

            got = permute(half(1).astype(jnp.bfloat16), "wide", dims, *step)
            value = half(0) + got.astype(jnp.float32)
        results.append(value.astype(jnp.bfloat16))
    return results[0] if len(results) == 1 else jnp.concatenate(results, axis=1)


def solution(mesh):
    in_specs = (
        P("wide", "narrow"),
        P("wide", "narrow"),
        P("narrow", "wide"),
        P("narrow", "wide"),
        P("wide", "narrow"),
        P("wide", "narrow"),
        P(),
        P(),
    )
    out_specs = P("wide", "narrow")
    return jax.shard_map(on_device, mesh=mesh, in_specs=in_specs, out_specs=out_specs, check_vma=False)
```

```python
import jax
import jax.numpy as jnp
from jax import lax
from jax.experimental import pallas as pl
from jax.experimental.pallas import tpu as pltpu
from jax.sharding import PartitionSpec as P


VMEM = pl.BlockSpec(memory_space=pltpu.VMEM)
SMEM = pl.BlockSpec(memory_space=pltpu.SMEM)
ANY = pl.BlockSpec(memory_space=pl.ANY)


def factors(size):
    pair = 2 if size % 2 == 0 else 1
    near = 2 if (size // pair) % 2 == 0 else 1
    return size // (pair * near), near, pair


def rounded(rows, unit):
    return -(-rows // unit) * unit


def permute(array, axis, dims, digit, amount):
    below = 1
    for size in dims[digit + 1:]:
        below *= size
    total = below
    for size in dims[:digit + 1]:
        total *= size
    pairs = [
        (at, at + (((at // below) % dims[digit] ^ amount) - (at // below) % dims[digit]) * below)
        for at in range(total)
    ]
    return lax.ppermute(array, axis, pairs)


def shift(array, size, amount):
    return lax.ppermute(array, "narrow", [(at, (at + amount) % size) for at in range(size)])


def halvings(size):
    if size == 1:
        return [0]
    return [2 * v for v in halvings(size // 2)] + [2 * v + 1 for v in halvings(size // 2)]


def pack(arrays):
    count, width = sum(a.shape[0] for a in arrays), arrays[0].shape[1]
    whole = count // 8 * 8
    rest = count - whole
    pieces = whole // rest if rest and whole else 1
    cut = rest > 0 and whole > 0 and whole % rest == 0 and width % (pieces * 128) == 0
    if not cut:
        whole, pieces = rounded(count, 8), 1
    lanes = width // pieces

    def body(*refs):
        sources, (out, *held, sems) = refs[:len(arrays)], refs[len(arrays):]
        copies = [
            pltpu.make_async_copy(source, target, sems.at[i])
            for i, (source, target) in enumerate(zip(sources, held))
        ]
        for copy in copies:
            copy.start()
        for copy in copies:
            copy.wait()
        rows = jnp.concatenate([ref[...].astype(jnp.float32) for ref in held])
        if not cut:
            if whole > count:
                rows = jnp.concatenate([rows, jnp.zeros((whole - count, width), jnp.float32)])
            out[...] = rows.astype(out.dtype)
            return
        out[:, pl.ds(0, width)] = rows[:whole].astype(out.dtype)
        beside = [
            rows[whole + i:whole + i + 1, j * lanes:(j + 1) * lanes]
            for i in range(rest)
            for j in range(pieces)
        ]
        out[:, pl.ds(width, lanes)] = jnp.concatenate(beside).astype(out.dtype)

    packed = pl.pallas_call(
        body,
        out_shape=jax.ShapeDtypeStruct((whole, width + lanes if cut else width), arrays[0].dtype),
        in_specs=[ANY] * len(arrays),
        out_specs=VMEM,
        scratch_shapes=[pltpu.VMEM(a.shape, a.dtype) for a in arrays]
        + [pltpu.SemaphoreType.DMA((len(arrays),))],
        compiler_params=pltpu.CompilerParams(vmem_limit_bytes=4 * 1024 * 1024),
        name="pack",
    )(*(pltpu.with_memory_space_constraint(a, pltpu.MemorySpace.HBM) for a in arrays))
    return packed, whole, pieces


def assemble(own, whole, pieces, counts, width):
    blocks = len(own)
    packed = own[0].shape
    total = blocks * sum(counts)
    across_lanes = width // pieces

    def body(*refs):
        out, stack = refs[-2], refs[-1]
        for b in range(blocks):
            stack[pl.ds(b * packed[0], packed[0]), :] = refs[b][...]
        row = lax.broadcasted_iota(jnp.int32, (total, blocks * packed[0]), 0)
        col = lax.broadcasted_iota(jnp.int32, (total, blocks * packed[0]), 1)
        held = jnp.zeros_like(row)
        block = jnp.zeros_like(row)
        at = first = 0
        for count in counts:
            for b in range(blocks):
                inside = (row >= at) & (row < at + count)
                held = jnp.where(inside, row - at + first, held)
                block = jnp.where(inside, b, block)
                at += count
            first += count

        def pick(wanted, valid):
            return (valid & (col == wanted)).astype(jnp.float32).astype(jnp.bfloat16)

        base = block * packed[0]
        uncut = pick(base + held, held < whole)
        for j in range(pieces):
            lanes = pl.ds(j * across_lanes, across_lanes)
            value = jnp.dot(uncut, stack[:, lanes], preferred_element_type=jnp.float32)
            if packed[1] > width:
                value = value + jnp.dot(
                    pick(base + (held - whole) * pieces + j, held >= whole),
                    stack[:, pl.ds(width, across_lanes)],
                    preferred_element_type=jnp.float32,
                )
            out[:, lanes] = value.astype(jnp.bfloat16)

    dtype = own[0].dtype
    return pl.pallas_call(
        body,
        out_shape=jax.ShapeDtypeStruct((total, width), dtype),
        in_specs=[VMEM] * blocks,
        out_specs=VMEM,
        scratch_shapes=[pltpu.VMEM((blocks * packed[0], packed[1]), dtype)],
        compiler_params=pltpu.CompilerParams(vmem_limit_bytes=6 * 1024 * 1024),
        cost_estimate=pl.CostEstimate(flops=10**9, bytes_accessed=10**6, transcendentals=0),
        name="assemble",
    )(*own)


def join(halves, layout):
    width = halves[0].shape[1]
    blocks = halves[0].shape[0] // sum(layout)
    e, r, k = (blocks * rows for rows in layout)
    count = len(halves)

    def body(*refs):
        main, side = refs[-2:]
        for h in range(count):
            main[pl.ds(h * e, e), :] = refs[h][pl.ds(0, e), :]
            main[pl.ds(count * e + h * r, r), :] = refs[h][pl.ds(e, r), :]
            side[pl.ds(h * k, k), :] = refs[h][pl.ds(e + r, k), :]

    dtype = halves[0].dtype
    return pl.pallas_call(
        body,
        out_shape=(
            jax.ShapeDtypeStruct((count * (e + r), width), dtype),
            jax.ShapeDtypeStruct((count * k, width), dtype),
        ),
        in_specs=[VMEM] * count,
        out_specs=(VMEM, VMEM),
        compiler_params=pltpu.CompilerParams(vmem_limit_bytes=4 * 1024 * 1024),
        cost_estimate=pl.CostEstimate(flops=10**9, bytes_accessed=10**6, transcendentals=0),
        name="join",
    )(*halves)


def across(left, right):
    return lax.dot_general(left, right, (((1,), (1,)), ((), ())), preferred_element_type=jnp.float32)


def parts_of(size, unit):
    for count in (4, 2):
        if size % (count * unit) == 0:
            return [(i * (size // count), size // count) for i in range(count)]
    return [(0, size)]


def first_of(place):
    if place is None:
        return 0
    steps, peers, share, offset = place
    return pl.multiple_of((lax.axis_index("narrow") + steps) % peers * share + offset, 128)


def streams(weights, buffers, sems, first, width, by_depth, by_unit):
    gate, up, down = weights
    both, below = buffers
    units, depths = [], []
    for i, (row, count) in enumerate(by_unit if below is not None else ()):
        units.append(
            pltpu.make_async_copy(
                down.at[pl.ds(first + row, count)], below.at[pl.ds(row, count)], sems.at[2, i]
            )
        )
    for i, (row, count) in enumerate(by_depth if both is not None else ()):
        some = pl.ds(row, count)
        depths.append(
            [
                pltpu.make_async_copy(
                    source.at[some, pl.ds(first, width)],
                    both.at[some, pl.ds(w * width, width)],
                    sems.at[w, i],
                )
                for w, source in enumerate((gate, up))
            ]
        )
    return units, depths


def fetch(weights, place, width):
    depth = weights[0].shape[0]
    by_depth, by_unit = parts_of(depth, 128), parts_of(width, 32)

    def body(gate, up, down, both, below, sems):
        first = first_of(place)
        units, depths = streams((gate, up, down), (both, below), sems, first, width, by_depth, by_unit)
        copies = units + [copy for pair in depths for copy in pair]
        for copy in copies:
            copy.start()
        for copy in copies:
            copy.wait()

    return pl.pallas_call(
        body,
        out_shape=(
            pltpu.VMEM((depth, 2 * width), jnp.bfloat16),
            pltpu.VMEM((width, depth), jnp.bfloat16),
        ),
        in_specs=[ANY, ANY, ANY],
        out_specs=(VMEM, VMEM),
        scratch_shapes=[pltpu.SemaphoreType.DMA((3, 4))],
        compiler_params=pltpu.CompilerParams(vmem_limit_bytes=1024 * 1024),
        cost_estimate=pl.CostEstimate(
            flops=4 * 10**9, bytes_accessed=6 * depth * width, transcendentals=0
        ),
        name="fetch",
    )(*weights)


def arriving(next_one, depth):
    _, _, width, both, below = next_one
    return [pltpu.VMEM((depth, 2 * width), jnp.bfloat16)] * both + [
        pltpu.VMEM((width, depth), jnp.bfloat16)
    ] * below


def while_arriving(next_one, depth, sources, targets, sems, work):
    if next_one is None:
        return work()
    _, place, width, both, below = next_one
    targets = list(targets)
    buffers = (targets.pop(0) if both else None, targets.pop(0) if below else None)
    units, depths = streams(
        sources, buffers, sems, first_of(place), width, parts_of(depth, 128), parts_of(width, 32)
    )
    copies = units + [copy for pair in depths for copy in pair]
    for copy in copies:
        copy.start()
    pl.when(lax.axis_index("narrow") >= 0)(work)
    for copy in copies:
        copy.wait()


def forward_half(half, side_rows, weights, width, next_one=None):
    depth = half.shape[1]
    rows = half.shape[0] - side_rows
    top = rounded(-(-side_rows // 2), 8)
    rest = side_rows - top

    def body(half_ref, both, below, *refs):
        sources, (out, *targets) = (refs[:3], refs[3:]) if next_one else ((), refs)
        sems = targets.pop() if next_one else None

        def work():
            out[pl.ds(0, rows), :] = jnp.dot(
                half_ref[pl.ds(0, rows), :], both[...], preferred_element_type=jnp.float32
            ).astype(jnp.bfloat16)
            side = across(half_ref[pl.ds(rows, side_rows), :], below[...]).astype(jnp.bfloat16)
            out[pl.ds(rows, top), pl.ds(0, width)] = side[:top]
            out[pl.ds(rows, rest), pl.ds(width, width)] = side[top:]
            if top > rest:
                out[pl.ds(rows + rest, top - rest), pl.ds(width, width)] = jnp.zeros(
                    (top - rest, width), jnp.bfloat16
                )

        while_arriving(next_one, depth, sources, targets, sems, work)

    more = arriving(next_one, depth) if next_one else []
    return pl.pallas_call(
        body,
        out_shape=[jax.ShapeDtypeStruct((rows + top, 2 * width), jnp.bfloat16)] + more,
        in_specs=[VMEM] * 3 + [ANY] * (3 if next_one else 0),
        out_specs=[VMEM] * (1 + len(more)),
        scratch_shapes=[pltpu.SemaphoreType.DMA((3, 4))] if next_one else [],
        compiler_params=pltpu.CompilerParams(vmem_limit_bytes=4 * 1024 * 1024),
        cost_estimate=pl.CostEstimate(
            flops=4 * depth * width * (rows + side_rows), bytes_accessed=10**6, transcendentals=0
        ),
        name="forward_half",
    )(half, *weights, *(next_one[0] if next_one else ()))


def forward(main, side, weights, place, width, dtype, next_one=None):
    rows, half = main.shape[0], side.shape[0] // 2
    depth = main.shape[1]
    by_depth, by_unit = parts_of(depth, 128), parts_of(width, 32)
    ready = len(weights) == 2

    def put_side(out, value):
        out[pl.ds(rows, half), pl.ds(0, width)] = value[:half].astype(dtype)
        out[pl.ds(rows, half), pl.ds(width, width)] = value[half:].astype(dtype)

    def body_ready(main_ref, side_ref, both, below, *refs):
        sources, (out, *targets) = (refs[:3], refs[3:]) if next_one else ((), refs)
        sems = targets.pop() if next_one else None

        def work():
            out[pl.ds(0, rows), :] = jnp.dot(
                main_ref[...], both[...], preferred_element_type=jnp.float32
            ).astype(dtype)
            put_side(out, across(side_ref[...], below[...]))

        while_arriving(next_one, depth, sources, targets, sems, work)

    def body(main_ref, side_ref, gate, up, down, out, both, below, total, sems):
        first = first_of(place)
        units, depths = streams((gate, up, down), (both, below), sems, first, width, by_depth, by_unit)
        for copy in units + [copy for pair in depths for copy in pair]:
            copy.start()
        for copy in units:
            copy.wait()
        put_side(out, across(side_ref[...], below[...]))
        for i, (row, count) in enumerate(by_depth):
            for copy in depths[i]:
                copy.wait()
            some = pl.ds(row, count)
            part = jnp.dot(main_ref[:, some], both[some, :], preferred_element_type=jnp.float32)
            if i > 0:
                part = total[...] + part
            if i == len(by_depth) - 1:
                out[pl.ds(0, rows), :] = part.astype(dtype)
            else:
                total[...] = part

    out_shape = [jax.ShapeDtypeStruct((rows + half, 2 * width), dtype)]
    operands = [main, side, *weights]
    specs = [VMEM] * 2 + [VMEM if ready else ANY] * len(weights)
    if ready:
        scratch = []
        if next_one is not None:
            operands += next_one[0]
            specs += [ANY] * 3
            out_shape += arriving(next_one, depth)
            scratch = [pltpu.SemaphoreType.DMA((3, 4))]
    else:
        scratch = [
            pltpu.VMEM((depth, 2 * width), jnp.bfloat16),
            pltpu.VMEM((width, depth), jnp.bfloat16),
            pltpu.VMEM((rows, 2 * width), jnp.float32),
            pltpu.SemaphoreType.DMA((3, 4)),
        ]
    return pl.pallas_call(
        body_ready if ready else body,
        out_shape=out_shape,
        in_specs=specs,
        out_specs=[VMEM] * len(out_shape),
        scratch_shapes=scratch,
        compiler_params=pltpu.CompilerParams(vmem_limit_bytes=(4 if ready else 20) * 1024 * 1024),
        cost_estimate=pl.CostEstimate(
            flops=4 * depth * width * (rows + half), bytes_accessed=6 * depth * width, transcendentals=0
        ),
        name="forward",
    )(*operands)


def coefficients(kept, received, picks, points, examples):
    width = kept.shape[1] // 2
    pairs, references = picks.shape[0] // examples, picks.shape[1]
    rows = examples + references
    count = points.shape[0]
    lanes = 128 if width % 128 == 0 else width
    middle = examples // 2
    top = rounded(-(-middle // 2), 8)
    pieces, left = [], middle
    while left:
        size = 16 if left == 16 or left >= 32 else left
        pieces.append((middle - left, size))
        left -= size
    pieces += [(middle + first, size) for first, size in pieces]
    arrays = [array for item in received for array in (item if isinstance(item, tuple) else (item,))]
    scale = 1.0 / (pairs * count)

    def body(points_ref, picks_ref, kept_ref, *refs):
        out, base_gate, base_up = refs[-3:]
        refs = list(refs[:-3])
        got = [
            tuple(refs.pop(0) for _ in item) if isinstance(item, tuple) else refs.pop(0)
            for item in received
        ]
        picks = picks_ref[...]
        steps = [points_ref[m].astype(jnp.float32) * 0.125 for m in range(count)]
        steps_1 = sum(steps[1:], steps[0])
        steps_2 = sum((t * t for t in steps[1:]), steps[0] * steps[0])

        def block(j, _):
            if lanes == width:
                of = [pl.ds(w * width, width) for w in range(2)]
            else:
                of = [pl.ds(pl.multiple_of(w * width + j * lanes, 128), lanes) for w in range(2)]

            def of_references(ref, w):
                if isinstance(ref, tuple):
                    return jnp.concatenate([half[pl.ds(0, references // 2), of[w]] for half in ref])
                return ref[pl.ds(0, references), of[w]]

            def of_examples(ref, first, size, w):
                if isinstance(ref, tuple):
                    h = first // middle
                    return ref[h][pl.ds(references // 2 + first - h * middle, size), of[w]]
                return ref[pl.ds(references + first, size), of[w]]

            def of_upstream(ref, h):
                if isinstance(ref, tuple):
                    return jnp.concatenate(
                        [ref[h][pl.ds(rows // 2, top), of[0]], ref[h][pl.ds(rows // 2, middle - top), of[1]]]
                    )
                return ref[pl.ds(rows, middle), of[h]]

            def total(take, *where):
                value = take(kept_ref, *where)
                for ref in got:
                    value = value + take(ref, *where).astype(jnp.float32)
                return value

            for w, target in enumerate((base_gate, base_up)):
                value = total(of_references, w)
                high = value.astype(jnp.bfloat16)
                low = (value - high.astype(jnp.float32)).astype(jnp.bfloat16)
                target[...] = jnp.dot(picks, high, preferred_element_type=jnp.float32) + jnp.dot(
                    picks, low, preferred_element_type=jnp.float32
                )
            upstream = [total(of_upstream, h) for h in range(2)]
            for first, piece in pieces:
                gate = total(of_examples, first, piece, 0) * 0.5
                up = total(of_examples, first, piece, 1)
                coef_gate = jnp.zeros_like(gate)
                coef_up = jnp.zeros_like(gate)
                for p in range(pairs):
                    start = base_gate[pl.ds(p * examples + first, piece), :] * 0.5
                    span = gate - start
                    flat = count + (count * start + steps_1 * span)
                    tilted = steps_1 + (steps_1 * start + steps_2 * span)
                    coef_up = coef_up + (count * start + steps_1 * span)
                    for t in steps:
                        half = start + t * span
                        v = jnp.tanh(half)
                        bent = half * v
                        turn = v - v * bent
                        coef_up = coef_up + bent
                        flat = flat + turn
                        tilted = tilted + t * turn
                    start_up = base_up[pl.ds(p * examples + first, piece), :]
                    coef_gate = coef_gate + (start_up * flat + (up - start_up) * tilted)
                base_gate[pl.ds(first, piece), :] = coef_gate * (0.5 * scale)
                base_up[pl.ds(first, piece), :] = coef_up * scale
            for w, source in enumerate((base_gate, base_up)):
                for h in range(2):
                    some = pl.ds(h * middle, middle)
                    out[some, of[w]] = (upstream[h] * source[some, :]).astype(jnp.bfloat16)
            return 0

        lax.fori_loop(0, width // lanes, block, 0)

    return pl.pallas_call(
        body,
        out_shape=jax.ShapeDtypeStruct((examples, 2 * width), jnp.bfloat16),
        in_specs=[SMEM, VMEM, VMEM] + [VMEM] * len(arrays),
        out_specs=VMEM,
        scratch_shapes=[pltpu.VMEM((pairs * examples, lanes), jnp.float32)] * 2,
        compiler_params=pltpu.CompilerParams(vmem_limit_bytes=4 * 1024 * 1024),
        cost_estimate=pl.CostEstimate(flops=5 * 10**9, bytes_accessed=10**6, transcendentals=0),
        name="coefficients",
    )(points, picks, kept, *arrays)


def backward(items, total, final, span=None):
    grads, weights, place = items[0]
    rows, width, depth = grads.shape[0], grads.shape[1] // 2, weights[0].shape[0]
    low, columns = span or (0, depth)
    by_depth = [(low + row, count) for row, count in parts_of(columns, 128)]
    ready = len(weights) == 1

    def body(*refs):
        grads_refs, refs = refs[:len(items)], refs[len(items):]
        if ready:
            boths, outs = refs[:len(items)], refs[len(items):]
        else:
            gate, up, *outs, both, sems = refs
            boths = [both]
            _, depths = streams((gate, up, None), (both, None), sems, first_of(place), width, by_depth, [])
            for pair in depths:
                for copy in pair:
                    copy.start()
        for i, (row, count) in enumerate(by_depth):
            some, own = pl.ds(row, count), pl.ds(row - low, count)
            if not ready:
                for copy in depths[i]:
                    copy.wait()
            value = None if total is None else outs[0][:, some]
            for grads_ref, both in zip(grads_refs, boths):
                part = across(grads_ref[...], both[some, :])
                value = part if value is None else value + part
            if final:
                outs[-2][:, own] = value[rows // 2:, :].astype(jnp.bfloat16)
                outs[-1][:, own] = value[:rows // 2, :]
            else:
                outs[-1][:, own] = value

    operands = [item[0] for item in items] + [w for item in items for w in item[1]]
    specs = [VMEM] * len(items) + [VMEM if ready else ANY] * (len(operands) - len(items))
    if total is not None:
        operands.append(total)
        specs.append(VMEM)
    if final:
        out_shape = (
            jax.ShapeDtypeStruct((rows // 2, columns), jnp.bfloat16),
            jax.ShapeDtypeStruct((rows // 2, columns), jnp.float32),
        )
        out_specs = (VMEM, VMEM)
    else:
        out_shape, out_specs = jax.ShapeDtypeStruct((rows, columns), jnp.float32), VMEM
    scratch = [pltpu.VMEM((depth, 2 * width), jnp.bfloat16), pltpu.SemaphoreType.DMA((2, 4))]
    return pl.pallas_call(
        body,
        out_shape=out_shape,
        in_specs=specs,
        out_specs=out_specs,
        scratch_shapes=[] if ready else scratch,
        compiler_params=pltpu.CompilerParams(vmem_limit_bytes=(4 if ready else 12) * 1024 * 1024),
        cost_estimate=pl.CostEstimate(
            flops=2 * rows * columns * sum(item[0].shape[1] for item in items),
            bytes_accessed=4 * width * columns,
            transcendentals=0,
        ),
        name="backward",
    )(*operands)


def choices(pair_ref, dims, e, r):
    far, near, pair = dims
    blocks = far * near * pair
    examples, pairs = pair_ref.shape

    def body(pair_ref, out, rows):
        at = lax.axis_index("wide")
        z, y, c = at // (near * pair), at // pair % near, at % pair
        col = lax.broadcasted_iota(jnp.int32, (examples, blocks * r), 1)
        name = jnp.zeros_like(col)
        for q in range(blocks):
            s, b, p = halvings(far)[q % far], q // far % near, q // (far * near)
            owner = ((z ^ s) * near + (y ^ b)) * pair + (c ^ p)
            rows[pl.ds(q * e, e), :] = pair_ref[pl.ds(owner * e, e), :]
            name = jnp.where((col >= q * r) & (col < (q + 1) * r), owner * r + col - q * r, name)
        for p in range(pairs):
            out[pl.ds(p * examples, examples), :] = (
                (rows[:, pl.ds(p, 1)] == name).astype(jnp.float32).astype(jnp.bfloat16)
            )

    return pl.pallas_call(
        body,
        out_shape=jax.ShapeDtypeStruct((pairs * examples, blocks * r), jnp.bfloat16),
        in_specs=[VMEM],
        out_specs=VMEM,
        scratch_shapes=[pltpu.VMEM((examples, pairs), jnp.int32)],
        compiler_params=pltpu.CompilerParams(vmem_limit_bytes=2 * 1024 * 1024),
        cost_estimate=pl.CostEstimate(flops=10**9, bytes_accessed=10**6, transcendentals=0),
        name="choices",
    )(pair_ref)


def chunks_of(width):
    if width % 128 or width < 512:
        return [(0, rounded(width, 128))]
    first = rounded(width // 2, 256)
    return [(0, first), (first, width - first)]


def on_device(
    examples, references, gate_weight, up_weight, down_weight, cotangent, pair_ref, points
):
    dims = factors(lax.axis_size("wide"))
    far, near, pair = dims
    peers = lax.axis_size("narrow")
    e, r, k = examples.shape[0], references.shape[0], cotangent.shape[0]
    depth, hidden = gate_weight.shape
    blocks = far * near * pair

    share = hidden // peers
    whole_weights = [gate_weight, up_weight, down_weight]
    aligned = share % 128 == 0
    ahead = aligned and peers == 2
    if aligned:
        whole_weights = [
            pltpu.with_memory_space_constraint(w, pltpu.MemorySpace.HBM) for w in whole_weights
        ]
    chunks = chunks_of(share)
    picks = choices(pair_ref, dims, e, r)

    def at_peer(steps, offset, width):
        if aligned:
            return whole_weights, (steps % peers, peers, share, offset)
        start = (lax.axis_index("narrow") + steps) % peers * share
        more = width - share

        def cut(weight, axis):
            piece = lax.dynamic_slice_in_dim(weight, start, share, axis)
            return jnp.pad(piece, [(0, more if d == axis else 0) for d in range(2)])

        return [cut(gate_weight, 1), cut(up_weight, 1), cut(down_weight, 0)], None

    own, whole, pieces = pack([references, examples, cotangent])
    column = {0: own}
    step = far // 2
    while step:
        for s in sorted(column):
            column[s + step] = permute(column[s], "wide", dims, 0, step)
        step //= 2
    beside = {}
    if near == 2:
        for s, block in column.items():
            beside[s] = permute(block, "wide", dims, 1, 1)
    order = halvings(far)
    plane = [column[s] for s in order] + [beside[s] for s in order if near == 2]
    half = assemble(plane, whole, pieces, (r, e, k), depth)
    blocks_of_weights = {}
    early = ahead and pair == 2 and len(chunks) == 2
    if ahead:
        wanted = [(1, chunk) for chunk in chunks] + [(0, chunk) for chunk in chunks[1 if early else 0:]]
        for s, chunk in wanted:
            blocks_of_weights[s, chunk[0]] = fetch(*at_peer(s, *chunk), chunk[1])
    halves = [half]
    if pair == 2:
        halves.append(permute(half, "wide", dims, 2, 1))

    parts = []
    if early:
        (offset, width), (next_offset, next_width) = chunks
        weights = blocks_of_weights[1, offset]
        count = half.shape[0] // (r + e + k) * k
        kept_one = (*at_peer(0, offset, width), width)
        (sent,) = forward_half(halves[0], count, weights, width)
        received = [shift(sent, peers, 1)]
        sent, both = forward_half(halves[1], count, weights, width, (*kept_one, True, False))
        received.append(shift(sent, peers, 1))
        parts.append((offset, width, [tuple(received)]))
    main, side = join(halves, (r, e, k))
    if early:
        sent, below = forward(
            main, side, blocks_of_weights[1, next_offset], None, next_width, jnp.bfloat16,
            (*kept_one, False, True),
        )
        parts.append((next_offset, next_width, [shift(sent, peers, 1)]))
        blocks_of_weights[0, offset] = (both, below)
    else:
        for offset, width in chunks:
            received = []
            for s in range(1, peers):
                weights, place = at_peer(s, offset, width)
                if ahead:
                    weights = blocks_of_weights[s, offset]
                (sent,) = forward(main, side, weights, place, width, jnp.bfloat16)
                received.append(shift(sent, peers, s))
            parts.append((offset, width, received))

    jobs = []
    for offset, width, received in parts:
        weights, place = at_peer(0, offset, width)
        if ahead:
            weights = blocks_of_weights[0, offset]
        (kept,) = forward(main, side, weights, place, width, jnp.float32)
        grads = coefficients(kept, received, picks, points, blocks * e)
        jobs.append((grads, offset, width, 0))
        jobs += [(shift(grads, peers, s), offset, width, s) for s in range(1, peers)]
    items = []
    for grads, offset, width, s in jobs:
        weights, place = at_peer(peers - s, offset, width)
        weights = blocks_of_weights[s, offset][:1] if ahead else weights[:2]
        items.append((grads, weights, place))
    if ahead and len(items) == 4:
        groups = [items[:1], items[1:3], items[3:]]
    else:
        groups = [[item] for item in items]
    total = None
    for group in groups[:-1]:
        total = backward(group, total, False)
    spans = [(0, depth // 2), (depth // 2, depth // 2)] if depth % 256 == 0 else [(0, depth)]
    last = [backward(groups[-1], total, pair == 2, span) for span in spans]

    results = []
    for i, value in enumerate(last):
        if pair == 2:
            sent, kept = value
            value = kept + permute(sent, "wide", dims, 2, 1).astype(jnp.float32)
        digits = [(1, 1)] * (near == 2) + [(0, 1 << bit) for bit in range(far.bit_length() - 1)]
        steps = list(digits)
        if i % 2 and len(steps) > 1:
            steps[:2] = steps[1::-1]
        for step in steps:
            at = digits.index(step)
            outer, inner = 1 << at, value.shape[0] >> (at + 1)
            digits.remove(step)

            def half(which):
                rows = [value[(2 * o + which) * inner:(2 * o + which + 1) * inner] for o in range(outer)]
                return rows[0] if outer == 1 else jnp.concatenate(rows)

            got = permute(half(1).astype(jnp.bfloat16), "wide", dims, *step)
            value = half(0) + got.astype(jnp.float32)
        results.append(value.astype(jnp.bfloat16))
    return results[0] if len(results) == 1 else jnp.concatenate(results, axis=1)


def solution(mesh):
    in_specs = (
        P("wide", "narrow"),
        P("wide", "narrow"),
        P("narrow", "wide"),
        P("narrow", "wide"),
        P("wide", "narrow"),
        P("wide", "narrow"),
        P(),
        P(),
    )
    out_specs = P("wide", "narrow")
    return jax.shard_map(on_device, mesh=mesh, in_specs=in_specs, out_specs=out_specs, check_vma=False)
```

```python
import jax
import jax.numpy as jnp
from jax import lax
from jax.experimental import pallas as pl
from jax.experimental.pallas import tpu as pltpu
from jax.sharding import PartitionSpec as P


VMEM = pl.BlockSpec(memory_space=pltpu.VMEM)
SMEM = pl.BlockSpec(memory_space=pltpu.SMEM)
ANY = pl.BlockSpec(memory_space=pl.ANY)


def factors(size):
    pair = 2 if size % 2 == 0 else 1
    near = 2 if (size // pair) % 2 == 0 else 1
    return size // (pair * near), near, pair


def rounded(rows, unit):
    return -(-rows // unit) * unit


def permute(array, axis, dims, digit, amount):
    below = 1
    for size in dims[digit + 1:]:
        below *= size
    total = below
    for size in dims[:digit + 1]:
        total *= size
    pairs = [
        (at, at + (((at // below) % dims[digit] ^ amount) - (at // below) % dims[digit]) * below)
        for at in range(total)
    ]
    return lax.ppermute(array, axis, pairs)


def shift(array, size, amount):
    return lax.ppermute(array, "narrow", [(at, (at + amount) % size) for at in range(size)])


def halvings(size):
    if size == 1:
        return [0]
    return [2 * v for v in halvings(size // 2)] + [2 * v + 1 for v in halvings(size // 2)]


def pack(arrays):
    count, width = sum(a.shape[0] for a in arrays), arrays[0].shape[1]
    whole = count // 8 * 8
    rest = count - whole
    pieces = whole // rest if rest and whole else 1
    cut = rest > 0 and whole > 0 and whole % rest == 0 and width % (pieces * 128) == 0
    if not cut:
        whole, pieces = rounded(count, 8), 1
    lanes = width // pieces

    def body(*refs):
        sources, (out, *held, sems) = refs[:len(arrays)], refs[len(arrays):]
        copies = [
            pltpu.make_async_copy(source, target, sems.at[i])
            for i, (source, target) in enumerate(zip(sources, held))
        ]
        for copy in copies:
            copy.start()
        for copy in copies:
            copy.wait()
        rows = jnp.concatenate([ref[...].astype(jnp.float32) for ref in held])
        if not cut:
            if whole > count:
                rows = jnp.concatenate([rows, jnp.zeros((whole - count, width), jnp.float32)])
            out[...] = rows.astype(out.dtype)
            return
        out[:, pl.ds(0, width)] = rows[:whole].astype(out.dtype)
        beside = [
            rows[whole + i:whole + i + 1, j * lanes:(j + 1) * lanes]
            for i in range(rest)
            for j in range(pieces)
        ]
        out[:, pl.ds(width, lanes)] = jnp.concatenate(beside).astype(out.dtype)

    packed = pl.pallas_call(
        body,
        out_shape=jax.ShapeDtypeStruct((whole, width + lanes if cut else width), arrays[0].dtype),
        in_specs=[ANY] * len(arrays),
        out_specs=VMEM,
        scratch_shapes=[pltpu.VMEM(a.shape, a.dtype) for a in arrays]
        + [pltpu.SemaphoreType.DMA((len(arrays),))],
        compiler_params=pltpu.CompilerParams(vmem_limit_bytes=4 * 1024 * 1024),
        name="pack",
    )(*(pltpu.with_memory_space_constraint(a, pltpu.MemorySpace.HBM) for a in arrays))
    return packed, whole, pieces


def assemble(own, whole, pieces, counts, width):
    blocks = len(own)
    packed = own[0].shape
    total = blocks * sum(counts)
    across_lanes = width // pieces

    def body(*refs):
        out, stack = refs[-2], refs[-1]
        for b in range(blocks):
            stack[pl.ds(b * packed[0], packed[0]), :] = refs[b][...]
        row = lax.broadcasted_iota(jnp.int32, (total, blocks * packed[0]), 0)
        col = lax.broadcasted_iota(jnp.int32, (total, blocks * packed[0]), 1)
        held = jnp.zeros_like(row)
        block = jnp.zeros_like(row)
        at = first = 0
        for count in counts:
            for b in range(blocks):
                inside = (row >= at) & (row < at + count)
                held = jnp.where(inside, row - at + first, held)
                block = jnp.where(inside, b, block)
                at += count
            first += count

        def pick(wanted, valid):
            return (valid & (col == wanted)).astype(jnp.float32).astype(jnp.bfloat16)

        base = block * packed[0]
        uncut = pick(base + held, held < whole)
        for j in range(pieces):
            lanes = pl.ds(j * across_lanes, across_lanes)
            value = jnp.dot(uncut, stack[:, lanes], preferred_element_type=jnp.float32)
            if packed[1] > width:
                value = value + jnp.dot(
                    pick(base + (held - whole) * pieces + j, held >= whole),
                    stack[:, pl.ds(width, across_lanes)],
                    preferred_element_type=jnp.float32,
                )
            out[:, lanes] = value.astype(jnp.bfloat16)

    dtype = own[0].dtype
    return pl.pallas_call(
        body,
        out_shape=jax.ShapeDtypeStruct((total, width), dtype),
        in_specs=[VMEM] * blocks,
        out_specs=VMEM,
        scratch_shapes=[pltpu.VMEM((blocks * packed[0], packed[1]), dtype)],
        compiler_params=pltpu.CompilerParams(vmem_limit_bytes=6 * 1024 * 1024),
        cost_estimate=pl.CostEstimate(flops=10**9, bytes_accessed=10**6, transcendentals=0),
        name="assemble",
    )(*own)


def join(halves, layout):
    width = halves[0].shape[1]
    blocks = halves[0].shape[0] // sum(layout)
    e, r, k = (blocks * rows for rows in layout)
    count = len(halves)

    def body(*refs):
        main, side = refs[-2:]
        for h in range(count):
            main[pl.ds(h * e, e), :] = refs[h][pl.ds(0, e), :]
            main[pl.ds(count * e + h * r, r), :] = refs[h][pl.ds(e, r), :]
            side[pl.ds(h * k, k), :] = refs[h][pl.ds(e + r, k), :]

    dtype = halves[0].dtype
    return pl.pallas_call(
        body,
        out_shape=(
            jax.ShapeDtypeStruct((count * (e + r), width), dtype),
            jax.ShapeDtypeStruct((count * k, width), dtype),
        ),
        in_specs=[VMEM] * count,
        out_specs=(VMEM, VMEM),
        compiler_params=pltpu.CompilerParams(vmem_limit_bytes=4 * 1024 * 1024),
        cost_estimate=pl.CostEstimate(flops=10**9, bytes_accessed=10**6, transcendentals=0),
        name="join",
    )(*halves)


def across(left, right):
    return lax.dot_general(left, right, (((1,), (1,)), ((), ())), preferred_element_type=jnp.float32)


def parts_of(size, unit):
    for count in (4, 2):
        if size % (count * unit) == 0:
            return [(i * (size // count), size // count) for i in range(count)]
    return [(0, size)]


def first_of(place):
    if place is None:
        return 0
    steps, peers, share, offset = place
    return pl.multiple_of((lax.axis_index("narrow") + steps) % peers * share + offset, 128)


def streams(weights, buffers, sems, first, width, by_depth, by_unit):
    gate, up, down = weights
    both, below = buffers
    units, depths = [], []
    for i, (row, count) in enumerate(by_unit if below is not None else ()):
        units.append(
            pltpu.make_async_copy(
                down.at[pl.ds(first + row, count)], below.at[pl.ds(row, count)], sems.at[2, i]
            )
        )
    for i, (row, count) in enumerate(by_depth if both is not None else ()):
        some = pl.ds(row, count)
        depths.append(
            [
                pltpu.make_async_copy(
                    source.at[some, pl.ds(first, width)],
                    both.at[some, pl.ds(w * width, width)],
                    sems.at[w, i],
                )
                for w, source in enumerate((gate, up))
            ]
        )
    return units, depths


def fetch(weights, place, width):
    depth = weights[0].shape[0]
    by_depth, by_unit = parts_of(depth, 128), parts_of(width, 32)

    def body(gate, up, down, both, below, sems):
        first = first_of(place)
        units, depths = streams((gate, up, down), (both, below), sems, first, width, by_depth, by_unit)
        copies = units + [copy for pair in depths for copy in pair]
        for copy in copies:
            copy.start()
        for copy in copies:
            copy.wait()

    return pl.pallas_call(
        body,
        out_shape=(
            pltpu.VMEM((depth, 2 * width), jnp.bfloat16),
            pltpu.VMEM((width, depth), jnp.bfloat16),
        ),
        in_specs=[ANY, ANY, ANY],
        out_specs=(VMEM, VMEM),
        scratch_shapes=[pltpu.SemaphoreType.DMA((3, 4))],
        compiler_params=pltpu.CompilerParams(vmem_limit_bytes=1024 * 1024),
        cost_estimate=pl.CostEstimate(
            flops=4 * 10**9, bytes_accessed=6 * depth * width, transcendentals=0
        ),
        name="fetch",
    )(*weights)


def arriving(next_one, depth):
    _, _, width, span, below, _ = next_one
    return [pltpu.VMEM((depth, 2 * width), jnp.bfloat16)] * (span is not None) + [
        pltpu.VMEM((width, depth), jnp.bfloat16)
    ] * below


def extras(next_one, depth, at):
    if next_one is None:
        return [], [], [], [], {}
    weights, _, _, _, _, into = next_one
    more = arriving(next_one, depth)
    scratch = [pltpu.SemaphoreType.DMA((3, 4))]
    if into is None:
        return [*weights], [ANY] * 3, more, scratch, {}
    return [*weights, into], [ANY] * 3 + [VMEM], more, scratch, {at + 3: 1}


def while_arriving(next_one, refs, work):
    if next_one is None:
        return work(refs[0])
    _, place, width, span, below, into = next_one
    sources, (out, *targets, sems) = refs[:3], refs[3 + (into is not None):]
    buffers = (targets.pop(0) if span else None, targets.pop(0) if below else None)
    first, count = span or (0, 0)
    units, depths = streams(
        sources,
        buffers,
        sems,
        first_of(place),
        width,
        [(first + row, rows) for row, rows in parts_of(count, 128)] if span else [],
        parts_of(width, 32),
    )
    copies = units + [copy for pair in depths for copy in pair]
    for copy in copies:
        copy.start()
    pl.when(lax.axis_index("narrow") >= 0)(lambda: work(out))
    for copy in copies:
        copy.wait()


def forward_half(half, side_rows, weights, width, next_one=None):
    depth = half.shape[1]
    rows = half.shape[0] - side_rows
    top = rounded(-(-side_rows // 2), 8)
    rest = side_rows - top

    def body(half_ref, both, below, *refs):
        def work(out):
            out[pl.ds(0, rows), :] = jnp.dot(
                half_ref[pl.ds(0, rows), :], both[...], preferred_element_type=jnp.float32
            ).astype(jnp.bfloat16)
            side = across(half_ref[pl.ds(rows, side_rows), :], below[...]).astype(jnp.bfloat16)
            out[pl.ds(rows, top), pl.ds(0, width)] = side[:top]
            out[pl.ds(rows, rest), pl.ds(width, width)] = side[top:]
            if top > rest:
                out[pl.ds(rows + rest, top - rest), pl.ds(width, width)] = jnp.zeros(
                    (top - rest, width), jnp.bfloat16
                )

        while_arriving(next_one, refs, work)

    operands, specs, more, scratch, aliases = extras(next_one, depth, 3)
    return pl.pallas_call(
        body,
        out_shape=[jax.ShapeDtypeStruct((rows + top, 2 * width), jnp.bfloat16)] + more,
        in_specs=[VMEM] * 3 + specs,
        out_specs=[VMEM] * (1 + len(more)),
        scratch_shapes=scratch,
        input_output_aliases=aliases,
        compiler_params=pltpu.CompilerParams(vmem_limit_bytes=4 * 1024 * 1024),
        cost_estimate=pl.CostEstimate(
            flops=4 * depth * width * (rows + side_rows), bytes_accessed=10**6, transcendentals=0
        ),
        name="forward_half",
    )(half, *weights, *operands)


def forward(main, side, weights, place, width, dtype, next_one=None):
    rows, half = main.shape[0], side.shape[0] // 2
    depth = main.shape[1]
    by_depth, by_unit = parts_of(depth, 128), parts_of(width, 32)
    ready = len(weights) == 2

    def put_side(out, value):
        out[pl.ds(rows, half), pl.ds(0, width)] = value[:half].astype(dtype)
        out[pl.ds(rows, half), pl.ds(width, width)] = value[half:].astype(dtype)

    def body_ready(main_ref, side_ref, both, below, *refs):
        def work(out):
            out[pl.ds(0, rows), :] = jnp.dot(
                main_ref[...], both[...], preferred_element_type=jnp.float32
            ).astype(dtype)
            put_side(out, across(side_ref[...], below[...]))

        while_arriving(next_one, refs, work)

    def body(main_ref, side_ref, gate, up, down, out, both, below, total, sems):
        first = first_of(place)
        units, depths = streams((gate, up, down), (both, below), sems, first, width, by_depth, by_unit)
        for copy in units + [copy for pair in depths for copy in pair]:
            copy.start()
        for copy in units:
            copy.wait()
        put_side(out, across(side_ref[...], below[...]))
        for i, (row, count) in enumerate(by_depth):
            for copy in depths[i]:
                copy.wait()
            some = pl.ds(row, count)
            part = jnp.dot(main_ref[:, some], both[some, :], preferred_element_type=jnp.float32)
            if i > 0:
                part = total[...] + part
            if i == len(by_depth) - 1:
                out[pl.ds(0, rows), :] = part.astype(dtype)
            else:
                total[...] = part

    out_shape = [jax.ShapeDtypeStruct((rows + half, 2 * width), dtype)]
    operands = [main, side, *weights]
    specs = [VMEM] * 2 + [VMEM if ready else ANY] * len(weights)
    aliases = {}
    if ready:
        operands_more, specs_more, more, scratch, aliases = extras(next_one, depth, 4)
        operands += operands_more
        specs += specs_more
        out_shape += more
    else:
        scratch = [
            pltpu.VMEM((depth, 2 * width), jnp.bfloat16),
            pltpu.VMEM((width, depth), jnp.bfloat16),
            pltpu.VMEM((rows, 2 * width), jnp.float32),
            pltpu.SemaphoreType.DMA((3, 4)),
        ]
    return pl.pallas_call(
        body_ready if ready else body,
        out_shape=out_shape,
        in_specs=specs,
        out_specs=[VMEM] * len(out_shape),
        scratch_shapes=scratch,
        input_output_aliases=aliases,
        compiler_params=pltpu.CompilerParams(vmem_limit_bytes=(4 if ready else 20) * 1024 * 1024),
        cost_estimate=pl.CostEstimate(
            flops=4 * depth * width * (rows + half), bytes_accessed=6 * depth * width, transcendentals=0
        ),
        name="forward",
    )(*operands)


def coefficients(kept, received, picks, points, examples):
    width = kept.shape[1] // 2
    pairs, references = picks.shape[0] // examples, picks.shape[1] // 2
    rows = examples + references
    count = points.shape[0]
    lanes = 128 if width % 128 == 0 else width
    middle = examples // 2
    top = rounded(-(-middle // 2), 8)
    pieces, left = [], middle
    while left:
        size = 16 if left == 16 or left >= 32 else left
        pieces.append((middle - left, size))
        left -= size
    pieces += [(middle + first, size) for first, size in pieces]
    arrays = [array for item in received for array in (item if isinstance(item, tuple) else (item,))]
    scale = 1.0 / (pairs * count)

    def body(points_ref, picks_ref, kept_ref, *refs):
        out, base_gate, base_up = refs[-3:]
        refs = list(refs[:-3])
        got = [
            tuple(refs.pop(0) for _ in item) if isinstance(item, tuple) else refs.pop(0)
            for item in received
        ]
        picks = picks_ref[...]
        steps = [points_ref[m].astype(jnp.float32) * 0.125 for m in range(count)]
        steps_1 = sum(steps[1:], steps[0])
        steps_2 = sum((t * t for t in steps[1:]), steps[0] * steps[0])

        def total(take, *where):
            value = take(kept_ref, *where)
            for ref in got:
                value = value + take(ref, *where).astype(jnp.float32)
            return value

        def of_references(ref, lanes_of):
            if isinstance(ref, tuple):
                return jnp.concatenate([half[pl.ds(0, references // 2), lanes_of] for half in ref])
            return ref[pl.ds(0, references), lanes_of]

        for w, target in enumerate((base_gate, base_up)):
            value = total(of_references, pl.ds(w * width, width))
            high = value.astype(jnp.bfloat16)
            low = (value - high.astype(jnp.float32)).astype(jnp.bfloat16)
            target[...] = jnp.dot(
                picks, jnp.concatenate([high, low]), preferred_element_type=jnp.float32
            )

        def block(j, _):
            here = pl.ds(0, width) if lanes == width else pl.ds(pl.multiple_of(j * lanes, 128), lanes)
            if lanes == width:
                of = [pl.ds(w * width, width) for w in range(2)]
            else:
                of = [pl.ds(pl.multiple_of(w * width + j * lanes, 128), lanes) for w in range(2)]

            def of_examples(ref, first, size, w):
                if isinstance(ref, tuple):
                    h = first // middle
                    return ref[h][pl.ds(references // 2 + first - h * middle, size), of[w]]
                return ref[pl.ds(references + first, size), of[w]]

            def of_upstream(ref, h):
                if isinstance(ref, tuple):
                    return jnp.concatenate(
                        [ref[h][pl.ds(rows // 2, top), of[0]], ref[h][pl.ds(rows // 2, middle - top), of[1]]]
                    )
                return ref[pl.ds(rows, middle), of[h]]

            upstream = [total(of_upstream, h) for h in range(2)]
            for first, piece in pieces:
                gate = total(of_examples, first, piece, 0) * 0.5
                up = total(of_examples, first, piece, 1)
                coef_gate = jnp.zeros_like(gate)
                coef_up = jnp.zeros_like(gate)
                for p in range(pairs):
                    start = base_gate[pl.ds(p * examples + first, piece), here] * 0.5
                    span = gate - start
                    flat = count + (count * start + steps_1 * span)
                    tilted = steps_1 + (steps_1 * start + steps_2 * span)
                    coef_up = coef_up + (count * start + steps_1 * span)
                    for t in steps:
                        half = start + t * span
                        v = jnp.tanh(half)
                        bent = half * v
                        turn = v - v * bent
                        coef_up = coef_up + bent
                        flat = flat + turn
                        tilted = tilted + t * turn
                    start_up = base_up[pl.ds(p * examples + first, piece), here]
                    coef_gate = coef_gate + (start_up * flat + (up - start_up) * tilted)
                base_gate[pl.ds(first, piece), here] = coef_gate * (0.5 * scale)
                base_up[pl.ds(first, piece), here] = coef_up * scale
            for w, source in enumerate((base_gate, base_up)):
                for h in range(2):
                    some = pl.ds(h * middle, middle)
                    out[some, of[w]] = (upstream[h] * source[some, here]).astype(jnp.bfloat16)
            return 0

        lax.fori_loop(0, width // lanes, block, 0)

    return pl.pallas_call(
        body,
        out_shape=jax.ShapeDtypeStruct((examples, 2 * width), jnp.bfloat16),
        in_specs=[SMEM, VMEM, VMEM] + [VMEM] * len(arrays),
        out_specs=VMEM,
        scratch_shapes=[pltpu.VMEM((pairs * examples, width), jnp.float32)] * 2,
        compiler_params=pltpu.CompilerParams(vmem_limit_bytes=4 * 1024 * 1024),
        cost_estimate=pl.CostEstimate(flops=5 * 10**9, bytes_accessed=10**6, transcendentals=0),
        name="coefficients",
    )(points, picks, kept, *arrays)


def backward(items, total, final, span=None):
    grads, weights, place = items[0]
    rows, width, depth = grads.shape[0], grads.shape[1] // 2, weights[0].shape[0]
    low, columns = span or (0, depth)
    by_depth = [(low + row, count) for row, count in (parts_of(columns, 128) if len(weights) > 1 else [(0, columns)])]
    ready = len(weights) == 1

    def body(*refs):
        grads_refs, refs = refs[:len(items)], refs[len(items):]
        if ready:
            boths, outs = refs[:len(items)], refs[len(items):]
        else:
            gate, up, *outs, both, sems = refs
            boths = [both]
            _, depths = streams((gate, up, None), (both, None), sems, first_of(place), width, by_depth, [])
            for pair in depths:
                for copy in pair:
                    copy.start()
        for i, (row, count) in enumerate(by_depth):
            some, own = pl.ds(row, count), pl.ds(row - low, count)
            if not ready:
                for copy in depths[i]:
                    copy.wait()
            value = None if total is None else outs[0][:, some]
            for grads_ref, both in zip(grads_refs, boths):
                part = across(grads_ref[...], both[some, :])
                value = part if value is None else value + part
            if final:
                outs[-2][:, own] = value[rows // 2:, :].astype(jnp.bfloat16)
                outs[-1][:, own] = value[:rows // 2, :]
            else:
                outs[-1][:, own] = value

    operands = [item[0] for item in items] + [w for item in items for w in item[1]]
    specs = [VMEM] * len(items) + [VMEM if ready else ANY] * (len(operands) - len(items))
    if total is not None:
        operands.append(total)
        specs.append(VMEM)
    if final:
        out_shape = (
            jax.ShapeDtypeStruct((rows // 2, columns), jnp.bfloat16),
            jax.ShapeDtypeStruct((rows // 2, columns), jnp.float32),
        )
        out_specs = (VMEM, VMEM)
    else:
        out_shape, out_specs = jax.ShapeDtypeStruct((rows, columns), jnp.float32), VMEM
    scratch = [pltpu.VMEM((depth, 2 * width), jnp.bfloat16), pltpu.SemaphoreType.DMA((2, 4))]
    return pl.pallas_call(
        body,
        out_shape=out_shape,
        in_specs=specs,
        out_specs=out_specs,
        scratch_shapes=[] if ready else scratch,
        compiler_params=pltpu.CompilerParams(vmem_limit_bytes=(4 if ready else 12) * 1024 * 1024),
        cost_estimate=pl.CostEstimate(
            flops=2 * rows * columns * sum(item[0].shape[1] for item in items),
            bytes_accessed=4 * width * columns,
            transcendentals=0,
        ),
        name="backward",
    )(*operands)


def choices(pair_ref, dims, e, r):
    far, near, pair = dims
    blocks = far * near * pair
    examples, pairs = pair_ref.shape

    def body(pair_ref, out, rows):
        at = lax.axis_index("wide")
        z, y, c = at // (near * pair), at // pair % near, at % pair
        col = lax.broadcasted_iota(jnp.int32, (examples, blocks * r), 1)
        name = jnp.zeros_like(col)
        for q in range(blocks):
            s, b, p = halvings(far)[q % far], q // far % near, q // (far * near)
            owner = ((z ^ s) * near + (y ^ b)) * pair + (c ^ p)
            rows[pl.ds(q * e, e), :] = pair_ref[pl.ds(owner * e, e), :]
            name = jnp.where((col >= q * r) & (col < (q + 1) * r), owner * r + col - q * r, name)
        for p in range(pairs):
            pick = (rows[:, pl.ds(p, 1)] == name).astype(jnp.float32).astype(jnp.bfloat16)
            for h in range(2):
                out[pl.ds(p * examples, examples), pl.ds(h * blocks * r, blocks * r)] = pick

    return pl.pallas_call(
        body,
        out_shape=jax.ShapeDtypeStruct((pairs * examples, 2 * blocks * r), jnp.bfloat16),
        in_specs=[VMEM],
        out_specs=VMEM,
        scratch_shapes=[pltpu.VMEM((examples, pairs), jnp.int32)],
        compiler_params=pltpu.CompilerParams(vmem_limit_bytes=2 * 1024 * 1024),
        cost_estimate=pl.CostEstimate(flops=10**9, bytes_accessed=10**6, transcendentals=0),
        name="choices",
    )(pair_ref)


def chunks_of(width):
    if width % 128 or width < 512:
        return [(0, rounded(width, 128))]
    first = rounded(width // 2, 256)
    return [(0, first), (first, width - first)]


def on_device(
    examples, references, gate_weight, up_weight, down_weight, cotangent, pair_ref, points
):
    dims = factors(lax.axis_size("wide"))
    far, near, pair = dims
    peers = lax.axis_size("narrow")
    e, r, k = examples.shape[0], references.shape[0], cotangent.shape[0]
    depth, hidden = gate_weight.shape
    blocks = far * near * pair

    share = hidden // peers
    whole_weights = [gate_weight, up_weight, down_weight]
    aligned = share % 128 == 0
    ahead = aligned and peers == 2
    if aligned:
        whole_weights = [
            pltpu.with_memory_space_constraint(w, pltpu.MemorySpace.HBM) for w in whole_weights
        ]
    chunks = chunks_of(share)
    picks = choices(pair_ref, dims, e, r)

    def at_peer(steps, offset, width):
        if aligned:
            return whole_weights, (steps % peers, peers, share, offset)
        start = (lax.axis_index("narrow") + steps) % peers * share
        more = width - share

        def cut(weight, axis):
            piece = lax.dynamic_slice_in_dim(weight, start, share, axis)
            return jnp.pad(piece, [(0, more if d == axis else 0) for d in range(2)])

        return [cut(gate_weight, 1), cut(up_weight, 1), cut(down_weight, 0)], None

    own, whole, pieces = pack([references, examples, cotangent])
    column = {0: own}
    step = far // 2
    while step:
        for s in sorted(column):
            column[s + step] = permute(column[s], "wide", dims, 0, step)
        step //= 2
    beside = {}
    if near == 2:
        for s, block in column.items():
            beside[s] = permute(block, "wide", dims, 1, 1)
    order = halvings(far)
    plane = [column[s] for s in order] + [beside[s] for s in order if near == 2]
    half = assemble(plane, whole, pieces, (r, e, k), depth)
    blocks_of_weights = {}
    early = ahead and pair == 2 and len(chunks) == 2
    if ahead:
        wanted = [(1, chunk) for chunk in chunks] + [(0, chunk) for chunk in chunks[1 if early else 0:]]
        for s, chunk in wanted:
            blocks_of_weights[s, chunk[0]] = fetch(*at_peer(s, *chunk), chunk[1])
    halves = [half]
    if pair == 2:
        halves.append(permute(half, "wide", dims, 2, 1))

    parts = []
    if early:
        (offset, width), (next_offset, next_width) = chunks
        weights = blocks_of_weights[1, offset]
        count = half.shape[0] // (r + e + k) * k
        kept_one = (*at_peer(0, offset, width), width)
        sent, below = forward_half(halves[0], count, weights, width, (*kept_one, None, True, None))
        received = [shift(sent, peers, 1)]
        upper = (*kept_one, (0, depth // 2), False, None)
        sent, both = forward_half(halves[1], count, weights, width, upper)
        received.append(shift(sent, peers, 1))
        parts.append((offset, width, [tuple(received)]))
    main, side = join(halves, (r, e, k))
    if early:
        lower = (*kept_one, (depth // 2, depth - depth // 2), False, both)
        weights = blocks_of_weights[1, next_offset]
        sent, both = forward(main, side, weights, None, next_width, jnp.bfloat16, lower)
        parts.append((next_offset, next_width, [shift(sent, peers, 1)]))
        blocks_of_weights[0, offset] = (both, below)
    else:
        for offset, width in chunks:
            received = []
            for s in range(1, peers):
                weights, place = at_peer(s, offset, width)
                if ahead:
                    weights = blocks_of_weights[s, offset]
                (sent,) = forward(main, side, weights, place, width, jnp.bfloat16)
                received.append(shift(sent, peers, s))
            parts.append((offset, width, received))

    jobs = []
    for offset, width, received in parts:
        weights, place = at_peer(0, offset, width)
        if ahead:
            weights = blocks_of_weights[0, offset]
        (kept,) = forward(main, side, weights, place, width, jnp.float32)
        grads = coefficients(kept, received, picks, points, blocks * e)
        jobs.append((grads, offset, width, 0))
        jobs += [(shift(grads, peers, s), offset, width, s) for s in range(1, peers)]
    items = []
    for grads, offset, width, s in jobs:
        weights, place = at_peer(peers - s, offset, width)
        weights = blocks_of_weights[s, offset][:1] if ahead else weights[:2]
        items.append((grads, weights, place))
    if ahead and len(items) == 4:
        groups = [items[:1], items[1:3], items[3:]]
    else:
        groups = [[item] for item in items]
    total = None
    for group in groups[:-1]:
        total = backward(group, total, False)
    spans = [(0, depth // 2), (depth // 2, depth // 2)] if depth % 256 == 0 else [(0, depth)]
    last = [backward(groups[-1], total, pair == 2, span) for span in spans]

    results = []
    for i, value in enumerate(last):
        if pair == 2:
            sent, kept = value
            value = kept + permute(sent, "wide", dims, 2, 1).astype(jnp.float32)
        digits = [(1, 1)] * (near == 2) + [(0, 1 << bit) for bit in range(far.bit_length() - 1)]
        steps = list(digits)
        if i % 2 and len(steps) > 1:
            steps[:2] = steps[1::-1]
        for step in steps:
            at = digits.index(step)
            outer, inner = 1 << at, value.shape[0] >> (at + 1)
            digits.remove(step)

            def half(which):
                rows = [value[(2 * o + which) * inner:(2 * o + which + 1) * inner] for o in range(outer)]
                return rows[0] if outer == 1 else jnp.concatenate(rows)

            got = permute(half(1).astype(jnp.bfloat16), "wide", dims, *step)
            value = half(0) + got.astype(jnp.float32)
        results.append(value.astype(jnp.bfloat16))
    return results[0] if len(results) == 1 else jnp.concatenate(results, axis=1)


def solution(mesh):
    in_specs = (
        P("wide", "narrow"),
        P("wide", "narrow"),
        P("narrow", "wide"),
        P("narrow", "wide"),
        P("wide", "narrow"),
        P("wide", "narrow"),
        P(),
        P(),
    )
    out_specs = P("wide", "narrow")
    return jax.shard_map(on_device, mesh=mesh, in_specs=in_specs, out_specs=out_specs, check_vma=False)
```

```python
import jax
import jax.numpy as jnp
from jax import lax
from jax.experimental import pallas as pl
from jax.experimental.pallas import tpu as pltpu
from jax.sharding import PartitionSpec as P


VMEM = pl.BlockSpec(memory_space=pltpu.VMEM)
SMEM = pl.BlockSpec(memory_space=pltpu.SMEM)
ANY = pl.BlockSpec(memory_space=pl.ANY)


def factors(size):
    pair = 2 if size % 2 == 0 else 1
    near = 2 if (size // pair) % 2 == 0 else 1
    return size // (pair * near), near, pair


def rounded(rows, unit):
    return -(-rows // unit) * unit


def permute(array, axis, dims, digit, amount):
    below = 1
    for size in dims[digit + 1:]:
        below *= size
    total = below
    for size in dims[:digit + 1]:
        total *= size
    pairs = [
        (at, at + (((at // below) % dims[digit] ^ amount) - (at // below) % dims[digit]) * below)
        for at in range(total)
    ]
    return lax.ppermute(array, axis, pairs)


def shift(array, size, amount):
    return lax.ppermute(array, "narrow", [(at, (at + amount) % size) for at in range(size)])


def halvings(size):
    if size == 1:
        return [0]
    return [2 * v for v in halvings(size // 2)] + [2 * v + 1 for v in halvings(size // 2)]


def pack(arrays):
    count, width = sum(a.shape[0] for a in arrays), arrays[0].shape[1]
    whole = count // 8 * 8
    rest = count - whole
    pieces = whole // rest if rest and whole else 1
    cut = rest > 0 and whole > 0 and whole % rest == 0 and width % (pieces * 128) == 0
    if not cut:
        whole, pieces = rounded(count, 8), 1
    lanes = width // pieces

    def body(*refs):
        sources, (out, *held, sems) = refs[:len(arrays)], refs[len(arrays):]
        copies = [
            pltpu.make_async_copy(source, target, sems.at[i])
            for i, (source, target) in enumerate(zip(sources, held))
        ]
        for copy in copies:
            copy.start()
        for copy in copies:
            copy.wait()
        rows = jnp.concatenate([ref[...].astype(jnp.float32) for ref in held])
        if not cut:
            if whole > count:
                rows = jnp.concatenate([rows, jnp.zeros((whole - count, width), jnp.float32)])
            out[...] = rows.astype(out.dtype)
            return
        out[:, pl.ds(0, width)] = rows[:whole].astype(out.dtype)
        beside = [
            rows[whole + i:whole + i + 1, j * lanes:(j + 1) * lanes]
            for i in range(rest)
            for j in range(pieces)
        ]
        out[:, pl.ds(width, lanes)] = jnp.concatenate(beside).astype(out.dtype)

    packed = pl.pallas_call(
        body,
        out_shape=jax.ShapeDtypeStruct((whole, width + lanes if cut else width), arrays[0].dtype),
        in_specs=[ANY] * len(arrays),
        out_specs=VMEM,
        scratch_shapes=[pltpu.VMEM(a.shape, a.dtype) for a in arrays]
        + [pltpu.SemaphoreType.DMA((len(arrays),))],
        compiler_params=pltpu.CompilerParams(vmem_limit_bytes=4 * 1024 * 1024),
        name="pack",
    )(*(pltpu.with_memory_space_constraint(a, pltpu.MemorySpace.HBM) for a in arrays))
    return packed, whole, pieces


def assemble(own, whole, pieces, counts, width):
    blocks = len(own)
    packed = own[0].shape
    total = blocks * sum(counts)
    across_lanes = width // pieces

    def body(*refs):
        out, stack = refs[-2], refs[-1]
        for b in range(blocks):
            stack[pl.ds(b * packed[0], packed[0]), :] = refs[b][...]
        row = lax.broadcasted_iota(jnp.int32, (total, blocks * packed[0]), 0)
        col = lax.broadcasted_iota(jnp.int32, (total, blocks * packed[0]), 1)
        held = jnp.zeros_like(row)
        block = jnp.zeros_like(row)
        at = first = 0
        for count in counts:
            for b in range(blocks):
                inside = (row >= at) & (row < at + count)
                held = jnp.where(inside, row - at + first, held)
                block = jnp.where(inside, b, block)
                at += count
            first += count

        def pick(wanted, valid):
            return (valid & (col == wanted)).astype(jnp.float32).astype(jnp.bfloat16)

        base = block * packed[0]
        uncut = pick(base + held, held < whole)
        for j in range(pieces):
            lanes = pl.ds(j * across_lanes, across_lanes)
            value = jnp.dot(uncut, stack[:, lanes], preferred_element_type=jnp.float32)
            if packed[1] > width:
                value = value + jnp.dot(
                    pick(base + (held - whole) * pieces + j, held >= whole),
                    stack[:, pl.ds(width, across_lanes)],
                    preferred_element_type=jnp.float32,
                )
            out[:, lanes] = value.astype(jnp.bfloat16)

    dtype = own[0].dtype
    return pl.pallas_call(
        body,
        out_shape=jax.ShapeDtypeStruct((total, width), dtype),
        in_specs=[VMEM] * blocks,
        out_specs=VMEM,
        scratch_shapes=[pltpu.VMEM((blocks * packed[0], packed[1]), dtype)],
        compiler_params=pltpu.CompilerParams(vmem_limit_bytes=6 * 1024 * 1024),
        cost_estimate=pl.CostEstimate(flops=10**9, bytes_accessed=10**6, transcendentals=0),
        name="assemble",
    )(*own)


def join(halves, layout):
    width = halves[0].shape[1]
    blocks = halves[0].shape[0] // sum(layout)
    e, r, k = (blocks * rows for rows in layout)
    count = len(halves)

    def body(*refs):
        main, side = refs[-2:]
        for h in range(count):
            main[pl.ds(h * e, e), :] = refs[h][pl.ds(0, e), :]
            main[pl.ds(count * e + h * r, r), :] = refs[h][pl.ds(e, r), :]
            side[pl.ds(h * k, k), :] = refs[h][pl.ds(e + r, k), :]

    dtype = halves[0].dtype
    return pl.pallas_call(
        body,
        out_shape=(
            jax.ShapeDtypeStruct((count * (e + r), width), dtype),
            jax.ShapeDtypeStruct((count * k, width), dtype),
        ),
        in_specs=[VMEM] * count,
        out_specs=(VMEM, VMEM),
        compiler_params=pltpu.CompilerParams(vmem_limit_bytes=4 * 1024 * 1024),
        cost_estimate=pl.CostEstimate(flops=10**9, bytes_accessed=10**6, transcendentals=0),
        name="join",
    )(*halves)


def across(left, right):
    return lax.dot_general(left, right, (((1,), (1,)), ((), ())), preferred_element_type=jnp.float32)


def parts_of(size, unit):
    for count in (4, 2):
        if size % (count * unit) == 0:
            return [(i * (size // count), size // count) for i in range(count)]
    return [(0, size)]


def first_of(place):
    if place is None:
        return 0
    steps, peers, share, offset = place
    return pl.multiple_of((lax.axis_index("narrow") + steps) % peers * share + offset, 128)


def streams(weights, buffers, sems, first, width, by_depth, by_unit):
    gate, up, down = weights
    both, below = buffers
    units, depths = [], []
    for i, (row, count) in enumerate(by_unit if below is not None else ()):
        units.append(
            pltpu.make_async_copy(
                down.at[pl.ds(first + row, count)], below.at[pl.ds(row, count)], sems.at[2, i]
            )
        )
    for i, (row, count) in enumerate(by_depth if both is not None else ()):
        some = pl.ds(row, count)
        depths.append(
            [
                pltpu.make_async_copy(
                    source.at[some, pl.ds(first, width)],
                    both.at[some, pl.ds(w * width, width)],
                    sems.at[w, i],
                )
                for w, source in enumerate((gate, up))
            ]
        )
    return units, depths


def fetch(weights, place, width):
    depth = weights[0].shape[0]
    by_depth, by_unit = parts_of(depth, 128), parts_of(width, 32)

    def body(gate, up, down, both, below, sems):
        first = first_of(place)
        units, depths = streams((gate, up, down), (both, below), sems, first, width, by_depth, by_unit)
        copies = units + [copy for pair in depths for copy in pair]
        for copy in copies:
            copy.start()
        for copy in copies:
            copy.wait()

    return pl.pallas_call(
        body,
        out_shape=(
            pltpu.VMEM((depth, 2 * width), jnp.bfloat16),
            pltpu.VMEM((width, depth), jnp.bfloat16),
        ),
        in_specs=[ANY, ANY, ANY],
        out_specs=(VMEM, VMEM),
        scratch_shapes=[pltpu.SemaphoreType.DMA((3, 4))],
        compiler_params=pltpu.CompilerParams(vmem_limit_bytes=1024 * 1024),
        cost_estimate=pl.CostEstimate(
            flops=4 * 10**9, bytes_accessed=6 * depth * width, transcendentals=0
        ),
        name="fetch",
    )(*weights)


def arriving(next_one, depth):
    _, _, width, span, below, _ = next_one
    return [pltpu.VMEM((depth, 2 * width), jnp.bfloat16)] * (span is not None) + [
        pltpu.VMEM((width, depth), jnp.bfloat16)
    ] * below


def extras(next_one, depth, at):
    if next_one is None:
        return [], [], [], [], {}
    weights, _, _, _, _, into = next_one
    more = arriving(next_one, depth)
    scratch = [pltpu.SemaphoreType.DMA((3, 4))]
    if into is None:
        return [*weights], [ANY] * 3, more, scratch, {}
    return [*weights, into], [ANY] * 3 + [VMEM], more, scratch, {at + 3: 1}


def while_arriving(next_one, refs, work):
    if next_one is None:
        return work(refs[0])
    _, place, width, span, below, into = next_one
    sources, (out, *targets, sems) = refs[:3], refs[3 + (into is not None):]
    buffers = (targets.pop(0) if span else None, targets.pop(0) if below else None)
    first, count = span or (0, 0)
    units, depths = streams(
        sources,
        buffers,
        sems,
        first_of(place),
        width,
        [(first + row, rows) for row, rows in parts_of(count, 128)] if span else [],
        parts_of(width, 32),
    )
    copies = units + [copy for pair in depths for copy in pair]
    for copy in copies:
        copy.start()
    pl.when(lax.axis_index("narrow") >= 0)(lambda: work(out))
    for copy in copies:
        copy.wait()


def forward_half(half, others, side_rows, weights, width, next_one=None):
    depth = half.shape[1]
    rows = half.shape[0] - side_rows
    inputs = [half, weights[0]] + ([weights[1], *others] if others else [])
    all_rows = rows + (side_rows if others else 0)

    def body(half_ref, both, *refs):
        refs = list(refs)
        below = refs.pop(0) if others else None
        side_refs = [refs.pop(0) for _ in others]

        def work(out):
            out[pl.ds(0, rows), :] = jnp.dot(
                half_ref[pl.ds(0, rows), :], both[...], preferred_element_type=jnp.float32
            ).astype(jnp.bfloat16)
            if others:
                side = jnp.concatenate([ref[pl.ds(rows, side_rows), :] for ref in side_refs])
                value = across(side, below[...]).astype(jnp.bfloat16)
                out[pl.ds(rows, side_rows), pl.ds(0, width)] = value[:side_rows]
                out[pl.ds(rows, side_rows), pl.ds(width, width)] = value[side_rows:]

        while_arriving(next_one, refs, work)

    operands, specs, more, scratch, aliases = extras(next_one, depth, len(inputs))
    return pl.pallas_call(
        body,
        out_shape=[jax.ShapeDtypeStruct((all_rows, 2 * width), jnp.bfloat16)] + more,
        in_specs=[VMEM] * len(inputs) + specs,
        out_specs=[VMEM] * (1 + len(more)),
        scratch_shapes=scratch,
        input_output_aliases=aliases,
        compiler_params=pltpu.CompilerParams(vmem_limit_bytes=4 * 1024 * 1024),
        cost_estimate=pl.CostEstimate(
            flops=4 * depth * width * all_rows, bytes_accessed=10**6, transcendentals=0
        ),
        name="forward_half",
    )(*inputs, *operands)


def forward(main, side, weights, place, width, dtype, next_one=None):
    rows, half = main.shape[0], side.shape[0] // 2
    depth = main.shape[1]
    by_depth, by_unit = parts_of(depth, 128), parts_of(width, 32)
    ready = len(weights) == 2

    def put_side(out, value):
        out[pl.ds(rows, half), pl.ds(0, width)] = value[:half].astype(dtype)
        out[pl.ds(rows, half), pl.ds(width, width)] = value[half:].astype(dtype)

    def body_ready(main_ref, side_ref, both, below, *refs):
        def work(out):
            out[pl.ds(0, rows), :] = jnp.dot(
                main_ref[...], both[...], preferred_element_type=jnp.float32
            ).astype(dtype)
            put_side(out, across(side_ref[...], below[...]))

        while_arriving(next_one, refs, work)

    def body(main_ref, side_ref, gate, up, down, out, both, below, total, sems):
        first = first_of(place)
        units, depths = streams((gate, up, down), (both, below), sems, first, width, by_depth, by_unit)
        for copy in units + [copy for pair in depths for copy in pair]:
            copy.start()
        for copy in units:
            copy.wait()
        put_side(out, across(side_ref[...], below[...]))
        for i, (row, count) in enumerate(by_depth):
            for copy in depths[i]:
                copy.wait()
            some = pl.ds(row, count)
            part = jnp.dot(main_ref[:, some], both[some, :], preferred_element_type=jnp.float32)
            if i > 0:
                part = total[...] + part
            if i == len(by_depth) - 1:
                out[pl.ds(0, rows), :] = part.astype(dtype)
            else:
                total[...] = part

    out_shape = [jax.ShapeDtypeStruct((rows + half, 2 * width), dtype)]
    operands = [main, side, *weights]
    specs = [VMEM] * 2 + [VMEM if ready else ANY] * len(weights)
    aliases = {}
    if ready:
        operands_more, specs_more, more, scratch, aliases = extras(next_one, depth, 4)
        operands += operands_more
        specs += specs_more
        out_shape += more
    else:
        scratch = [
            pltpu.VMEM((depth, 2 * width), jnp.bfloat16),
            pltpu.VMEM((width, depth), jnp.bfloat16),
            pltpu.VMEM((rows, 2 * width), jnp.float32),
            pltpu.SemaphoreType.DMA((3, 4)),
        ]
    return pl.pallas_call(
        body_ready if ready else body,
        out_shape=out_shape,
        in_specs=specs,
        out_specs=[VMEM] * len(out_shape),
        scratch_shapes=scratch,
        input_output_aliases=aliases,
        compiler_params=pltpu.CompilerParams(vmem_limit_bytes=(4 if ready else 20) * 1024 * 1024),
        cost_estimate=pl.CostEstimate(
            flops=4 * depth * width * (rows + half), bytes_accessed=6 * depth * width, transcendentals=0
        ),
        name="forward",
    )(*operands)


def coefficients(kept, received, picks, points, examples):
    width = kept.shape[1] // 2
    pairs, references = picks.shape[0] // examples, picks.shape[1] // 2
    rows = examples + references
    count = points.shape[0]
    lanes = 128 if width % 128 == 0 else width
    middle = examples // 2
    pieces, left = [], middle
    while left:
        size = 16 if left == 16 or left >= 32 else left
        pieces.append((middle - left, size))
        left -= size
    pieces += [(middle + first, size) for first, size in pieces]
    arrays = [array for item in received for array in (item if isinstance(item, tuple) else (item,))]
    scale = 1.0 / (pairs * count)

    def body(points_ref, picks_ref, kept_ref, *refs):
        out, base_gate, base_up = refs[-3:]
        refs = list(refs[:-3])
        got = [
            tuple(refs.pop(0) for _ in item) if isinstance(item, tuple) else refs.pop(0)
            for item in received
        ]
        picks = picks_ref[...]
        steps = [points_ref[m].astype(jnp.float32) * 0.125 for m in range(count)]
        steps_1 = sum(steps[1:], steps[0])
        steps_2 = sum((t * t for t in steps[1:]), steps[0] * steps[0])

        def total(take, *where):
            value = take(kept_ref, *where)
            for ref in got:
                value = value + take(ref, *where).astype(jnp.float32)
            return value

        def of_references(ref, lanes_of):
            if isinstance(ref, tuple):
                return jnp.concatenate([half[pl.ds(0, references // 2), lanes_of] for half in ref])
            return ref[pl.ds(0, references), lanes_of]

        for w, target in enumerate((base_gate, base_up)):
            value = total(of_references, pl.ds(w * width, width))
            high = value.astype(jnp.bfloat16)
            low = (value - high.astype(jnp.float32)).astype(jnp.bfloat16)
            target[...] = jnp.dot(
                picks, jnp.concatenate([high, low]), preferred_element_type=jnp.float32
            )

        def block(j, _):
            here = pl.ds(0, width) if lanes == width else pl.ds(pl.multiple_of(j * lanes, 128), lanes)
            if lanes == width:
                of = [pl.ds(w * width, width) for w in range(2)]
            else:
                of = [pl.ds(pl.multiple_of(w * width + j * lanes, 128), lanes) for w in range(2)]

            def of_examples(ref, first, size, w):
                if isinstance(ref, tuple):
                    h = first // middle
                    return ref[h][pl.ds(references // 2 + first - h * middle, size), of[w]]
                return ref[pl.ds(references + first, size), of[w]]

            def of_upstream(ref, h):
                ref, first = (ref[1], rows // 2) if isinstance(ref, tuple) else (ref, rows)
                return ref[pl.ds(first, middle), of[h]]

            upstream = [total(of_upstream, h) for h in range(2)]
            for first, piece in pieces:
                gate = total(of_examples, first, piece, 0) * 0.5
                up = total(of_examples, first, piece, 1)
                coef_gate = jnp.zeros_like(gate)
                coef_up = jnp.zeros_like(gate)
                for p in range(pairs):
                    start = base_gate[pl.ds(p * examples + first, piece), here] * 0.5
                    span = gate - start
                    flat = count + (count * start + steps_1 * span)
                    tilted = steps_1 + (steps_1 * start + steps_2 * span)
                    coef_up = coef_up + (count * start + steps_1 * span)
                    for t in steps:
                        half = start + t * span
                        v = jnp.tanh(half)
                        bent = half * v
                        turn = v - v * bent
                        coef_up = coef_up + bent
                        flat = flat + turn
                        tilted = tilted + t * turn
                    start_up = base_up[pl.ds(p * examples + first, piece), here]
                    coef_gate = coef_gate + (start_up * flat + (up - start_up) * tilted)
                base_gate[pl.ds(first, piece), here] = coef_gate * (0.5 * scale)
                base_up[pl.ds(first, piece), here] = coef_up * scale
            for w, source in enumerate((base_gate, base_up)):
                for h in range(2):
                    some = pl.ds(h * middle, middle)
                    out[some, of[w]] = (upstream[h] * source[some, here]).astype(jnp.bfloat16)
            return 0

        lax.fori_loop(0, width // lanes, block, 0)

    return pl.pallas_call(
        body,
        out_shape=jax.ShapeDtypeStruct((examples, 2 * width), jnp.bfloat16),
        in_specs=[SMEM, VMEM, VMEM] + [VMEM] * len(arrays),
        out_specs=VMEM,
        scratch_shapes=[pltpu.VMEM((pairs * examples, width), jnp.float32)] * 2,
        compiler_params=pltpu.CompilerParams(vmem_limit_bytes=4 * 1024 * 1024),
        cost_estimate=pl.CostEstimate(flops=5 * 10**9, bytes_accessed=10**6, transcendentals=0),
        name="coefficients",
    )(points, picks, kept, *arrays)


def backward(items, total, final, span=None):
    grads, weights, place = items[0]
    rows, width, depth = grads.shape[0], grads.shape[1] // 2, weights[0].shape[0]
    low, columns = span or (0, depth)
    by_depth = [(low + row, count) for row, count in (parts_of(columns, 128) if len(weights) > 1 else [(0, columns)])]
    ready = len(weights) == 1

    def body(*refs):
        grads_refs, refs = refs[:len(items)], refs[len(items):]
        if ready:
            boths, outs = refs[:len(items)], refs[len(items):]
        else:
            gate, up, *outs, both, sems = refs
            boths = [both]
            _, depths = streams((gate, up, None), (both, None), sems, first_of(place), width, by_depth, [])
            for pair in depths:
                for copy in pair:
                    copy.start()
        for i, (row, count) in enumerate(by_depth):
            some, own = pl.ds(row, count), pl.ds(row - low, count)
            if not ready:
                for copy in depths[i]:
                    copy.wait()
            value = None if total is None else outs[0][:, some]
            for grads_ref, both in zip(grads_refs, boths):
                part = across(grads_ref[...], both[some, :])
                value = part if value is None else value + part
            if final:
                outs[-2][:, own] = value[rows // 2:, :].astype(jnp.bfloat16)
                outs[-1][:, own] = value[:rows // 2, :]
            else:
                outs[-1][:, own] = value

    operands = [item[0] for item in items] + [w for item in items for w in item[1]]
    specs = [VMEM] * len(items) + [VMEM if ready else ANY] * (len(operands) - len(items))
    if total is not None:
        operands.append(total)
        specs.append(VMEM)
    if final:
        out_shape = (
            jax.ShapeDtypeStruct((rows // 2, columns), jnp.bfloat16),
            jax.ShapeDtypeStruct((rows // 2, columns), jnp.float32),
        )
        out_specs = (VMEM, VMEM)
    else:
        out_shape, out_specs = jax.ShapeDtypeStruct((rows, columns), jnp.float32), VMEM
    scratch = [pltpu.VMEM((depth, 2 * width), jnp.bfloat16), pltpu.SemaphoreType.DMA((2, 4))]
    return pl.pallas_call(
        body,
        out_shape=out_shape,
        in_specs=specs,
        out_specs=out_specs,
        scratch_shapes=[] if ready else scratch,
        compiler_params=pltpu.CompilerParams(vmem_limit_bytes=(4 if ready else 12) * 1024 * 1024),
        cost_estimate=pl.CostEstimate(
            flops=2 * rows * columns * sum(item[0].shape[1] for item in items),
            bytes_accessed=4 * width * columns,
            transcendentals=0,
        ),
        name="backward",
    )(*operands)


def choices(pair_ref, dims, e, r):
    far, near, pair = dims
    blocks = far * near * pair
    examples, pairs = pair_ref.shape

    def body(pair_ref, out, rows):
        at = lax.axis_index("wide")
        z, y, c = at // (near * pair), at // pair % near, at % pair
        col = lax.broadcasted_iota(jnp.int32, (examples, blocks * r), 1)
        name = jnp.zeros_like(col)
        for q in range(blocks):
            s, b, p = halvings(far)[q % far], q // far % near, q // (far * near)
            owner = ((z ^ s) * near + (y ^ b)) * pair + (c ^ p)
            rows[pl.ds(q * e, e), :] = pair_ref[pl.ds(owner * e, e), :]
            name = jnp.where((col >= q * r) & (col < (q + 1) * r), owner * r + col - q * r, name)
        for p in range(pairs):
            pick = (rows[:, pl.ds(p, 1)] == name).astype(jnp.float32).astype(jnp.bfloat16)
            for h in range(2):
                out[pl.ds(p * examples, examples), pl.ds(h * blocks * r, blocks * r)] = pick

    return pl.pallas_call(
        body,
        out_shape=jax.ShapeDtypeStruct((pairs * examples, 2 * blocks * r), jnp.bfloat16),
        in_specs=[VMEM],
        out_specs=VMEM,
        scratch_shapes=[pltpu.VMEM((examples, pairs), jnp.int32)],
        compiler_params=pltpu.CompilerParams(vmem_limit_bytes=2 * 1024 * 1024),
        cost_estimate=pl.CostEstimate(flops=10**9, bytes_accessed=10**6, transcendentals=0),
        name="choices",
    )(pair_ref)


def chunks_of(width):
    if width % 128 or width < 512:
        return [(0, rounded(width, 128))]
    first = rounded(width // 2, 256)
    return [(0, first), (first, width - first)]


def on_device(
    examples, references, gate_weight, up_weight, down_weight, cotangent, pair_ref, points
):
    dims = factors(lax.axis_size("wide"))
    far, near, pair = dims
    peers = lax.axis_size("narrow")
    e, r, k = examples.shape[0], references.shape[0], cotangent.shape[0]
    depth, hidden = gate_weight.shape
    blocks = far * near * pair

    share = hidden // peers
    whole_weights = [gate_weight, up_weight, down_weight]
    aligned = share % 128 == 0
    ahead = aligned and peers == 2
    if aligned:
        whole_weights = [
            pltpu.with_memory_space_constraint(w, pltpu.MemorySpace.HBM) for w in whole_weights
        ]
    chunks = chunks_of(share)
    picks = choices(pair_ref, dims, e, r)

    def at_peer(steps, offset, width):
        if aligned:
            return whole_weights, (steps % peers, peers, share, offset)
        start = (lax.axis_index("narrow") + steps) % peers * share
        more = width - share

        def cut(weight, axis):
            piece = lax.dynamic_slice_in_dim(weight, start, share, axis)
            return jnp.pad(piece, [(0, more if d == axis else 0) for d in range(2)])

        return [cut(gate_weight, 1), cut(up_weight, 1), cut(down_weight, 0)], None

    own, whole, pieces = pack([references, examples, cotangent])
    column = {0: own}
    step = far // 2
    while step:
        for s in sorted(column):
            column[s + step] = permute(column[s], "wide", dims, 0, step)
        step //= 2
    beside = {}
    if near == 2:
        for s, block in column.items():
            beside[s] = permute(block, "wide", dims, 1, 1)
    order = halvings(far)
    plane = [column[s] for s in order] + [beside[s] for s in order if near == 2]
    half = assemble(plane, whole, pieces, (r, e, k), depth)
    blocks_of_weights = {}
    early = ahead and pair == 2 and len(chunks) == 2
    if ahead:
        wanted = [(1, chunk) for chunk in chunks] + [(0, chunk) for chunk in chunks[1 if early else 0:]]
        for s, chunk in wanted:
            blocks_of_weights[s, chunk[0]] = fetch(*at_peer(s, *chunk), chunk[1])
    halves = [half]
    if pair == 2:
        halves.append(permute(half, "wide", dims, 2, 1))

    parts = []
    if early:
        (offset, width), (next_offset, next_width) = chunks
        weights = blocks_of_weights[1, offset]
        count = half.shape[0] // (r + e + k) * k
        kept_one = (*at_peer(0, offset, width), width)
        (sent,) = forward_half(halves[0], [], count, weights, width)
        received = [shift(sent, peers, 1)]
        upper = (*kept_one, (0, depth // 2), False, None)
        sent, both = forward_half(halves[1], halves, count, weights, width, upper)
        received.append(shift(sent, peers, 1))
        parts.append((offset, width, [tuple(received)]))
    main, side = join(halves, (r, e, k))
    if early:
        lower = (*kept_one, (depth // 2, depth - depth // 2), False, both)
        weights = blocks_of_weights[1, next_offset]
        sent, both = forward(main, side, weights, None, next_width, jnp.bfloat16, lower)
        parts.append((next_offset, next_width, [shift(sent, peers, 1)]))
        weights = blocks_of_weights[0, next_offset]
        kept_last, below = forward(
            main, side, weights, None, next_width, jnp.float32, (*kept_one, None, True, None)
        )
        blocks_of_weights[0, offset] = (both, below)
    else:
        for offset, width in chunks:
            received = []
            for s in range(1, peers):
                weights, place = at_peer(s, offset, width)
                if ahead:
                    weights = blocks_of_weights[s, offset]
                (sent,) = forward(main, side, weights, place, width, jnp.bfloat16)
                received.append(shift(sent, peers, s))
            parts.append((offset, width, received))

    jobs = []
    for i, (offset, width, received) in enumerate(parts):
        weights, place = at_peer(0, offset, width)
        if ahead:
            weights = blocks_of_weights[0, offset]
        if early and i == 1:
            kept = kept_last
        else:
            (kept,) = forward(main, side, weights, place, width, jnp.float32)
        grads = coefficients(kept, received, picks, points, blocks * e)
        jobs.append((grads, offset, width, 0))
        jobs += [(shift(grads, peers, s), offset, width, s) for s in range(1, peers)]
    items = []
    for grads, offset, width, s in jobs:
        weights, place = at_peer(peers - s, offset, width)
        weights = blocks_of_weights[s, offset][:1] if ahead else weights[:2]
        items.append((grads, weights, place))
    if ahead and len(items) == 4:
        groups = [items[:1], items[1:3], items[3:]]
    else:
        groups = [[item] for item in items]
    total = None
    for group in groups[:-1]:
        total = backward(group, total, False)
    spans = [(0, depth // 2), (depth // 2, depth // 2)] if depth % 256 == 0 else [(0, depth)]
    last = [backward(groups[-1], total, pair == 2, span) for span in spans]

    results = []
    for i, value in enumerate(last):
        if pair == 2:
            sent, kept = value
            value = kept + permute(sent, "wide", dims, 2, 1).astype(jnp.float32)
        digits = [(1, 1)] * (near == 2) + [(0, 1 << bit) for bit in range(far.bit_length() - 1)]
        steps = list(digits)
        if i % 2 and len(steps) > 1:
            steps[:2] = steps[1::-1]
        for step in steps:
            at = digits.index(step)
            outer, inner = 1 << at, value.shape[0] >> (at + 1)
            digits.remove(step)

            def half(which):
                rows = [value[(2 * o + which) * inner:(2 * o + which + 1) * inner] for o in range(outer)]
                return rows[0] if outer == 1 else jnp.concatenate(rows)

            got = permute(half(1).astype(jnp.bfloat16), "wide", dims, *step)
            value = half(0) + got.astype(jnp.float32)
        results.append(value.astype(jnp.bfloat16))
    return results[0] if len(results) == 1 else jnp.concatenate(results, axis=1)


def solution(mesh):
    in_specs = (
        P("wide", "narrow"),
        P("wide", "narrow"),
        P("narrow", "wide"),
        P("narrow", "wide"),
        P("wide", "narrow"),
        P("wide", "narrow"),
        P(),
        P(),
    )
    out_specs = P("wide", "narrow")
    return jax.shard_map(on_device, mesh=mesh, in_specs=in_specs, out_specs=out_specs, check_vma=False)
```

```python
import jax
import jax.numpy as jnp
from jax import lax
from jax.experimental import pallas as pl
from jax.experimental.pallas import tpu as pltpu
from jax.sharding import PartitionSpec as P


VMEM = pl.BlockSpec(memory_space=pltpu.VMEM)
SMEM = pl.BlockSpec(memory_space=pltpu.SMEM)
ANY = pl.BlockSpec(memory_space=pl.ANY)


def factors(size):
    pair = 2 if size % 2 == 0 else 1
    near = 2 if (size // pair) % 2 == 0 else 1
    return size // (pair * near), near, pair


def rounded(rows, unit):
    return -(-rows // unit) * unit


def permute(array, axis, dims, digit, amount):
    below = 1
    for size in dims[digit + 1:]:
        below *= size
    total = below
    for size in dims[:digit + 1]:
        total *= size
    pairs = [
        (at, at + (((at // below) % dims[digit] ^ amount) - (at // below) % dims[digit]) * below)
        for at in range(total)
    ]
    return lax.ppermute(array, axis, pairs)


def shift(array, size, amount):
    return lax.ppermute(array, "narrow", [(at, (at + amount) % size) for at in range(size)])


def halvings(size):
    if size == 1:
        return [0]
    return [2 * v for v in halvings(size // 2)] + [2 * v + 1 for v in halvings(size // 2)]


def pack(arrays):
    count, width = sum(a.shape[0] for a in arrays), arrays[0].shape[1]
    whole = count // 8 * 8
    rest = count - whole
    pieces = whole // rest if rest and whole else 1
    cut = rest > 0 and whole > 0 and whole % rest == 0 and width % (pieces * 128) == 0
    if not cut:
        whole, pieces = rounded(count, 8), 1
    lanes = width // pieces

    def body(*refs):
        sources, (out, *held, sems) = refs[:len(arrays)], refs[len(arrays):]
        copies = [
            pltpu.make_async_copy(source, target, sems.at[i])
            for i, (source, target) in enumerate(zip(sources, held))
        ]
        for copy in copies:
            copy.start()
        for copy in copies:
            copy.wait()
        rows = jnp.concatenate([ref[...].astype(jnp.float32) for ref in held])
        if not cut:
            if whole > count:
                rows = jnp.concatenate([rows, jnp.zeros((whole - count, width), jnp.float32)])
            out[...] = rows.astype(out.dtype)
            return
        out[:, pl.ds(0, width)] = rows[:whole].astype(out.dtype)
        beside = [
            rows[whole + i:whole + i + 1, j * lanes:(j + 1) * lanes]
            for i in range(rest)
            for j in range(pieces)
        ]
        out[:, pl.ds(width, lanes)] = jnp.concatenate(beside).astype(out.dtype)

    packed = pl.pallas_call(
        body,
        out_shape=jax.ShapeDtypeStruct((whole, width + lanes if cut else width), arrays[0].dtype),
        in_specs=[ANY] * len(arrays),
        out_specs=VMEM,
        scratch_shapes=[pltpu.VMEM(a.shape, a.dtype) for a in arrays]
        + [pltpu.SemaphoreType.DMA((len(arrays),))],
        compiler_params=pltpu.CompilerParams(vmem_limit_bytes=4 * 1024 * 1024),
        name="pack",
    )(*(pltpu.with_memory_space_constraint(a, pltpu.MemorySpace.HBM) for a in arrays))
    return packed, whole, pieces


def assemble(own, whole, pieces, counts, width):
    blocks = len(own)
    packed = own[0].shape
    total = blocks * sum(counts)
    across_lanes = width // pieces

    def body(*refs):
        out, stack = refs[-2], refs[-1]
        for b in range(blocks):
            stack[pl.ds(b * packed[0], packed[0]), :] = refs[b][...]
        row = lax.broadcasted_iota(jnp.int32, (total, blocks * packed[0]), 0)
        col = lax.broadcasted_iota(jnp.int32, (total, blocks * packed[0]), 1)
        held = jnp.zeros_like(row)
        block = jnp.zeros_like(row)
        at = first = 0
        for count in counts:
            for b in range(blocks):
                inside = (row >= at) & (row < at + count)
                held = jnp.where(inside, row - at + first, held)
                block = jnp.where(inside, b, block)
                at += count
            first += count

        def pick(wanted, valid):
            return (valid & (col == wanted)).astype(jnp.float32).astype(jnp.bfloat16)

        base = block * packed[0]
        uncut = pick(base + held, held < whole)
        for j in range(pieces):
            lanes = pl.ds(j * across_lanes, across_lanes)
            value = jnp.dot(uncut, stack[:, lanes], preferred_element_type=jnp.float32)
            if packed[1] > width:
                value = value + jnp.dot(
                    pick(base + (held - whole) * pieces + j, held >= whole),
                    stack[:, pl.ds(width, across_lanes)],
                    preferred_element_type=jnp.float32,
                )
            out[:, lanes] = value.astype(jnp.bfloat16)

    dtype = own[0].dtype
    return pl.pallas_call(
        body,
        out_shape=jax.ShapeDtypeStruct((total, width), dtype),
        in_specs=[VMEM] * blocks,
        out_specs=VMEM,
        scratch_shapes=[pltpu.VMEM((blocks * packed[0], packed[1]), dtype)],
        compiler_params=pltpu.CompilerParams(vmem_limit_bytes=6 * 1024 * 1024),
        cost_estimate=pl.CostEstimate(flops=10**9, bytes_accessed=10**6, transcendentals=0),
        name="assemble",
    )(*own)


def join(halves, layout):
    width = halves[0].shape[1]
    blocks = halves[0].shape[0] // sum(layout)
    e, r, k = (blocks * rows for rows in layout)
    count = len(halves)

    def body(*refs):
        main, side = refs[-2:]
        for h in range(count):
            main[pl.ds(h * e, e), :] = refs[h][pl.ds(0, e), :]
            main[pl.ds(count * e + h * r, r), :] = refs[h][pl.ds(e, r), :]
            side[pl.ds(h * k, k), :] = refs[h][pl.ds(e + r, k), :]

    dtype = halves[0].dtype
    return pl.pallas_call(
        body,
        out_shape=(
            jax.ShapeDtypeStruct((count * (e + r), width), dtype),
            jax.ShapeDtypeStruct((count * k, width), dtype),
        ),
        in_specs=[VMEM] * count,
        out_specs=(VMEM, VMEM),
        compiler_params=pltpu.CompilerParams(vmem_limit_bytes=4 * 1024 * 1024),
        cost_estimate=pl.CostEstimate(flops=10**9, bytes_accessed=10**6, transcendentals=0),
        name="join",
    )(*halves)


def across(left, right):
    return lax.dot_general(left, right, (((1,), (1,)), ((), ())), preferred_element_type=jnp.float32)


def parts_of(size, unit):
    for count in (4, 2):
        if size % (count * unit) == 0:
            return [(i * (size // count), size // count) for i in range(count)]
    return [(0, size)]


def first_of(place):
    if place is None:
        return 0
    steps, peers, share, offset = place
    return pl.multiple_of((lax.axis_index("narrow") + steps) % peers * share + offset, 128)


def streams(weights, buffers, sems, first, width, by_depth, by_unit):
    gate, up, down = weights
    both, below = buffers
    units, depths = [], []
    for i, (row, count) in enumerate(by_unit if below is not None else ()):
        units.append(
            pltpu.make_async_copy(
                down.at[pl.ds(first + row, count)], below.at[pl.ds(row, count)], sems.at[2, i]
            )
        )
    for i, (row, count) in enumerate(by_depth if both is not None else ()):
        some = pl.ds(row, count)
        depths.append(
            [
                pltpu.make_async_copy(
                    source.at[some, pl.ds(first, width)],
                    both.at[some, pl.ds(w * width, width)],
                    sems.at[w, i],
                )
                for w, source in enumerate((gate, up))
            ]
        )
    return units, depths


def fetch(weights, place, width):
    depth = weights[0].shape[0]
    by_depth, by_unit = parts_of(depth, 128), parts_of(width, 32)

    def body(gate, up, down, both, below, sems):
        first = first_of(place)
        units, depths = streams((gate, up, down), (both, below), sems, first, width, by_depth, by_unit)
        copies = units + [copy for pair in depths for copy in pair]
        for copy in copies:
            copy.start()
        for copy in copies:
            copy.wait()

    return pl.pallas_call(
        body,
        out_shape=(
            pltpu.VMEM((depth, 2 * width), jnp.bfloat16),
            pltpu.VMEM((width, depth), jnp.bfloat16),
        ),
        in_specs=[ANY, ANY, ANY],
        out_specs=(VMEM, VMEM),
        scratch_shapes=[pltpu.SemaphoreType.DMA((3, 4))],
        compiler_params=pltpu.CompilerParams(vmem_limit_bytes=1024 * 1024),
        cost_estimate=pl.CostEstimate(
            flops=4 * 10**9, bytes_accessed=6 * depth * width, transcendentals=0
        ),
        name="fetch",
    )(*weights)


def arriving(next_one, depth):
    _, _, width, span, below, _ = next_one
    return [pltpu.VMEM((depth, 2 * width), jnp.bfloat16)] * (span is not None) + [
        pltpu.VMEM((width, depth), jnp.bfloat16)
    ] * below


def extras(next_one, depth, at):
    if next_one is None:
        return [], [], [], [], {}
    weights, _, _, _, _, into = next_one
    more = arriving(next_one, depth)
    scratch = [pltpu.SemaphoreType.DMA((3, 4))]
    if into is None:
        return [*weights], [ANY] * 3, more, scratch, {}
    return [*weights, into], [ANY] * 3 + [VMEM], more, scratch, {at + 3: 1}


def while_arriving(next_one, refs, work):
    if next_one is None:
        return work(refs[0])
    _, place, width, span, below, into = next_one
    sources, (out, *targets, sems) = refs[:3], refs[3 + (into is not None):]
    buffers = (targets.pop(0) if span else None, targets.pop(0) if below else None)
    first, count = span or (0, 0)
    units, depths = streams(
        sources,
        buffers,
        sems,
        first_of(place),
        width,
        [(first + row, rows) for row, rows in parts_of(count, 128)] if span else [],
        parts_of(width, 32),
    )
    copies = units + [copy for pair in depths for copy in pair]
    for copy in copies:
        copy.start()
    pl.when(lax.axis_index("narrow") >= 0)(lambda: work(out))
    for copy in copies:
        copy.wait()


def forward_half(half, others, side_rows, weights, width, next_one=None):
    depth = half.shape[1]
    rows = half.shape[0] - side_rows
    inputs = [half, weights[0]] + ([weights[1], *others] if others else [])
    all_rows = rows + (side_rows if others else 0)

    def body(half_ref, both, *refs):
        refs = list(refs)
        below = refs.pop(0) if others else None
        side_refs = [refs.pop(0) for _ in others]

        def work(out):
            out[pl.ds(0, rows), :] = jnp.dot(
                half_ref[pl.ds(0, rows), :], both[...], preferred_element_type=jnp.float32
            ).astype(jnp.bfloat16)
            if others:
                side = jnp.concatenate([ref[pl.ds(rows, side_rows), :] for ref in side_refs])
                value = across(side, below[...]).astype(jnp.bfloat16)
                out[pl.ds(rows, side_rows), pl.ds(0, width)] = value[:side_rows]
                out[pl.ds(rows, side_rows), pl.ds(width, width)] = value[side_rows:]

        while_arriving(next_one, refs, work)

    operands, specs, more, scratch, aliases = extras(next_one, depth, len(inputs))
    return pl.pallas_call(
        body,
        out_shape=[jax.ShapeDtypeStruct((all_rows, 2 * width), jnp.bfloat16)] + more,
        in_specs=[VMEM] * len(inputs) + specs,
        out_specs=[VMEM] * (1 + len(more)),
        scratch_shapes=scratch,
        input_output_aliases=aliases,
        compiler_params=pltpu.CompilerParams(vmem_limit_bytes=4 * 1024 * 1024),
        cost_estimate=pl.CostEstimate(
            flops=4 * depth * width * all_rows, bytes_accessed=10**6, transcendentals=0
        ),
        name="forward_half",
    )(*inputs, *operands)


def forward(main, side, weights, place, width, dtype, next_one=None):
    rows, half = main.shape[0], side.shape[0] // 2
    depth = main.shape[1]
    by_depth, by_unit = parts_of(depth, 128), parts_of(width, 32)
    ready = len(weights) == 2

    def put_side(out, value):
        out[pl.ds(rows, half), pl.ds(0, width)] = value[:half].astype(dtype)
        out[pl.ds(rows, half), pl.ds(width, width)] = value[half:].astype(dtype)

    def body_ready(main_ref, side_ref, both, below, *refs):
        def work(out):
            out[pl.ds(0, rows), :] = jnp.dot(
                main_ref[...], both[...], preferred_element_type=jnp.float32
            ).astype(dtype)
            put_side(out, across(side_ref[...], below[...]))

        while_arriving(next_one, refs, work)

    def body(main_ref, side_ref, gate, up, down, out, both, below, total, sems):
        first = first_of(place)
        units, depths = streams((gate, up, down), (both, below), sems, first, width, by_depth, by_unit)
        for copy in units + [copy for pair in depths for copy in pair]:
            copy.start()
        for copy in units:
            copy.wait()
        put_side(out, across(side_ref[...], below[...]))
        for i, (row, count) in enumerate(by_depth):
            for copy in depths[i]:
                copy.wait()
            some = pl.ds(row, count)
            part = jnp.dot(main_ref[:, some], both[some, :], preferred_element_type=jnp.float32)
            if i > 0:
                part = total[...] + part
            if i == len(by_depth) - 1:
                out[pl.ds(0, rows), :] = part.astype(dtype)
            else:
                total[...] = part

    out_shape = [jax.ShapeDtypeStruct((rows + half, 2 * width), dtype)]
    operands = [main, side, *weights]
    specs = [VMEM] * 2 + [VMEM if ready else ANY] * len(weights)
    aliases = {}
    if ready:
        operands_more, specs_more, more, scratch, aliases = extras(next_one, depth, 4)
        operands += operands_more
        specs += specs_more
        out_shape += more
    else:
        scratch = [
            pltpu.VMEM((depth, 2 * width), jnp.bfloat16),
            pltpu.VMEM((width, depth), jnp.bfloat16),
            pltpu.VMEM((rows, 2 * width), jnp.float32),
            pltpu.SemaphoreType.DMA((3, 4)),
        ]
    return pl.pallas_call(
        body_ready if ready else body,
        out_shape=out_shape,
        in_specs=specs,
        out_specs=[VMEM] * len(out_shape),
        scratch_shapes=scratch,
        input_output_aliases=aliases,
        compiler_params=pltpu.CompilerParams(vmem_limit_bytes=(4 if ready else 20) * 1024 * 1024),
        cost_estimate=pl.CostEstimate(
            flops=4 * depth * width * (rows + half), bytes_accessed=6 * depth * width, transcendentals=0
        ),
        name="forward",
    )(*operands)


def coefficients(kept, received, picks, points, examples):
    width = kept.shape[1] // 2
    pairs, references = picks.shape[0] // examples, picks.shape[1] // 2
    rows = examples + references
    count = points.shape[0]
    lanes = 128 if width % 128 == 0 else width
    middle = examples // 2
    pieces, left = [], middle
    while left:
        size = 16 if left == 16 or left >= 32 else left
        pieces.append((middle - left, size))
        left -= size
    pieces += [(middle + first, size) for first, size in pieces]
    arrays = [array for item in received for array in (item if isinstance(item, tuple) else (item,))]
    scale = 1.0 / (pairs * count)

    def body(points_ref, picks_ref, kept_ref, *refs):
        out, base_gate, base_up = refs[-3:]
        refs = list(refs[:-3])
        got = [
            tuple(refs.pop(0) for _ in item) if isinstance(item, tuple) else refs.pop(0)
            for item in received
        ]
        picks = picks_ref[...]
        steps = [points_ref[m].astype(jnp.float32) * 0.125 for m in range(count)]
        steps_1 = sum(steps[1:], steps[0])
        steps_2 = sum((t * t for t in steps[1:]), steps[0] * steps[0])

        def total(take, *where):
            value = take(kept_ref, *where)
            for ref in got:
                value = value + take(ref, *where).astype(jnp.float32)
            return value

        def of_references(ref, lanes_of):
            if isinstance(ref, tuple):
                return jnp.concatenate([half[pl.ds(0, references // 2), lanes_of] for half in ref])
            return ref[pl.ds(0, references), lanes_of]

        for w, target in enumerate((base_gate, base_up)):
            value = total(of_references, pl.ds(w * width, width))
            high = value.astype(jnp.bfloat16)
            low = (value - high.astype(jnp.float32)).astype(jnp.bfloat16)
            target[...] = jnp.dot(
                picks, jnp.concatenate([high, low]), preferred_element_type=jnp.float32
            )

        def block(j, _):
            here = pl.ds(0, width) if lanes == width else pl.ds(pl.multiple_of(j * lanes, 128), lanes)
            if lanes == width:
                of = [pl.ds(w * width, width) for w in range(2)]
            else:
                of = [pl.ds(pl.multiple_of(w * width + j * lanes, 128), lanes) for w in range(2)]

            def of_examples(ref, first, size, w):
                if isinstance(ref, tuple):
                    h = first // middle
                    return ref[h][pl.ds(references // 2 + first - h * middle, size), of[w]]
                return ref[pl.ds(references + first, size), of[w]]

            def of_upstream(ref, h):
                ref, first = (ref[1], rows // 2) if isinstance(ref, tuple) else (ref, rows)
                return ref[pl.ds(first, middle), of[h]]

            upstream = [total(of_upstream, h) for h in range(2)]
            for first, piece in pieces:
                gate = total(of_examples, first, piece, 0) * 0.5
                up = total(of_examples, first, piece, 1)
                coef_gate = jnp.zeros_like(gate)
                coef_up = jnp.zeros_like(gate)
                for p in range(pairs):
                    start = base_gate[pl.ds(p * examples + first, piece), here] * 0.5
                    span = gate - start
                    flat = count + (count * start + steps_1 * span)
                    tilted = steps_1 + (steps_1 * start + steps_2 * span)
                    coef_up = coef_up + (count * start + steps_1 * span)
                    for t in steps:
                        half = start + t * span
                        v = jnp.tanh(half)
                        bent = half * v
                        turn = v - v * bent
                        coef_up = coef_up + bent
                        flat = flat + turn
                        tilted = tilted + t * turn
                    start_up = base_up[pl.ds(p * examples + first, piece), here]
                    coef_gate = coef_gate + (start_up * flat + (up - start_up) * tilted)
                base_gate[pl.ds(first, piece), here] = coef_gate * (0.5 * scale)
                base_up[pl.ds(first, piece), here] = coef_up * scale
            for w, source in enumerate((base_gate, base_up)):
                for h in range(2):
                    some = pl.ds(h * middle, middle)
                    out[some, of[w]] = (upstream[h] * source[some, here]).astype(jnp.bfloat16)
            return 0

        lax.fori_loop(0, width // lanes, block, 0)

    return pl.pallas_call(
        body,
        out_shape=jax.ShapeDtypeStruct((examples, 2 * width), jnp.bfloat16),
        in_specs=[SMEM, VMEM, VMEM] + [VMEM] * len(arrays),
        out_specs=VMEM,
        scratch_shapes=[pltpu.VMEM((pairs * examples, width), jnp.float32)] * 2,
        compiler_params=pltpu.CompilerParams(vmem_limit_bytes=4 * 1024 * 1024),
        cost_estimate=pl.CostEstimate(flops=5 * 10**9, bytes_accessed=10**6, transcendentals=0),
        name="coefficients",
    )(points, picks, kept, *arrays)


def backward(items, total, final, span=None):
    grads, weights, place = items[0]
    rows, width, depth = grads.shape[0], grads.shape[1] // 2, weights[0].shape[0]
    low, columns = span or (0, depth)
    by_depth = [(low + row, count) for row, count in (parts_of(columns, 128) if len(weights) > 1 else [(0, columns)])]
    ready = len(weights) == 1

    def body(*refs):
        grads_refs, refs = refs[:len(items)], refs[len(items):]
        if ready:
            boths, outs = refs[:len(items)], refs[len(items):]
        else:
            gate, up, *outs, both, sems = refs
            boths = [both]
            _, depths = streams((gate, up, None), (both, None), sems, first_of(place), width, by_depth, [])
            for pair in depths:
                for copy in pair:
                    copy.start()
        for i, (row, count) in enumerate(by_depth):
            some, own = pl.ds(row, count), pl.ds(row - low, count)
            if not ready:
                for copy in depths[i]:
                    copy.wait()
            value = None if total is None else outs[0][:, some]
            for grads_ref, both in zip(grads_refs, boths):
                part = across(grads_ref[...], both[some, :])
                value = part if value is None else value + part
            if final:
                outs[-2][:, own] = value[rows // 2:, :].astype(jnp.bfloat16)
                outs[-1][:, own] = value[:rows // 2, :]
            else:
                outs[-1][:, own] = value

    operands = [item[0] for item in items] + [w for item in items for w in item[1]]
    specs = [VMEM] * len(items) + [VMEM if ready else ANY] * (len(operands) - len(items))
    if total is not None:
        operands.append(total)
        specs.append(VMEM)
    if final:
        out_shape = (
            jax.ShapeDtypeStruct((rows // 2, columns), jnp.bfloat16),
            jax.ShapeDtypeStruct((rows // 2, columns), jnp.float32),
        )
        out_specs = (VMEM, VMEM)
    else:
        out_shape, out_specs = jax.ShapeDtypeStruct((rows, columns), jnp.float32), VMEM
    scratch = [pltpu.VMEM((depth, 2 * width), jnp.bfloat16), pltpu.SemaphoreType.DMA((2, 4))]
    return pl.pallas_call(
        body,
        out_shape=out_shape,
        in_specs=specs,
        out_specs=out_specs,
        scratch_shapes=[] if ready else scratch,
        compiler_params=pltpu.CompilerParams(vmem_limit_bytes=(4 if ready else 12) * 1024 * 1024),
        cost_estimate=pl.CostEstimate(
            flops=2 * rows * columns * sum(item[0].shape[1] for item in items),
            bytes_accessed=4 * width * columns,
            transcendentals=0,
        ),
        name="backward",
    )(*operands)


def choices(pair_ref, dims, e, r):
    far, near, pair = dims
    blocks = far * near * pair
    examples, pairs = pair_ref.shape

    def body(pair_ref, out, rows, table):
        table[pl.ds(0, examples), :] = pair_ref[...]
        at = lax.axis_index("wide")
        z, y, c = at // (near * pair), at // pair % near, at % pair
        col = lax.broadcasted_iota(jnp.int32, (examples, blocks * r), 1)
        name = jnp.zeros_like(col)
        for q in range(blocks):
            s, b, p = halvings(far)[q % far], q // far % near, q // (far * near)
            owner = ((z ^ s) * near + (y ^ b)) * pair + (c ^ p)
            rows[pl.ds(q * e, e), :] = table[pl.ds(owner * e, e), :]
            name = jnp.where((col >= q * r) & (col < (q + 1) * r), owner * r + col - q * r, name)
        for p in range(pairs):
            pick = (rows[:, pl.ds(p, 1)] == name).astype(jnp.float32).astype(jnp.bfloat16)
            for h in range(2):
                out[pl.ds(p * examples, examples), pl.ds(h * blocks * r, blocks * r)] = pick

    return pl.pallas_call(
        body,
        out_shape=jax.ShapeDtypeStruct((pairs * examples, 2 * blocks * r), jnp.bfloat16),
        in_specs=[VMEM],
        out_specs=VMEM,
        scratch_shapes=[
            pltpu.VMEM((examples, pairs), jnp.int32),
            pltpu.VMEM((rounded(examples, 8) + 8, pairs), jnp.int32),
        ],
        compiler_params=pltpu.CompilerParams(vmem_limit_bytes=2 * 1024 * 1024),
        cost_estimate=pl.CostEstimate(flops=10**9, bytes_accessed=10**6, transcendentals=0),
        name="choices",
    )(pair_ref)


def chunks_of(width):
    if width % 128 or width < 512:
        return [(0, rounded(width, 128))]
    first = rounded(width // 2, 256)
    return [(0, first), (first, width - first)]


def on_device(
    examples, references, gate_weight, up_weight, down_weight, cotangent, pair_ref, points
):
    dims = factors(lax.axis_size("wide"))
    far, near, pair = dims
    peers = lax.axis_size("narrow")
    e, r, k = examples.shape[0], references.shape[0], cotangent.shape[0]
    depth, hidden = gate_weight.shape
    blocks = far * near * pair

    share = hidden // peers
    whole_weights = [gate_weight, up_weight, down_weight]
    aligned = share % 128 == 0
    ahead = aligned and peers == 2
    if aligned:
        whole_weights = [
            pltpu.with_memory_space_constraint(w, pltpu.MemorySpace.HBM) for w in whole_weights
        ]
    chunks = chunks_of(share)
    picks = choices(pair_ref, dims, e, r)

    def at_peer(steps, offset, width):
        if aligned:
            return whole_weights, (steps % peers, peers, share, offset)
        start = (lax.axis_index("narrow") + steps) % peers * share
        more = width - share

        def cut(weight, axis):
            piece = lax.dynamic_slice_in_dim(weight, start, share, axis)
            return jnp.pad(piece, [(0, more if d == axis else 0) for d in range(2)])

        return [cut(gate_weight, 1), cut(up_weight, 1), cut(down_weight, 0)], None

    own, whole, pieces = pack([references, examples, cotangent])
    column = {0: own}
    step = far // 2
    while step:
        for s in sorted(column):
            column[s + step] = permute(column[s], "wide", dims, 0, step)
        step //= 2
    beside = {}
    if near == 2:
        for s, block in column.items():
            beside[s] = permute(block, "wide", dims, 1, 1)
    order = halvings(far)
    plane = [column[s] for s in order] + [beside[s] for s in order if near == 2]
    half = assemble(plane, whole, pieces, (r, e, k), depth)
    blocks_of_weights = {}
    early = ahead and pair == 2 and len(chunks) == 2
    if ahead:
        wanted = [(1, chunk) for chunk in chunks] + [(0, chunk) for chunk in chunks[1 if early else 0:]]
        for s, chunk in wanted:
            blocks_of_weights[s, chunk[0]] = fetch(*at_peer(s, *chunk), chunk[1])
    halves = [half]
    if pair == 2:
        halves.append(permute(half, "wide", dims, 2, 1))

    parts = []
    if early:
        (offset, width), (next_offset, next_width) = chunks
        weights = blocks_of_weights[1, offset]
        count = half.shape[0] // (r + e + k) * k
        kept_one = (*at_peer(0, offset, width), width)
        (sent,) = forward_half(halves[0], [], count, weights, width)
        received = [shift(sent, peers, 1)]
        upper = (*kept_one, (0, depth // 2), False, None)
        sent, both = forward_half(halves[1], halves, count, weights, width, upper)
        received.append(shift(sent, peers, 1))
        parts.append((offset, width, [tuple(received)]))
    main, side = join(halves, (r, e, k))
    if early:
        lower = (*kept_one, (depth // 2, depth - depth // 2), False, both)
        weights = blocks_of_weights[1, next_offset]
        sent, both = forward(main, side, weights, None, next_width, jnp.bfloat16, lower)
        parts.append((next_offset, next_width, [shift(sent, peers, 1)]))
        weights = blocks_of_weights[0, next_offset]
        kept_last, below = forward(
            main, side, weights, None, next_width, jnp.float32, (*kept_one, None, True, None)
        )
        blocks_of_weights[0, offset] = (both, below)
    else:
        for offset, width in chunks:
            received = []
            for s in range(1, peers):
                weights, place = at_peer(s, offset, width)
                if ahead:
                    weights = blocks_of_weights[s, offset]
                (sent,) = forward(main, side, weights, place, width, jnp.bfloat16)
                received.append(shift(sent, peers, s))
            parts.append((offset, width, received))

    jobs = []
    for i, (offset, width, received) in enumerate(parts):
        weights, place = at_peer(0, offset, width)
        if ahead:
            weights = blocks_of_weights[0, offset]
        if early and i == 1:
            kept = kept_last
        else:
            (kept,) = forward(main, side, weights, place, width, jnp.float32)
        grads = coefficients(kept, received, picks, points, blocks * e)
        jobs.append((grads, offset, width, 0))
        jobs += [(shift(grads, peers, s), offset, width, s) for s in range(1, peers)]
    items = []
    for grads, offset, width, s in jobs:
        weights, place = at_peer(peers - s, offset, width)
        weights = blocks_of_weights[s, offset][:1] if ahead else weights[:2]
        items.append((grads, weights, place))
    if ahead and len(items) == 4:
        groups = [items[:1], items[1:3], items[3:]]
    else:
        groups = [[item] for item in items]
    total = None
    for group in groups[:-1]:
        total = backward(group, total, False)
    cut = depth // 2 if depth % 1024 else depth // 8 * 5
    spans = [(0, cut), (cut, depth - cut)] if depth % 256 == 0 else [(0, depth)]
    last = [backward(groups[-1], total, pair == 2, span) for span in spans]

    results = []
    for i, value in enumerate(last):
        if pair == 2:
            sent, kept = value
            value = kept + permute(sent, "wide", dims, 2, 1).astype(jnp.float32)
        digits = [(1, 1)] * (near == 2) + [(0, 1 << bit) for bit in range(far.bit_length() - 1)]
        steps = list(digits)
        if i % 2 and len(steps) > 1:
            steps[:2] = steps[1::-1]
        for step in steps:
            at = digits.index(step)
            outer, inner = 1 << at, value.shape[0] >> (at + 1)
            digits.remove(step)

            def half(which):
                rows = [value[(2 * o + which) * inner:(2 * o + which + 1) * inner] for o in range(outer)]
                return rows[0] if outer == 1 else jnp.concatenate(rows)

            got = permute(half(1).astype(jnp.bfloat16), "wide", dims, *step)
            value = half(0) + got.astype(jnp.float32)
        results.append(value)
    return jnp.concatenate(results, axis=1).astype(jnp.bfloat16)


def solution(mesh):
    in_specs = (
        P("wide", "narrow"),
        P("wide", "narrow"),
        P("narrow", "wide"),
        P("narrow", "wide"),
        P("wide", "narrow"),
        P("wide", "narrow"),
        P(),
        P(),
    )
    out_specs = P("wide", "narrow")
    return jax.shard_map(on_device, mesh=mesh, in_specs=in_specs, out_specs=out_specs, check_vma=False)
```

```python
import jax
import jax.numpy as jnp
from jax import lax
from jax.experimental import pallas as pl
from jax.experimental.pallas import tpu as pltpu
from jax.sharding import PartitionSpec as P


VMEM = pl.BlockSpec(memory_space=pltpu.VMEM)
SMEM = pl.BlockSpec(memory_space=pltpu.SMEM)
ANY = pl.BlockSpec(memory_space=pl.ANY)


def factors(size):
    pair = 2 if size % 2 == 0 else 1
    near = 2 if (size // pair) % 2 == 0 else 1
    return size // (pair * near), near, pair


def rounded(rows, unit):
    return -(-rows // unit) * unit


def permute(array, axis, dims, digit, amount):
    below = 1
    for size in dims[digit + 1:]:
        below *= size
    total = below
    for size in dims[:digit + 1]:
        total *= size
    pairs = [
        (at, at + (((at // below) % dims[digit] ^ amount) - (at // below) % dims[digit]) * below)
        for at in range(total)
    ]
    return lax.ppermute(array, axis, pairs)


def shift(array, size, amount):
    return lax.ppermute(array, "narrow", [(at, (at + amount) % size) for at in range(size)])


def halvings(size):
    if size == 1:
        return [0]
    return [2 * v for v in halvings(size // 2)] + [2 * v + 1 for v in halvings(size // 2)]


def pack(arrays):
    count, width = sum(a.shape[0] for a in arrays), arrays[0].shape[1]
    whole = count // 8 * 8
    rest = count - whole
    pieces = whole // rest if rest and whole else 1
    cut = rest > 0 and whole > 0 and whole % rest == 0 and width % (pieces * 128) == 0
    if not cut:
        whole, pieces = rounded(count, 8), 1
    lanes = width // pieces

    def body(*refs):
        sources, (out, *held, sems) = refs[:len(arrays)], refs[len(arrays):]
        copies = [
            pltpu.make_async_copy(source, target, sems.at[i])
            for i, (source, target) in enumerate(zip(sources, held))
        ]
        for copy in copies:
            copy.start()
        for copy in copies:
            copy.wait()
        rows = jnp.concatenate([ref[...].astype(jnp.float32) for ref in held])
        if not cut:
            if whole > count:
                rows = jnp.concatenate([rows, jnp.zeros((whole - count, width), jnp.float32)])
            out[...] = rows.astype(out.dtype)
            return
        out[:, pl.ds(0, width)] = rows[:whole].astype(out.dtype)
        beside = [
            rows[whole + i:whole + i + 1, j * lanes:(j + 1) * lanes]
            for i in range(rest)
            for j in range(pieces)
        ]
        out[:, pl.ds(width, lanes)] = jnp.concatenate(beside).astype(out.dtype)

    packed = pl.pallas_call(
        body,
        out_shape=jax.ShapeDtypeStruct((whole, width + lanes if cut else width), arrays[0].dtype),
        in_specs=[ANY] * len(arrays),
        out_specs=VMEM,
        scratch_shapes=[pltpu.VMEM(a.shape, a.dtype) for a in arrays]
        + [pltpu.SemaphoreType.DMA((len(arrays),))],
        compiler_params=pltpu.CompilerParams(vmem_limit_bytes=4 * 1024 * 1024),
        name="pack",
    )(*(pltpu.with_memory_space_constraint(a, pltpu.MemorySpace.HBM) for a in arrays))
    return packed, whole, pieces


def assemble(own, whole, pieces, counts, width):
    blocks = len(own)
    packed = own[0].shape
    total = blocks * sum(counts)
    across_lanes = width // pieces

    def body(*refs):
        out, stack = refs[-2], refs[-1]
        for b in range(blocks):
            stack[pl.ds(b * packed[0], packed[0]), :] = refs[b][...]
        row = lax.broadcasted_iota(jnp.int32, (total, blocks * packed[0]), 0)
        col = lax.broadcasted_iota(jnp.int32, (total, blocks * packed[0]), 1)
        held = jnp.zeros_like(row)
        block = jnp.zeros_like(row)
        at = first = 0
        for count in counts:
            for b in range(blocks):
                inside = (row >= at) & (row < at + count)
                held = jnp.where(inside, row - at + first, held)
                block = jnp.where(inside, b, block)
                at += count
            first += count

        def pick(wanted, valid):
            return (valid & (col == wanted)).astype(jnp.float32).astype(jnp.bfloat16)

        base = block * packed[0]
        uncut = pick(base + held, held < whole)
        for j in range(pieces):
            lanes = pl.ds(j * across_lanes, across_lanes)
            value = jnp.dot(uncut, stack[:, lanes], preferred_element_type=jnp.float32)
            if packed[1] > width:
                value = value + jnp.dot(
                    pick(base + (held - whole) * pieces + j, held >= whole),
                    stack[:, pl.ds(width, across_lanes)],
                    preferred_element_type=jnp.float32,
                )
            out[:, lanes] = value.astype(jnp.bfloat16)

    dtype = own[0].dtype
    return pl.pallas_call(
        body,
        out_shape=jax.ShapeDtypeStruct((total, width), dtype),
        in_specs=[VMEM] * blocks,
        out_specs=VMEM,
        scratch_shapes=[pltpu.VMEM((blocks * packed[0], packed[1]), dtype)],
        compiler_params=pltpu.CompilerParams(vmem_limit_bytes=6 * 1024 * 1024),
        cost_estimate=pl.CostEstimate(flops=10**9, bytes_accessed=10**6, transcendentals=0),
        name="assemble",
    )(*own)


def join(halves, layout):
    width = halves[0].shape[1]
    blocks = halves[0].shape[0] // sum(layout)
    e, r, k = (blocks * rows for rows in layout)
    count = len(halves)

    def body(*refs):
        main, side = refs[-2:]
        for h in range(count):
            main[pl.ds(h * e, e), :] = refs[h][pl.ds(0, e), :]
            main[pl.ds(count * e + h * r, r), :] = refs[h][pl.ds(e, r), :]
            side[pl.ds(h * k, k), :] = refs[h][pl.ds(e + r, k), :]

    dtype = halves[0].dtype
    return pl.pallas_call(
        body,
        out_shape=(
            jax.ShapeDtypeStruct((count * (e + r), width), dtype),
            jax.ShapeDtypeStruct((count * k, width), dtype),
        ),
        in_specs=[VMEM] * count,
        out_specs=(VMEM, VMEM),
        compiler_params=pltpu.CompilerParams(vmem_limit_bytes=4 * 1024 * 1024),
        cost_estimate=pl.CostEstimate(flops=10**9, bytes_accessed=10**6, transcendentals=0),
        name="join",
    )(*halves)


def across(left, right):
    return lax.dot_general(left, right, (((1,), (1,)), ((), ())), preferred_element_type=jnp.float32)


def parts_of(size, unit):
    for count in (4, 2):
        if size % (count * unit) == 0:
            return [(i * (size // count), size // count) for i in range(count)]
    return [(0, size)]


def first_of(place):
    if place is None:
        return 0
    steps, peers, share, offset = place
    return pl.multiple_of((lax.axis_index("narrow") + steps) % peers * share + offset, 128)


def streams(weights, buffers, sems, first, width, by_depth, by_unit):
    gate, up, down = weights
    both, below = buffers
    units, depths = [], []
    for i, (row, count) in enumerate(by_unit if below is not None else ()):
        units.append(
            pltpu.make_async_copy(
                down.at[pl.ds(first + row, count)], below.at[pl.ds(row, count)], sems.at[2, i]
            )
        )
    for i, (row, count) in enumerate(by_depth if both is not None else ()):
        some = pl.ds(row, count)
        depths.append(
            [
                pltpu.make_async_copy(
                    source.at[some, pl.ds(first, width)],
                    both.at[some, pl.ds(w * width, width)],
                    sems.at[w, i],
                )
                for w, source in enumerate((gate, up))
            ]
        )
    return units, depths


def fetch(weights, place, width):
    depth = weights[0].shape[0]
    by_depth, by_unit = parts_of(depth, 128), parts_of(width, 32)

    def body(gate, up, down, both, below, sems):
        first = first_of(place)
        units, depths = streams((gate, up, down), (both, below), sems, first, width, by_depth, by_unit)
        copies = units + [copy for pair in depths for copy in pair]
        for copy in copies:
            copy.start()
        for copy in copies:
            copy.wait()

    return pl.pallas_call(
        body,
        out_shape=(
            pltpu.VMEM((depth, 2 * width), jnp.bfloat16),
            pltpu.VMEM((width, depth), jnp.bfloat16),
        ),
        in_specs=[ANY, ANY, ANY],
        out_specs=(VMEM, VMEM),
        scratch_shapes=[pltpu.SemaphoreType.DMA((3, 4))],
        compiler_params=pltpu.CompilerParams(vmem_limit_bytes=1024 * 1024),
        cost_estimate=pl.CostEstimate(
            flops=4 * 10**9, bytes_accessed=6 * depth * width, transcendentals=0
        ),
        name="fetch",
    )(*weights)


def arriving(next_one, depth):
    _, _, width, span, below, _ = next_one
    return [pltpu.VMEM((depth, 2 * width), jnp.bfloat16)] * (span is not None) + [
        pltpu.VMEM((width, depth), jnp.bfloat16)
    ] * below


def extras(next_one, depth, at):
    if next_one is None:
        return [], [], [], [], {}
    weights, _, _, _, _, into = next_one
    more = arriving(next_one, depth)
    scratch = [pltpu.SemaphoreType.DMA((3, 4))]
    if into is None:
        return [*weights], [ANY] * 3, more, scratch, {}
    return [*weights, into], [ANY] * 3 + [VMEM], more, scratch, {at + 3: 1}


def while_arriving(next_one, refs, work):
    if next_one is None:
        return work(refs[0])
    _, place, width, span, below, into = next_one
    sources, (out, *targets, sems) = refs[:3], refs[3 + (into is not None):]
    buffers = (targets.pop(0) if span else None, targets.pop(0) if below else None)
    first, count = span or (0, 0)
    units, depths = streams(
        sources,
        buffers,
        sems,
        first_of(place),
        width,
        [(first + row, rows) for row, rows in parts_of(count, 128)] if span else [],
        parts_of(width, 32),
    )
    copies = units + [copy for pair in depths for copy in pair]
    for copy in copies:
        copy.start()
    pl.when(lax.axis_index("narrow") >= 0)(lambda: work(out))
    for copy in copies:
        copy.wait()


def forward_half(half, others, side_rows, weights, width, next_one=None):
    depth = half.shape[1]
    rows = half.shape[0] - side_rows
    inputs = [half, weights[0]] + ([weights[1], *others] if others else [])
    all_rows = rows + (side_rows if others else 0)

    def body(half_ref, both, *refs):
        refs = list(refs)
        below = refs.pop(0) if others else None
        side_refs = [refs.pop(0) for _ in others]

        def work(out):
            out[pl.ds(0, rows), :] = jnp.dot(
                half_ref[pl.ds(0, rows), :], both[...], preferred_element_type=jnp.float32
            ).astype(jnp.bfloat16)
            if others:
                side = jnp.concatenate([ref[pl.ds(rows, side_rows), :] for ref in side_refs])
                value = across(side, below[...]).astype(jnp.bfloat16)
                out[pl.ds(rows, side_rows), pl.ds(0, width)] = value[:side_rows]
                out[pl.ds(rows, side_rows), pl.ds(width, width)] = value[side_rows:]

        while_arriving(next_one, refs, work)

    operands, specs, more, scratch, aliases = extras(next_one, depth, len(inputs))
    return pl.pallas_call(
        body,
        out_shape=[jax.ShapeDtypeStruct((all_rows, 2 * width), jnp.bfloat16)] + more,
        in_specs=[VMEM] * len(inputs) + specs,
        out_specs=[VMEM] * (1 + len(more)),
        scratch_shapes=scratch,
        input_output_aliases=aliases,
        compiler_params=pltpu.CompilerParams(vmem_limit_bytes=4 * 1024 * 1024),
        cost_estimate=pl.CostEstimate(
            flops=4 * depth * width * all_rows, bytes_accessed=10**6, transcendentals=0
        ),
        name="forward_half",
    )(*inputs, *operands)


def forward(main, side, weights, place, width, dtype, next_one=None):
    rows, half = main.shape[0], side.shape[0] // 2
    depth = main.shape[1]
    by_depth, by_unit = parts_of(depth, 128), parts_of(width, 32)
    ready = len(weights) == 2

    def put_side(out, value):
        out[pl.ds(rows, half), pl.ds(0, width)] = value[:half].astype(dtype)
        out[pl.ds(rows, half), pl.ds(width, width)] = value[half:].astype(dtype)

    def body_ready(main_ref, side_ref, both, below, *refs):
        def work(out):
            out[pl.ds(0, rows), :] = jnp.dot(
                main_ref[...], both[...], preferred_element_type=jnp.float32
            ).astype(dtype)
            put_side(out, across(side_ref[...], below[...]))

        while_arriving(next_one, refs, work)

    def body(main_ref, side_ref, gate, up, down, out, both, below, total, sems):
        first = first_of(place)
        units, depths = streams((gate, up, down), (both, below), sems, first, width, by_depth, by_unit)
        for copy in units + [copy for pair in depths for copy in pair]:
            copy.start()
        for copy in units:
            copy.wait()
        put_side(out, across(side_ref[...], below[...]))
        for i, (row, count) in enumerate(by_depth):
            for copy in depths[i]:
                copy.wait()
            some = pl.ds(row, count)
            part = jnp.dot(main_ref[:, some], both[some, :], preferred_element_type=jnp.float32)
            if i > 0:
                part = total[...] + part
            if i == len(by_depth) - 1:
                out[pl.ds(0, rows), :] = part.astype(dtype)
            else:
                total[...] = part

    out_shape = [jax.ShapeDtypeStruct((rows + half, 2 * width), dtype)]
    operands = [main, side, *weights]
    specs = [VMEM] * 2 + [VMEM if ready else ANY] * len(weights)
    aliases = {}
    if ready:
        operands_more, specs_more, more, scratch, aliases = extras(next_one, depth, 4)
        operands += operands_more
        specs += specs_more
        out_shape += more
    else:
        scratch = [
            pltpu.VMEM((depth, 2 * width), jnp.bfloat16),
            pltpu.VMEM((width, depth), jnp.bfloat16),
            pltpu.VMEM((rows, 2 * width), jnp.float32),
            pltpu.SemaphoreType.DMA((3, 4)),
        ]
    return pl.pallas_call(
        body_ready if ready else body,
        out_shape=out_shape,
        in_specs=specs,
        out_specs=[VMEM] * len(out_shape),
        scratch_shapes=scratch,
        input_output_aliases=aliases,
        compiler_params=pltpu.CompilerParams(vmem_limit_bytes=(4 if ready else 20) * 1024 * 1024),
        cost_estimate=pl.CostEstimate(
            flops=4 * depth * width * (rows + half), bytes_accessed=6 * depth * width, transcendentals=0
        ),
        name="forward",
    )(*operands)


def coefficients(kept, received, picks, points, examples):
    width = kept.shape[1] // 2
    pairs, references = picks.shape[0] // examples, picks.shape[1] // 2
    rows = examples + references
    count = points.shape[0]
    lanes = 128 if width % 128 == 0 else width
    middle = examples // 2
    pieces, left = [], middle
    while left:
        size = 16 if left == 16 or left >= 32 else left
        pieces.append((middle - left, size))
        left -= size
    pieces += [(middle + first, size) for first, size in pieces]
    arrays = [array for item in received for array in (item if isinstance(item, tuple) else (item,))]
    scale = 1.0 / (pairs * count)

    def body(points_ref, picks_ref, kept_ref, *refs):
        out, base_gate, base_up = refs[-3:]
        refs = list(refs[:-3])
        got = [
            tuple(refs.pop(0) for _ in item) if isinstance(item, tuple) else refs.pop(0)
            for item in received
        ]
        picks = picks_ref[...]
        steps = [points_ref[m].astype(jnp.float32) * 0.125 for m in range(count)]
        steps_1 = sum(steps[1:], steps[0])
        steps_2 = sum((t * t for t in steps[1:]), steps[0] * steps[0])

        def total(take, *where):
            value = take(kept_ref, *where)
            for ref in got:
                value = value + take(ref, *where).astype(jnp.float32)
            return value

        def of_references(ref, lanes_of):
            if isinstance(ref, tuple):
                return jnp.concatenate([half[pl.ds(0, references // 2), lanes_of] for half in ref])
            return ref[pl.ds(0, references), lanes_of]

        for w, target in enumerate((base_gate, base_up)):
            value = total(of_references, pl.ds(w * width, width))
            high = value.astype(jnp.bfloat16)
            low = (value - high.astype(jnp.float32)).astype(jnp.bfloat16)
            target[...] = jnp.dot(
                picks, jnp.concatenate([high, low]), preferred_element_type=jnp.float32
            )

        def block(j, _):
            here = pl.ds(0, width) if lanes == width else pl.ds(pl.multiple_of(j * lanes, 128), lanes)
            if lanes == width:
                of = [pl.ds(w * width, width) for w in range(2)]
            else:
                of = [pl.ds(pl.multiple_of(w * width + j * lanes, 128), lanes) for w in range(2)]

            def of_examples(ref, first, size, w):
                if isinstance(ref, tuple):
                    h = first // middle
                    return ref[h][pl.ds(references // 2 + first - h * middle, size), of[w]]
                return ref[pl.ds(references + first, size), of[w]]

            def of_upstream(ref, h):
                ref, first = (ref[1], rows // 2) if isinstance(ref, tuple) else (ref, rows)
                return ref[pl.ds(first, middle), of[h]]

            upstream = [total(of_upstream, h) for h in range(2)]
            for first, piece in pieces:
                gate = total(of_examples, first, piece, 0) * 0.5
                up = total(of_examples, first, piece, 1)
                coef_gate = jnp.zeros_like(gate)
                coef_up = jnp.zeros_like(gate)
                for p in range(pairs):
                    start = base_gate[pl.ds(p * examples + first, piece), here] * 0.5
                    span = gate - start
                    flat = count + (count * start + steps_1 * span)
                    tilted = steps_1 + (steps_1 * start + steps_2 * span)
                    coef_up = coef_up + (count * start + steps_1 * span)
                    for t in steps:
                        half = start + t * span
                        v = jnp.tanh(half)
                        bent = half * v
                        turn = v - v * bent
                        coef_up = coef_up + bent
                        flat = flat + turn
                        tilted = tilted + t * turn
                    start_up = base_up[pl.ds(p * examples + first, piece), here]
                    coef_gate = coef_gate + (start_up * flat + (up - start_up) * tilted)
                base_gate[pl.ds(first, piece), here] = coef_gate * (0.5 * scale)
                base_up[pl.ds(first, piece), here] = coef_up * scale
            for w, source in enumerate((base_gate, base_up)):
                for h in range(2):
                    some = pl.ds(h * middle, middle)
                    out[some, of[w]] = (upstream[h] * source[some, here]).astype(jnp.bfloat16)
            return 0

        lax.fori_loop(0, width // lanes, block, 0)

    return pl.pallas_call(
        body,
        out_shape=jax.ShapeDtypeStruct((examples, 2 * width), jnp.bfloat16),
        in_specs=[SMEM, VMEM, VMEM] + [VMEM] * len(arrays),
        out_specs=VMEM,
        scratch_shapes=[pltpu.VMEM((pairs * examples, width), jnp.float32)] * 2,
        compiler_params=pltpu.CompilerParams(vmem_limit_bytes=4 * 1024 * 1024),
        cost_estimate=pl.CostEstimate(flops=5 * 10**9, bytes_accessed=10**6, transcendentals=0),
        name="coefficients",
    )(points, picks, kept, *arrays)


def backward(items, total, final, span=None):
    grads, weights, place = items[0]
    rows, width, depth = grads.shape[0], grads.shape[1] // 2, weights[0].shape[0]
    low, columns = span or (0, depth)
    by_depth = [(low + row, count) for row, count in (parts_of(columns, 128) if len(weights) > 1 else [(0, columns)])]
    ready = len(weights) == 1

    def body(*refs):
        grads_refs, refs = refs[:len(items)], refs[len(items):]
        if ready:
            boths, outs = refs[:len(items)], refs[len(items):]
        else:
            gate, up, *outs, both, sems = refs
            boths = [both]
            _, depths = streams((gate, up, None), (both, None), sems, first_of(place), width, by_depth, [])
            for pair in depths:
                for copy in pair:
                    copy.start()
        for i, (row, count) in enumerate(by_depth):
            some, own = pl.ds(row, count), pl.ds(row - low, count)
            if not ready:
                for copy in depths[i]:
                    copy.wait()
            value = None if total is None else outs[0][:, some]
            for grads_ref, both in zip(grads_refs, boths):
                part = across(grads_ref[...], both[some, :])
                value = part if value is None else value + part
            if final:
                outs[-2][:, own] = value[rows // 2:, :].astype(jnp.bfloat16)
                outs[-1][:, own] = value[:rows // 2, :]
            else:
                outs[-1][:, own] = value

    operands = [item[0] for item in items] + [w for item in items for w in item[1]]
    specs = [VMEM] * len(items) + [VMEM if ready else ANY] * (len(operands) - len(items))
    if total is not None:
        operands.append(total)
        specs.append(VMEM)
    if final:
        out_shape = (
            jax.ShapeDtypeStruct((rows // 2, columns), jnp.bfloat16),
            jax.ShapeDtypeStruct((rows // 2, columns), jnp.float32),
        )
        out_specs = (VMEM, VMEM)
    else:
        out_shape, out_specs = jax.ShapeDtypeStruct((rows, columns), jnp.float32), VMEM
    scratch = [pltpu.VMEM((depth, 2 * width), jnp.bfloat16), pltpu.SemaphoreType.DMA((2, 4))]
    return pl.pallas_call(
        body,
        out_shape=out_shape,
        in_specs=specs,
        out_specs=out_specs,
        scratch_shapes=[] if ready else scratch,
        compiler_params=pltpu.CompilerParams(vmem_limit_bytes=(4 if ready else 12) * 1024 * 1024),
        cost_estimate=pl.CostEstimate(
            flops=2 * rows * columns * sum(item[0].shape[1] for item in items),
            bytes_accessed=4 * width * columns,
            transcendentals=0,
        ),
        name="backward",
    )(*operands)


def choices(pair_ref, dims, e, r):
    far, near, pair = dims
    blocks = far * near * pair
    examples, pairs = pair_ref.shape

    long = rounded(examples + 8, 128)

    def body(turned, out, rows, wide, table):
        wide[...] = jnp.zeros_like(wide)
        wide[pl.ds(0, pairs), pl.ds(0, examples)] = turned[...]
        table[...] = wide[...].T
        at = lax.axis_index("wide")
        z, y, c = at // (near * pair), at // pair % near, at % pair
        col = lax.broadcasted_iota(jnp.int32, (examples, blocks * r), 1)
        name = jnp.zeros_like(col)
        for q in range(blocks):
            s, b, p = halvings(far)[q % far], q // far % near, q // (far * near)
            owner = ((z ^ s) * near + (y ^ b)) * pair + (c ^ p)
            rows[pl.ds(q * e, e), :] = table[pl.ds(owner * e, e), pl.ds(0, pairs)]
            name = jnp.where((col >= q * r) & (col < (q + 1) * r), owner * r + col - q * r, name)
        for p in range(pairs):
            pick = (rows[:, pl.ds(p, 1)] == name).astype(jnp.float32).astype(jnp.bfloat16)
            for h in range(2):
                out[pl.ds(p * examples, examples), pl.ds(h * blocks * r, blocks * r)] = pick

    return pl.pallas_call(
        body,
        out_shape=jax.ShapeDtypeStruct((pairs * examples, 2 * blocks * r), jnp.bfloat16),
        in_specs=[VMEM],
        out_specs=VMEM,
        scratch_shapes=[
            pltpu.VMEM((examples, pairs), jnp.int32),
            pltpu.VMEM((128, long), jnp.int32),
            pltpu.VMEM((long, 128), jnp.int32),
        ],
        compiler_params=pltpu.CompilerParams(vmem_limit_bytes=2 * 1024 * 1024),
        cost_estimate=pl.CostEstimate(flops=10**9, bytes_accessed=10**6, transcendentals=0),
        name="choices",
    )(pair_ref.T)


def chunks_of(width):
    if width % 128 or width < 512:
        return [(0, rounded(width, 128))]
    first = rounded(width // 2, 256)
    return [(0, first), (first, width - first)]


def on_device(
    examples, references, gate_weight, up_weight, down_weight, cotangent, pair_ref, points
):
    dims = factors(lax.axis_size("wide"))
    far, near, pair = dims
    peers = lax.axis_size("narrow")
    e, r, k = examples.shape[0], references.shape[0], cotangent.shape[0]
    depth, hidden = gate_weight.shape
    blocks = far * near * pair

    share = hidden // peers
    whole_weights = [gate_weight, up_weight, down_weight]
    aligned = share % 128 == 0
    ahead = aligned and peers == 2
    if aligned:
        whole_weights = [
            pltpu.with_memory_space_constraint(w, pltpu.MemorySpace.HBM) for w in whole_weights
        ]
    chunks = chunks_of(share)
    picks = choices(pair_ref, dims, e, r)

    def at_peer(steps, offset, width):
        if aligned:
            return whole_weights, (steps % peers, peers, share, offset)
        start = (lax.axis_index("narrow") + steps) % peers * share
        more = width - share

        def cut(weight, axis):
            piece = lax.dynamic_slice_in_dim(weight, start, share, axis)
            return jnp.pad(piece, [(0, more if d == axis else 0) for d in range(2)])

        return [cut(gate_weight, 1), cut(up_weight, 1), cut(down_weight, 0)], None

    own, whole, pieces = pack([references, examples, cotangent])
    column = {0: own}
    step = far // 2
    while step:
        for s in sorted(column):
            column[s + step] = permute(column[s], "wide", dims, 0, step)
        step //= 2
    beside = {}
    if near == 2:
        for s, block in column.items():
            beside[s] = permute(block, "wide", dims, 1, 1)
    order = halvings(far)
    plane = [column[s] for s in order] + [beside[s] for s in order if near == 2]
    half = assemble(plane, whole, pieces, (r, e, k), depth)
    blocks_of_weights = {}
    early = ahead and pair == 2 and len(chunks) == 2
    if ahead:
        wanted = [(1, chunk) for chunk in chunks] + [(0, chunk) for chunk in chunks[1 if early else 0:]]
        for s, chunk in wanted:
            blocks_of_weights[s, chunk[0]] = fetch(*at_peer(s, *chunk), chunk[1])
    halves = [half]
    if pair == 2:
        halves.append(permute(half, "wide", dims, 2, 1))

    parts = []
    if early:
        (offset, width), (next_offset, next_width) = chunks
        weights = blocks_of_weights[1, offset]
        count = half.shape[0] // (r + e + k) * k
        kept_one = (*at_peer(0, offset, width), width)
        (sent,) = forward_half(halves[0], [], count, weights, width)
        received = [shift(sent, peers, 1)]
        upper = (*kept_one, (0, depth // 2), False, None)
        sent, both = forward_half(halves[1], halves, count, weights, width, upper)
        received.append(shift(sent, peers, 1))
        parts.append((offset, width, [tuple(received)]))
    main, side = join(halves, (r, e, k))
    if early:
        lower = (*kept_one, (depth // 2, depth - depth // 2), False, both)
        weights = blocks_of_weights[1, next_offset]
        sent, both = forward(main, side, weights, None, next_width, jnp.bfloat16, lower)
        parts.append((next_offset, next_width, [shift(sent, peers, 1)]))
        weights = blocks_of_weights[0, next_offset]
        kept_last, below = forward(
            main, side, weights, None, next_width, jnp.float32, (*kept_one, None, True, None)
        )
        blocks_of_weights[0, offset] = (both, below)
    else:
        for offset, width in chunks:
            received = []
            for s in range(1, peers):
                weights, place = at_peer(s, offset, width)
                if ahead:
                    weights = blocks_of_weights[s, offset]
                (sent,) = forward(main, side, weights, place, width, jnp.bfloat16)
                received.append(shift(sent, peers, s))
            parts.append((offset, width, received))

    jobs = []
    for i, (offset, width, received) in enumerate(parts):
        weights, place = at_peer(0, offset, width)
        if ahead:
            weights = blocks_of_weights[0, offset]
        if early and i == 1:
            kept = kept_last
        else:
            (kept,) = forward(main, side, weights, place, width, jnp.float32)
        grads = coefficients(kept, received, picks, points, blocks * e)
        jobs.append((grads, offset, width, 0))
        jobs += [(shift(grads, peers, s), offset, width, s) for s in range(1, peers)]
    items = []
    for grads, offset, width, s in jobs:
        weights, place = at_peer(peers - s, offset, width)
        weights = blocks_of_weights[s, offset][:1] if ahead else weights[:2]
        items.append((grads, weights, place))
    if ahead and len(items) == 4:
        groups = [items[:1], items[1:3], items[3:]]
    else:
        groups = [[item] for item in items]
    total = None
    for group in groups[:-1]:
        total = backward(group, total, False)
    spans = [(0, depth // 2), (depth // 2, depth // 2)] if depth % 256 == 0 else [(0, depth)]
    last = [backward(groups[-1], total, pair == 2, span) for span in spans]

    results = []
    for i, value in enumerate(last):
        if pair == 2:
            sent, kept = value
            value = kept + permute(sent, "wide", dims, 2, 1).astype(jnp.float32)
        digits = [(1, 1)] * (near == 2) + [(0, 1 << bit) for bit in range(far.bit_length() - 1)]
        steps = list(digits)
        if i % 2 and len(steps) > 1:
            steps[:2] = steps[1::-1]
        for step in steps:
            at = digits.index(step)
            outer, inner = 1 << at, value.shape[0] >> (at + 1)
            digits.remove(step)

            def half(which):
                rows = [value[(2 * o + which) * inner:(2 * o + which + 1) * inner] for o in range(outer)]
                return rows[0] if outer == 1 else jnp.concatenate(rows)

            got = permute(half(1).astype(jnp.bfloat16), "wide", dims, *step)
            value = half(0) + got.astype(jnp.float32)
        results.append(value)
    return jnp.concatenate(results, axis=1).astype(jnp.bfloat16)


def solution(mesh):
    in_specs = (
        P("wide", "narrow"),
        P("wide", "narrow"),
        P("narrow", "wide"),
        P("narrow", "wide"),
        P("wide", "narrow"),
        P("wide", "narrow"),
        P(),
        P(),
    )
    out_specs = P("wide", "narrow")
    return jax.shard_map(on_device, mesh=mesh, in_specs=in_specs, out_specs=out_specs, check_vma=False)
```
